32 devices in a mesh: dp: 4 (over y, z), ep: 8 (over x, core).
Axes of the slice: x: 4, y: 2, z: 2, core: 2. Of those that a mesh axis runs over, the one named last changes fastest.
The devices are a block of a 4x4x8 slice.
Arguments:
- hidden_in: bfloat16 [32768, 1536], P(('dp', 'ep')), parts along dimension 0
- topk_idx: int32 [32768, 6], P(('dp', 'ep')), parts along dimension 0
- norm_gain: bfloat16 [1536], replicated
- w_router: bfloat16 [1536, 64], replicated
- w_sgate: bfloat16 [1536, 1], replicated
- s_gate: bfloat16 [1536, 1024], replicated
- s_up: bfloat16 [1536, 1024], replicated
- s_down: bfloat16 [1024, 1536], replicated
- w_gate: bfloat16 [64, 1536, 512], P('ep')
- w_up: bfloat16 [64, 1536, 512], P('ep')
- w_down: bfloat16 [64, 512, 1536], P('ep')
Outputs:
- output: bfloat16 [32768, 1536], P(('dp', 'ep')), parts along dimension 0
There are 4 independent parts. The reference program is written for one: setup_inputs(seed, part) draws one part's arguments, and reference() takes and returns one part's arrays. A program takes and returns all parts, laid end to end along the dimension named above; an argument that names none is the same for every part.
All inputs are finite; a program needn't handle non-finite values.
Results may differ from the reference program's by a relative error of at most 0.001.
Values are sent between devices in bfloat16 or wider.
A program may use at most 768 MiB of HBM per device.

```python
import jax
import jax.numpy as jnp
from jax import lax

HIDDEN = 1536
EXPERTS = 64
EXPERT_SLOTS = 64
TOP_K = 6
EXPERT_FF = 512
SHARED_FF = 1024
TOKENS_DEV = 1024
GROUP_SIZE = 8

TOKENS = TOKENS_DEV * GROUP_SIZE
CAPACITY = (5 * TOKENS * TOP_K + 4 * EXPERTS - 1) // (4 * EXPERTS)
LOCAL_MAX = (2 * TOKENS_DEV * TOP_K + EXPERTS - 1) // EXPERTS
HOT_COUNT = EXPERTS // 4


def row_order(sub_key):
    return jax.random.permutation(sub_key, TOKENS_DEV)


def draw_routing(route_key):
    key_perm, key_shift, key_rows, key_cols = jax.random.split(route_key, 4)
    per_dev = TOKENS_DEV * TOP_K
    base_perm = jax.random.permutation(key_perm, EXPERTS)
    shifts = jax.random.randint(key_shift, (GROUP_SIZE,), 0, HOT_COUNT)
    pos_index = jnp.arange(per_dev)
    hot_total = HOT_COUNT * LOCAL_MAX
    rest_total = per_dev - hot_total
    rank_seq = jnp.where(pos_index < hot_total, pos_index // LOCAL_MAX,
                         HOT_COUNT + ((pos_index - hot_total) * (EXPERTS - HOT_COUNT)) // rest_total)
    choice = base_perm[(rank_seq[None, :] + shifts[:, None]) % EXPERTS]
    choice = choice.reshape(GROUP_SIZE, TOP_K, TOKENS_DEV).transpose(0, 2, 1)
    row_perm = jax.vmap(row_order)(jax.random.split(key_rows, GROUP_SIZE))
    choice = jnp.take_along_axis(choice, row_perm[:, :, None], axis=1)
    scores = jax.random.randint(key_cols, (GROUP_SIZE, TOKENS_DEV, TOP_K), 0, 1 << 20) * TOP_K + jnp.arange(TOP_K)
    choice = jnp.take_along_axis(choice, jnp.argsort(scores, axis=2), axis=2)
    return choice.reshape(TOKENS, TOP_K).astype(jnp.int32)


def setup_inputs(seed: int = 0, part: int = 0) -> dict:
    base_key = jax.random.key(seed)
    key_x, key_route = jax.random.split(jax.random.fold_in(base_key, part))
    weight_keys = jax.random.split(base_key, 9)
    in_scale = HIDDEN ** -0.5
    down_scale = (EXPERTS / TOP_K) * EXPERT_FF ** -0.5
    live_mask = (jnp.arange(EXPERT_SLOTS) < EXPERTS).astype(jnp.float32)[:, None, None]
    return {
        'hidden_in': (0.5 * jax.random.normal(key_x, (TOKENS, HIDDEN), jnp.float32)).astype(jnp.bfloat16),
        'topk_idx': draw_routing(key_route),
        'norm_gain': (1.0 + 0.3 * jax.random.normal(weight_keys[0], (HIDDEN,), jnp.float32)).astype(jnp.bfloat16),
        'w_router': (in_scale * jax.random.normal(weight_keys[1], (HIDDEN, EXPERTS), jnp.float32)).astype(jnp.bfloat16),
        'w_sgate': (in_scale * jax.random.normal(weight_keys[2], (HIDDEN, 1), jnp.float32)).astype(jnp.bfloat16),
        's_gate': (in_scale * jax.random.normal(weight_keys[3], (HIDDEN, SHARED_FF), jnp.float32)).astype(jnp.bfloat16),
        's_up': (in_scale * jax.random.normal(weight_keys[4], (HIDDEN, SHARED_FF), jnp.float32)).astype(jnp.bfloat16),
        's_down': (SHARED_FF ** -0.5 * jax.random.normal(weight_keys[5], (SHARED_FF, HIDDEN), jnp.float32)).astype(jnp.bfloat16),
        'w_gate': (in_scale * live_mask * jax.random.normal(weight_keys[6], (EXPERT_SLOTS, HIDDEN, EXPERT_FF), jnp.float32)).astype(jnp.bfloat16),
        'w_up': (in_scale * live_mask * jax.random.normal(weight_keys[7], (EXPERT_SLOTS, HIDDEN, EXPERT_FF), jnp.float32)).astype(jnp.bfloat16),
        'w_down': (down_scale * live_mask * jax.random.normal(weight_keys[8], (EXPERT_SLOTS, EXPERT_FF, HIDDEN), jnp.float32)).astype(jnp.bfloat16),
    }


def rms_norm(hidden_in, norm_gain):
    x_f32 = hidden_in.astype(jnp.float32)
    inv_rms = lax.rsqrt(jnp.mean(x_f32 * x_f32, axis=-1, keepdims=True) + 1e-6)
    return (x_f32 * inv_rms * norm_gain.astype(jnp.float32)).astype(jnp.bfloat16)


def expert_mlp(operands):
    expert_rows, gate_w, up_w, down_w = operands
    expert_act = (jax.nn.silu(jnp.dot(expert_rows, gate_w, preferred_element_type=jnp.float32))
                  * jnp.dot(expert_rows, up_w, preferred_element_type=jnp.float32)).astype(jnp.bfloat16)
    return jnp.dot(expert_act, down_w, preferred_element_type=jnp.float32).astype(jnp.bfloat16)


def reference(hidden_in, topk_idx, norm_gain, w_router, w_sgate, s_gate, s_up, s_down, w_gate, w_up, w_down):
    normed = rms_norm(hidden_in, norm_gain)
    router_probs = jax.nn.softmax(jnp.dot(normed, w_router, preferred_element_type=jnp.float32), axis=-1)
    gate_vals = jnp.take_along_axis(router_probs, topk_idx, axis=1)
    flat_ids = topk_idx.reshape(-1)
    onehot = (flat_ids[:, None] == jnp.arange(EXPERTS)[None, :]).astype(jnp.int32)
    position = jnp.sum((jnp.cumsum(onehot, axis=0) - onehot) * onehot, axis=1)
    slot_pos = jnp.where(position < CAPACITY, flat_ids * CAPACITY + position, EXPERTS * CAPACITY)
    token_of = jnp.arange(TOKENS * TOP_K) // TOP_K
    row_table = jnp.full((EXPERTS * CAPACITY,), TOKENS, jnp.int32).at[slot_pos].set(token_of, mode='drop')
    expert_rows = jnp.take(normed, row_table, axis=0, mode='fill', fill_value=0).reshape(EXPERTS, CAPACITY, HIDDEN)
    results = lax.map(expert_mlp, (expert_rows, w_gate[:EXPERTS], w_up[:EXPERTS], w_down[:EXPERTS]))
    picked = jnp.take(results.reshape(EXPERTS * CAPACITY, HIDDEN), slot_pos, axis=0, mode='fill', fill_value=0)
    picked = picked.reshape(TOKENS, TOP_K, HIDDEN)
    routed = jnp.sum(gate_vals[:, :, None] * picked.astype(jnp.float32), axis=1)
    shared_act = (jax.nn.silu(jnp.dot(normed, s_gate, preferred_element_type=jnp.float32))
                  * jnp.dot(normed, s_up, preferred_element_type=jnp.float32)).astype(jnp.bfloat16)
    shared_val = jnp.dot(shared_act, s_down, preferred_element_type=jnp.float32)
    shared_gate = jax.nn.sigmoid(jnp.dot(normed, w_sgate, preferred_element_type=jnp.float32))
    return (hidden_in.astype(jnp.float32) + routed + shared_gate * shared_val).astype(jnp.bfloat16)
```

```python
import functools

import jax
import jax.numpy as jnp
from jax import lax
from jax.experimental import pallas as pl
from jax.experimental.pallas import tpu as pltpu
from jax.sharding import PartitionSpec as P


F32, BF16 = jnp.float32, jnp.bfloat16
CLASSES = (64, 128, 192)


def rms_norm(hidden_in, norm_gain):
    x_f32 = hidden_in.astype(F32)
    inv_rms = lax.rsqrt(jnp.mean(x_f32 * x_f32, axis=-1, keepdims=True) + 1e-6)
    return (x_f32 * inv_rms * norm_gain.astype(F32)).astype(BF16)


def shared_expert(normed, w_sgate, s_gate, s_up, s_down):
    shared_act = (jax.nn.silu(jnp.dot(normed, s_gate, preferred_element_type=F32))
                  * jnp.dot(normed, s_up, preferred_element_type=F32)).astype(BF16)
    shared_val = jnp.dot(shared_act, s_down, preferred_element_type=F32)
    return jax.nn.sigmoid(jnp.dot(normed, w_sgate, preferred_element_type=F32)) * shared_val


def expert_kernel(first, classes, count_ref, ha_ref, hb_ref, pos_ref, gate_ref, wg_ref, wu_ref, wd_ref, *rest):
    if first:
        ya_ref, yb_ref, e_ref = rest
    else:
        ya_in, yb_in, ya_ref, yb_ref, e_ref = rest
    slot = pl.program_id(0)
    half = ha_ref.shape[0]
    toks = 2 * half
    hidden = ha_ref.shape[1]
    tile = 256

    @pl.when(slot == 0)
    def _():
        if first:
            ya_ref[...] = jnp.zeros_like(ya_ref)
            yb_ref[...] = jnp.zeros_like(yb_ref)
        else:
            ya_ref[...] = ya_in[...]
            yb_ref[...] = yb_in[...]

    count = count_ref[slot]
    low = 0
    for rows in classes:
        @pl.when((count > low) & (count <= rows))
        def _(rows=rows):
            pos = pos_ref[0]
            gate = gate_ref[0]
            hit = lax.broadcasted_iota(jnp.int32, (rows, toks), 0).astype(F32) == pos
            pick = jnp.where(hit, 1.0, 0.0).astype(BF16)
            x = (jnp.dot(pick[:, :half], ha_ref[...], preferred_element_type=F32)
                 + jnp.dot(pick[:, half:], hb_ref[...], preferred_element_type=F32)).astype(BF16)
            gate_proj = jnp.dot(x, wg_ref[0], preferred_element_type=F32)
            up_proj = jnp.dot(x, wu_ref[0], preferred_element_type=F32)
            act = (jax.nn.silu(gate_proj) * up_proj).astype(BF16)
            out = jnp.dot(act, wd_ref[0], preferred_element_type=F32).astype(BF16)
            for piece in range(3):
                e_ref[pl.ds(piece * rows, rows), :] = out
            g1 = gate.astype(BF16).astype(F32)
            g2 = (gate - g1).astype(BF16).astype(F32)
            g3 = gate - g1 - g2
            rows8 = lax.broadcasted_iota(jnp.int32, (8, toks), 0)
            packed = jnp.where(rows8 == 0, pos, jnp.where(rows8 == 1, g1, jnp.where(rows8 == 2, g2, g3)))
            cols = packed.T
            lane = lax.broadcasted_iota(jnp.int32, (toks, 3 * rows), 1)
            part0, part1 = lane < rows, lane < 2 * rows
            lane_slot = jnp.where(part0, lane, jnp.where(part1, lane - rows, lane - 2 * rows)).astype(F32)
            g_lane = jnp.where(part0, cols[:, 1:2], jnp.where(part1, cols[:, 2:3], cols[:, 3:4]))
            mix = jnp.where(lane_slot == cols[:, 0:1], g_lane, 0.0).astype(BF16)

            def column(i, carry):
                sl = pl.ds(pl.multiple_of(i * tile, tile), tile)
                add = jnp.dot(mix, e_ref[pl.ds(0, 3 * rows), sl], preferred_element_type=F32)
                ya_ref[:, sl] += add[:half]
                yb_ref[:, sl] += add[half:]
                return carry

            lax.fori_loop(0, hidden // tile, column, 0)
        low = rows


def expert_call(count, ha, hb, pos, gate, wg, wu, wd, sums, local_max):
    half, hidden = ha.shape
    slots, _, ff = wg.shape
    first = sums is None
    classes = tuple(c for c in CLASSES if c < local_max) + (local_max,)
    whole = pl.BlockSpec((half, hidden), lambda s: (0, 0), pipeline_mode=pl.Buffered(1))
    row = pl.BlockSpec((1, 1, 2 * half), lambda s: (s, 0, 0))
    in_specs = [pl.BlockSpec(memory_space=pltpu.SMEM), whole, whole, row, row,
                pl.BlockSpec((1, hidden, ff), lambda s: (s, 0, 0)),
                pl.BlockSpec((1, hidden, ff), lambda s: (s, 0, 0)),
                pl.BlockSpec((1, ff, hidden), lambda s: (s, 0, 0))]
    args = [count, ha, hb, pos, gate, wg, wu, wd]
    aliases = {}
    if not first:
        in_specs += [whole, whole]
        args += list(sums)
        aliases = {8: 0, 9: 1}
    out = jax.ShapeDtypeStruct((half, hidden), F32)
    return pl.pallas_call(
        functools.partial(expert_kernel, first, classes),
        grid=(slots,),
        out_shape=(out, out),
        in_specs=in_specs,
        out_specs=(whole, whole),
        scratch_shapes=[pltpu.VMEM((3 * local_max, hidden), BF16)],
        input_output_aliases=aliases,
        compiler_params=pltpu.CompilerParams(dimension_semantics=("arbitrary",), vmem_limit_bytes=60 * 1024 * 1024),
        cost_estimate=pl.CostEstimate(flops=slots * 3 * local_max * hidden * ff * 2, transcendentals=0,
                                      bytes_accessed=slots * 3 * hidden * ff * 2),
        name="experts",
    )(*args)


def solution(mesh):
    group_size = mesh.shape['ep']
    cores = 2
    right = [(i, (i + cores) % group_size) for i in range(group_size)]
    left = [(i, (i - cores) % group_size) for i in range(group_size)]
    sibling = [(i, i ^ 1) for i in range(group_size)]

    def device_block(hidden_in, topk_idx, norm_gain, w_router, w_sgate, s_gate, s_up, s_down, w_gate, w_up, w_down):
        tok_dev, hidden = hidden_in.shape
        top_k = topk_idx.shape[1]
        experts = w_router.shape[1]
        slots_dev = w_gate.shape[0]
        half = tok_dev // 2
        capacity = (5 * tok_dev * group_size * top_k + 4 * experts - 1) // (4 * experts)
        local_max = (2 * tok_dev * top_k + experts - 1) // experts
        me = lax.axis_index('ep')

        def go_right(v):
            return lax.ppermute(v, 'ep', right)

        def go_left(v):
            return lax.ppermute(v, 'ep', left)

        sib_gate = lax.ppermute(w_gate, 'ep', sibling)
        sib_up = lax.ppermute(w_up, 'ep', sibling)
        sib_down = lax.ppermute(w_down, 'ep', sibling)

        normed = rms_norm(hidden_in, norm_gain)
        ha, hb = normed[:half], normed[half:]
        ha_r1, hb_l1 = go_right(ha), go_left(hb)
        ha_r2, hb_l2 = go_right(ha_r1), go_left(hb_l1)
        hb_r1, ha_l1 = go_right(hb), go_left(ha)

        router_probs = jax.nn.softmax(jnp.dot(normed, w_router, preferred_element_type=F32), axis=-1)
        chosen = topk_idx[:, :, None] == jnp.arange(experts)[None, None, :]
        gate_vals = jnp.sum(jnp.where(chosen, router_probs[:, None, :], 0.0), axis=-1)
        table = jnp.concatenate([topk_idx.T.astype(F32), gate_vals.T], axis=0)
        tables = lax.all_gather(table, 'ep')
        first_slot = (me // cores) * (cores * slots_dev)
        slot_ids = (first_slot + jnp.arange(cores * slots_dev)).astype(F32)
        hits = tables[:, None, :top_k, :] == slot_ids[None, :, None, None]
        onehot = jnp.any(hits, axis=2)
        gates = jnp.sum(jnp.where(hits, tables[:, None, top_k:, :], 0.0), axis=2)
        counts = jnp.sum(onehot.astype(F32), axis=2)
        dev = jnp.arange(group_size)
        lower = jnp.sum(jnp.where(dev[:, None, None] > dev[None, :, None], counts[None], 0.0), axis=1)
        before = (jnp.arange(tok_dev)[:, None] < jnp.arange(tok_dev)[None, :]).astype(BF16)
        local_pos = jnp.einsum('det,tu->deu', onehot.astype(BF16), before, preferred_element_type=F32)
        kept = onehot & (local_pos + lower[:, :, None] < capacity)
        slot_pos = jnp.where(kept, local_pos, -1.0)
        kept_count = jnp.clip(capacity - lower, 0.0, counts).astype(jnp.int32)

        def experts_for(step, pair_a, pair_b):
            source = (me + step * cores) % group_size
            pos = lax.dynamic_index_in_dim(slot_pos, source, 0, keepdims=False).reshape(cores, slots_dev, 1, tok_dev)
            gate = lax.dynamic_index_in_dim(gates, source, 0, keepdims=False).reshape(cores, slots_dev, 1, tok_dev)
            cnt = lax.dynamic_index_in_dim(kept_count, source, 0, keepdims=False).reshape(cores, slots_dev)
            mine = me % cores

            def pick(v, i):
                return lax.dynamic_index_in_dim(v, i, 0, keepdims=False)

            sums = expert_call(pick(cnt, mine), pair_a, pair_b, pick(pos, mine), pick(gate, mine),
                               w_gate, w_up, w_down, None, local_max)
            return expert_call(pick(cnt, 1 - mine), pair_a, pair_b, pick(pos, 1 - mine), pick(gate, 1 - mine),
                               sib_gate, sib_up, sib_down, sums, local_max)

        y0a, y0b = experts_for(0, ha, hb)
        y2a, y2b = experts_for(2, ha_r2, hb_l2)
        p_ra, p_lb = go_right(y2a), go_left(y2b)
        y1a, y1b = experts_for(1, ha_l1, hb_l1)
        d_b = go_right(y1b)
        y3a, y3b = experts_for(3, ha_r1, hb_r1)
        d_a = go_left(y3a)
        z_a = go_right(y1a + p_ra)
        z_b = go_left(y3b + p_lb)
        shared_val = shared_expert(normed, w_sgate, s_gate, s_up, s_down)
        base = hidden_in.astype(F32) + shared_val
        out_a = (base[:half] + (y0a + d_a + z_a)).astype(BF16)
        out_b = (base[half:] + (y0b + d_b + z_b)).astype(BF16)
        return jnp.concatenate([out_a, out_b], axis=0)

    row_spec = P(('dp', 'ep'), None)
    full_spec = P(None, None)
    slot_spec = P('ep', None, None)
    in_specs = (row_spec, row_spec, P(None), full_spec, full_spec, full_spec, full_spec, full_spec,
                slot_spec, slot_spec, slot_spec)
    return jax.shard_map(device_block, mesh=mesh, in_specs=in_specs, out_specs=row_spec, check_vma=False)
```

```python
import functools

import jax
import jax.numpy as jnp
from jax import lax
from jax.experimental import pallas as pl
from jax.experimental.pallas import tpu as pltpu
from jax.sharding import PartitionSpec as P


F32, BF16 = jnp.float32, jnp.bfloat16
CLASSES = (64, 128, 192)


def rms_norm(hidden_in, norm_gain):
    x_f32 = hidden_in.astype(F32)
    inv_rms = lax.rsqrt(jnp.mean(x_f32 * x_f32, axis=-1, keepdims=True) + 1e-6)
    return (x_f32 * inv_rms * norm_gain.astype(F32)).astype(BF16)


def shared_expert(normed, w_sgate, s_gate, s_up, s_down):
    shared_act = (jax.nn.silu(jnp.dot(normed, s_gate, preferred_element_type=F32))
                  * jnp.dot(normed, s_up, preferred_element_type=F32)).astype(BF16)
    shared_val = jnp.dot(shared_act, s_down, preferred_element_type=F32)
    return jax.nn.sigmoid(jnp.dot(normed, w_sgate, preferred_element_type=F32)) * shared_val


def route_kernel(geom, ids_ref, own_ref, sib_ref, next_ref, far_ref, prev_ref, slot_ref, gate_ref, list_ref, count_ref, hot_ref):
    top_k, slots_dev, capacity, local_max = geom
    toks = own_ref.shape[1]
    slots = 2 * slots_dev
    chip, core = ids_ref[8], ids_ref[9]
    order = lax.broadcasted_iota(jnp.int32, (slots, 1), 0)
    slot_id = chip * slots + jnp.where(order < slots_dev, core * slots_dev + order, (1 - core) * slots_dev + order - slots_dev)
    slot_id = slot_id.astype(F32)
    tables = []
    for j, ref in enumerate((own_ref, next_ref, far_ref, prev_ref)):
        pair = (own_ref[...], sib_ref[...]) if j == 0 else (ref[0], ref[1])
        tables.append(pair)
    counts = []
    for j in range(4):
        for i in range(2):
            table = tables[j][i]
            hot = jnp.zeros((slots, toks), F32)
            gate = jnp.zeros((slots, toks), F32)
            for k in range(top_k):
                hit = table[k:k + 1, :] == slot_id
                hot = hot + jnp.where(hit, 1.0, 0.0)
                if i == 0:
                    gate = gate + jnp.where(hit, table[top_k + k:top_k + k + 1, :], 0.0)
            counts.append(jnp.sum(hot, axis=1, keepdims=True))
            if i == 0:
                hot_ref[pl.ds(j * slots, slots), :] = hot
                gate_ref[j] = gate
    hot_all = hot_ref[...]
    hot_bf = hot_all.astype(BF16)
    tile = 256
    for c in range(toks // tile):
        rows = lax.broadcasted_iota(jnp.int32, (toks, tile), 0)
        cols = lax.broadcasted_iota(jnp.int32, (toks, tile), 1) + c * tile
        before = jnp.where(rows < cols, 1.0, 0.0).astype(BF16)
        pos = jnp.dot(hot_bf, before, preferred_element_type=F32)
        for j in range(4):
            lower = jnp.zeros((slots, 1), F32)
            for q in range(8):
                lower = lower + counts[q] * (ids_ref[q] < ids_ref[2 * j]).astype(F32)
            part = pos[j * slots:(j + 1) * slots]
            kept = (hot_all[j * slots:(j + 1) * slots, c * tile:(c + 1) * tile] > 0.0) & (part + lower < capacity)
            slot_ref[j, :, c * tile:(c + 1) * tile] = jnp.where(kept, part, -1.0)
            if c == 0:
                count_ref[j] = jnp.broadcast_to(jnp.clip(capacity - lower, 0.0, counts[2 * j]), (slots, 128))
    token = lax.broadcasted_iota(jnp.int32, (8, toks), 1)
    high, low = token // 32, token % 32
    row8 = lax.broadcasted_iota(jnp.int32, (8, toks), 0)
    digits = jnp.where(row8 == 0, high, low).astype(F32).astype(BF16)
    row_of = lax.broadcasted_iota(jnp.int32, (slots, toks), 0)
    count_row = lax.broadcasted_iota(jnp.int32, (slots, 128), 0)

    def lists(e, carry):
        for j in range(4):
            pos = jnp.sum(jnp.where(row_of == e, slot_ref[j], 0.0), axis=0, keepdims=True)
            want = lax.broadcasted_iota(jnp.int32, (local_max, toks), 0).astype(F32)
            pick = jnp.where(want == pos, 1.0, 0.0).astype(BF16)
            got = lax.dot_general(digits, pick, (((1,), (1,)), ((), ())), preferred_element_type=F32)
            found = 32.0 * got[0:1] + got[1:2]
            held = jnp.sum(jnp.where(count_row == e, count_ref[j], 0.0), axis=0, keepdims=True)[:, 0:1]
            lane = lax.broadcasted_iota(jnp.int32, (1, local_max), 1).astype(F32)
            found = jnp.where(lane < held, found, float(toks)).astype(jnp.int32)
            list_ref[j, e] = jnp.broadcast_to(found, (8, local_max))
        return carry

    lax.fori_loop(0, slots, lists, 0)


def route_call(ids, own, sib, nxt, far, prv, top_k, slots_dev, capacity, local_max):
    toks = own.shape[1]
    slots = 2 * slots_dev
    vmem = pl.BlockSpec(memory_space=pltpu.VMEM)
    return pl.pallas_call(
        functools.partial(route_kernel, (top_k, slots_dev, capacity, local_max)),
        out_shape=(jax.ShapeDtypeStruct((4, slots, toks), F32), jax.ShapeDtypeStruct((4, slots, toks), F32),
                   jax.ShapeDtypeStruct((4, slots, 8, local_max), jnp.int32), jax.ShapeDtypeStruct((4, slots, 128), F32)),
        in_specs=[pl.BlockSpec(memory_space=pltpu.SMEM)] + [vmem] * 5,
        out_specs=(vmem,) * 4,
        scratch_shapes=[pltpu.VMEM((4 * slots, toks), F32)],
        cost_estimate=pl.CostEstimate(flops=20_000_000_000, transcendentals=0, bytes_accessed=2_000_000),
        name="route",
    )(ids, own, sib, nxt, far, prv)


def expert_kernel(classes, slots_dev, list_ref, count_ref, ha_ref, hb_ref, slot_ref, gate_ref, og, ou, od, sg, su, sd, dep_ref,
                  ya_ref, yb_ref, wg_ref, wu_ref, wd_ref, e_ref, y_ref, sems):
    step = pl.program_id(0)
    steps = 2 * slots_dev
    half, hidden = ha_ref.shape
    toks = 2 * half
    blocks = hidden // 128
    pitch = 16
    unroll = 8

    def copies(refs, i, b):
        return [pltpu.make_async_copy(src.at[i], dst.at[b], sems.at[n, b])
                for n, (src, dst) in enumerate(zip(refs, (wg_ref, wu_ref, wd_ref)))]

    def fetch(i, b):
        @pl.when(i < slots_dev)
        def _():
            for c in copies((og, ou, od), i, b):
                c.start()

        @pl.when(i >= slots_dev)
        def _():
            for c in copies((sg, su, sd), i - slots_dev, b):
                c.start()

    @pl.when(step == 0)
    def _():
        fetch(step, 0)

    @pl.when(step + 1 < steps)
    def _():
        fetch(step + 1, (step + 1) % 2)

    @pl.when(step == 0)
    def _():
        y_ref[...] = jnp.zeros_like(y_ref)

    buf = step % 2
    for c in copies((og, ou, od), 0, buf):
        c.wait()
    count = count_ref[step]
    row_of = lax.broadcasted_iota(jnp.int32, (steps, toks), 0)
    pos = jnp.sum(jnp.where(row_of == step, slot_ref[...], 0.0), axis=0, keepdims=True)
    gate = jnp.sum(jnp.where(row_of == step, gate_ref[...], 0.0), axis=0, keepdims=True)
    low = 0
    for rows in classes:
        @pl.when((count > low) & (count <= rows))
        def _(rows=rows):
            hit = lax.broadcasted_iota(jnp.int32, (rows, toks), 0).astype(F32) == pos
            pick = jnp.where(hit, 1.0, 0.0).astype(BF16)
            gcol = jnp.sum(jnp.where(hit, gate, 0.0), axis=1, keepdims=True)
            x = (jnp.dot(pick[:, :half], ha_ref[...], preferred_element_type=F32)
                 + jnp.dot(pick[:, half:], hb_ref[...], preferred_element_type=F32)).astype(BF16)
            gate_proj = jnp.dot(x, wg_ref[buf], preferred_element_type=F32)
            up_proj = jnp.dot(x, wu_ref[buf], preferred_element_type=F32)
            act = (jax.nn.silu(gate_proj) * up_proj).astype(BF16)
            out = jnp.dot(act, wd_ref[buf], preferred_element_type=F32).astype(BF16).astype(F32) * gcol
            for j in range(blocks):
                e_ref[pl.ds(j, rows, stride=pitch), :] = out[:, j * 128:(j + 1) * 128]
        low = rows

    def scatter(i, carry):
        spots, sums = [], []
        for u in range(unroll):
            r = i * unroll + u
            spot = pl.ds(pl.multiple_of(list_ref[step, r] * pitch, pitch), pitch)
            row = pl.ds(pl.multiple_of(r * pitch, pitch), pitch)
            spots.append(spot)
            sums.append(y_ref[spot, :] + e_ref[row, :])
        for spot, v in zip(spots, sums):
            y_ref[spot, :] = v
        return carry

    lax.fori_loop(0, (count + unroll - 1) // unroll, scatter, 0)

    @pl.when(step == steps - 1)
    def _():
        group = 64

        def unpack(i, carry):
            to = pl.ds(pl.multiple_of(i * group, group), group)
            for ref, start in ((ya_ref, 0), (yb_ref, half)):
                for j in range(blocks):
                    ref[to, j * 128:(j + 1) * 128] = y_ref[pl.ds((start + i * group) * pitch + j, group, stride=pitch), :]
            return carry

        lax.fori_loop(0, half // group, unpack, 0)


def expert_call(rows_list, count, ha, hb, slot, gate, own, sib, dep, local_max):
    half, hidden = ha.shape
    slots_dev, _, ff = own[0].shape
    classes = tuple(c for c in CLASSES if c < local_max) + (local_max,)
    whole = pl.BlockSpec((half, hidden), lambda s: (0, 0), pipeline_mode=pl.Buffered(1))
    table = pl.BlockSpec(slot.shape, lambda s: (0, 0), pipeline_mode=pl.Buffered(1))
    smem = pl.BlockSpec(memory_space=pltpu.SMEM)
    hbm = pl.BlockSpec(memory_space=pl.ANY)
    out = jax.ShapeDtypeStruct((half, hidden), F32)
    return pl.pallas_call(
        functools.partial(expert_kernel, classes, slots_dev),
        grid=(2 * slots_dev,),
        out_shape=(out, out),
        in_specs=[smem, smem, whole, whole, table, table] + [hbm] * 7,
        out_specs=(whole, whole),
        scratch_shapes=[pltpu.VMEM((2, hidden, ff), BF16), pltpu.VMEM((2, hidden, ff), BF16), pltpu.VMEM((2, ff, hidden), BF16),
                        pltpu.VMEM((local_max * 16, 128), F32), pltpu.VMEM(((2 * half + 8) * 16, 128), F32),
                        pltpu.SemaphoreType.DMA((3, 2))],
        compiler_params=pltpu.CompilerParams(dimension_semantics=("arbitrary",), vmem_limit_bytes=60 * 1024 * 1024),
        cost_estimate=pl.CostEstimate(flops=2 * slots_dev * 3 * local_max * hidden * ff * 2, transcendentals=0,
                                      bytes_accessed=2 * slots_dev * 3 * hidden * ff * 2),
        name="experts",
    )(rows_list, count, ha, hb, slot, gate, *own, *sib, dep)


def solution(mesh):
    group_size = mesh.shape['ep']
    cores = 2
    right = [(i, (i + cores) % group_size) for i in range(group_size)]
    left = [(i, (i - cores) % group_size) for i in range(group_size)]
    far = [(i, (i + group_size // 2) % group_size) for i in range(group_size)]
    sibling = [(i, i ^ 1) for i in range(group_size)]

    def device_block(hidden_in, topk_idx, norm_gain, w_router, w_sgate, s_gate, s_up, s_down, w_gate, w_up, w_down):
        tok_dev, hidden = hidden_in.shape
        top_k = topk_idx.shape[1]
        experts = w_router.shape[1]
        slots_dev = w_gate.shape[0]
        half = tok_dev // 2
        capacity = (5 * tok_dev * group_size * top_k + 4 * experts - 1) // (4 * experts)
        local_max = (2 * tok_dev * top_k + experts - 1) // experts
        me = lax.axis_index('ep')

        def go_right(v):
            return lax.ppermute(v, 'ep', right)

        def go_left(v):
            return lax.ppermute(v, 'ep', left)

        sib_gate = lax.ppermute(w_gate, 'ep', sibling)
        sib_up = lax.ppermute(w_up, 'ep', sibling)
        sib_down = lax.ppermute(w_down, 'ep', sibling)

        own_w = (w_gate, w_up, w_down)
        sib_w = (sib_gate, sib_up, sib_down)
        chip, core = me // cores, me % cores

        def after(v, *deps):
            return lax.optimization_barrier((v,) + deps)[0]

        normed = rms_norm(hidden_in, norm_gain)
        ha, hb = normed[:half], normed[half:]
        ha_r1, hb_l1 = go_right(ha), go_left(hb)

        router_probs = jax.nn.softmax(jnp.dot(normed, w_router, preferred_element_type=F32), axis=-1)
        chosen = topk_idx[:, :, None] == jnp.arange(experts)[None, None, :]
        gate_vals = jnp.sum(jnp.where(chosen, router_probs[:, None, :], 0.0), axis=-1)
        pad = (-2 * top_k) % 8
        table = jnp.concatenate([topk_idx.T.astype(F32), gate_vals.T, jnp.zeros((pad, tok_dev), F32)], axis=0)
        sib_table = lax.ppermute(table, 'ep', sibling)
        pair = jnp.stack([table, sib_table])
        t_r1, t_l1 = go_right(pair), go_left(pair)
        t_far = lax.ppermute(pair, 'ep', far)

        ha_r2, hb_l2 = go_right(ha_r1), go_left(hb_l1)
        hb_r1, ha_l1 = go_right(after(hb, ha_r1)), go_left(after(ha, hb_l1))

        steps = jnp.arange(group_size // cores)
        rel = cores * ((chip + steps) % (group_size // cores))
        ids = jnp.concatenate([jnp.stack([rel + core, rel + 1 - core], axis=1).reshape(-1), jnp.stack([chip, core])]).astype(jnp.int32)
        slot, gate, lists, kept = route_call(ids, table, sib_table, t_l1, t_far, t_r1, top_k, slots_dev, capacity, local_max)
        lists = lists[:, :, 0, :]
        kept = kept[:, :, 0].astype(jnp.int32)

        def experts_for(j, part_a, part_b, dep):
            return expert_call(lists[j], kept[j], part_a, part_b, slot[j], gate[j], own_w, sib_w, dep, local_max)

        y2a, y2b = experts_for(2, ha_r2, hb_l2, normed)
        p_ra, p_lb = go_right(y2a), go_left(y2b)
        y1a, y1b = experts_for(1, ha_l1, hb_l1, y2a)
        d_b = go_right(y1b)
        y3a, y3b = experts_for(3, ha_r1, hb_r1, y1a)
        d_a = go_left(y3a)
        z_a = go_right(y1a + p_ra)
        z_b = go_left(y3b + p_lb)
        y0a, y0b = experts_for(0, ha, hb, y3a)
        shared_val = shared_expert(after(normed, y3a), w_sgate, s_gate, s_up, s_down)
        base = hidden_in.astype(F32) + shared_val
        out_a = (base[:half] + (y0a + d_a + z_a)).astype(BF16)
        out_b = (base[half:] + (y0b + d_b + z_b)).astype(BF16)
        return jnp.concatenate([out_a, out_b], axis=0)

    row_spec = P(('dp', 'ep'), None)
    full_spec = P(None, None)
    slot_spec = P('ep', None, None)
    in_specs = (row_spec, row_spec, P(None), full_spec, full_spec, full_spec, full_spec, full_spec,
                slot_spec, slot_spec, slot_spec)
    return jax.shard_map(device_block, mesh=mesh, in_specs=in_specs, out_specs=row_spec, check_vma=False)
```

```python
import functools

import jax
import jax.numpy as jnp
from jax import lax
from jax.experimental import pallas as pl
from jax.experimental.pallas import tpu as pltpu
from jax.sharding import PartitionSpec as P


F32, BF16 = jnp.float32, jnp.bfloat16
CLASSES = (64, 128, 192)


def norm_kernel(x_ref, gain_ref, ha_ref, hb_ref):
    gain = gain_ref[...].astype(F32)
    for i, out_ref in enumerate((ha_ref, hb_ref)):
        x = x_ref[i].astype(F32)
        inv_rms = lax.rsqrt(jnp.mean(x * x, axis=-1, keepdims=True) + 1e-6)
        out_ref[...] = (x * inv_rms * gain).astype(BF16)


def norm_call(hidden_in, norm_gain):
    toks, hidden = hidden_in.shape
    half, rows = toks // 2, 128
    out = jax.ShapeDtypeStruct((half, hidden), BF16)
    block = pl.BlockSpec((rows, hidden), lambda i: (i, 0))
    return pl.pallas_call(
        norm_kernel,
        grid=(half // rows,),
        out_shape=(out, out),
        in_specs=[pl.BlockSpec((2, rows, hidden), lambda i: (0, i, 0)), pl.BlockSpec((1, hidden), lambda i: (0, 0))],
        out_specs=(block, block),
        compiler_params=pltpu.CompilerParams(dimension_semantics=("arbitrary",)),
        cost_estimate=pl.CostEstimate(flops=4 * toks * hidden, transcendentals=toks, bytes_accessed=4 * toks * hidden),
        name="norm",
    )(hidden_in.reshape(2, half, hidden), norm_gain.reshape(1, hidden))


def final_kernel(base_a, base_b, za_ref, zb_ref, out_ref):
    out_ref[0] = (base_a[...] + za_ref[...]).astype(BF16)
    out_ref[1] = (base_b[...] + zb_ref[...]).astype(BF16)


def final_call(base_a, base_b, za, zb):
    half, hidden = za.shape
    rows = 128
    block = pl.BlockSpec((rows, hidden), lambda i: (i, 0))
    out = pl.pallas_call(
        final_kernel,
        grid=(half // rows,),
        out_shape=jax.ShapeDtypeStruct((2, half, hidden), BF16),
        in_specs=[block] * 4,
        out_specs=pl.BlockSpec((2, rows, hidden), lambda i: (0, i, 0)),
        compiler_params=pltpu.CompilerParams(dimension_semantics=("arbitrary",)),
        cost_estimate=pl.CostEstimate(flops=2 * half * hidden, transcendentals=0, bytes_accessed=20 * half * hidden),
        name="final",
    )(base_a, base_b, za, zb)
    return out.reshape(2 * half, hidden)


def shared_expert(normed, w_sgate, s_gate, s_up, s_down):
    shared_act = (jax.nn.silu(jnp.dot(normed, s_gate, preferred_element_type=F32))
                  * jnp.dot(normed, s_up, preferred_element_type=F32)).astype(BF16)
    shared_val = jnp.dot(shared_act, s_down, preferred_element_type=F32)
    return jax.nn.sigmoid(jnp.dot(normed, w_sgate, preferred_element_type=F32)) * shared_val


def route_kernel(geom, ids_ref, own_ref, sib_ref, next_ref, far_ref, prev_ref, slot_ref, gate_ref, list_ref, count_ref, hot_ref):
    top_k, slots_dev, capacity, local_max = geom
    toks = own_ref.shape[1]
    slots = 2 * slots_dev
    chip, core = ids_ref[8], ids_ref[9]
    order = lax.broadcasted_iota(jnp.int32, (slots, 1), 0)
    slot_id = chip * slots + jnp.where(order < slots_dev, core * slots_dev + order, (1 - core) * slots_dev + order - slots_dev)
    slot_id = slot_id.astype(F32)
    tables = []
    for j, ref in enumerate((own_ref, next_ref, far_ref, prev_ref)):
        pair = (own_ref[...], sib_ref[...]) if j == 0 else (ref[0], ref[1])
        tables.append(pair)
    counts = []
    for j in range(4):
        for i in range(2):
            table = tables[j][i]
            hot = jnp.zeros((slots, toks), F32)
            gate = jnp.zeros((slots, toks), F32)
            for k in range(top_k):
                hit = table[k:k + 1, :] == slot_id
                hot = hot + jnp.where(hit, 1.0, 0.0)
                if i == 0:
                    gate = gate + jnp.where(hit, table[top_k + k:top_k + k + 1, :], 0.0)
            counts.append(jnp.sum(hot, axis=1, keepdims=True))
            if i == 0:
                hot_ref[pl.ds(j * slots, slots), :] = hot
                gate_ref[j] = gate
    hot_all = hot_ref[...]
    hot_bf = hot_all.astype(BF16)
    tile = 256
    for c in range(toks // tile):
        rows = lax.broadcasted_iota(jnp.int32, (toks, tile), 0)
        cols = lax.broadcasted_iota(jnp.int32, (toks, tile), 1) + c * tile
        before = jnp.where(rows < cols, 1.0, 0.0).astype(BF16)
        pos = jnp.dot(hot_bf, before, preferred_element_type=F32)
        for j in range(4):
            lower = jnp.zeros((slots, 1), F32)
            for q in range(8):
                lower = lower + counts[q] * (ids_ref[q] < ids_ref[2 * j]).astype(F32)
            part = pos[j * slots:(j + 1) * slots]
            kept = (hot_all[j * slots:(j + 1) * slots, c * tile:(c + 1) * tile] > 0.0) & (part + lower < capacity)
            slot_ref[j, :, c * tile:(c + 1) * tile] = jnp.where(kept, part, -1.0)
            if c == 0:
                count_ref[j] = jnp.broadcast_to(jnp.clip(capacity - lower, 0.0, counts[2 * j]), (slots, 128))
    token = lax.broadcasted_iota(jnp.int32, (8, toks), 1)
    high, low = token // 32, token % 32
    row8 = lax.broadcasted_iota(jnp.int32, (8, toks), 0)
    digits = jnp.where(row8 == 0, high, low).astype(F32).astype(BF16)
    row_of = lax.broadcasted_iota(jnp.int32, (slots, toks), 0)
    count_row = lax.broadcasted_iota(jnp.int32, (slots, 128), 0)

    def lists(e, carry):
        for j in range(4):
            pos = jnp.sum(jnp.where(row_of == e, slot_ref[j], 0.0), axis=0, keepdims=True)
            want = lax.broadcasted_iota(jnp.int32, (local_max, toks), 0).astype(F32)
            pick = jnp.where(want == pos, 1.0, 0.0).astype(BF16)
            got = lax.dot_general(digits, pick, (((1,), (1,)), ((), ())), preferred_element_type=F32)
            found = 32.0 * got[0:1] + got[1:2]
            held = jnp.sum(jnp.where(count_row == e, count_ref[j], 0.0), axis=0, keepdims=True)[:, 0:1]
            lane = lax.broadcasted_iota(jnp.int32, (1, local_max), 1).astype(F32)
            found = jnp.where(lane < held, found, float(toks)).astype(jnp.int32)
            list_ref[j, e] = jnp.broadcast_to(found, (8, local_max))
        return carry

    lax.fori_loop(0, slots, lists, 0)


def route_call(ids, own, sib, nxt, far, prv, top_k, slots_dev, capacity, local_max):
    toks = own.shape[1]
    slots = 2 * slots_dev
    vmem = pl.BlockSpec(memory_space=pltpu.VMEM)
    return pl.pallas_call(
        functools.partial(route_kernel, (top_k, slots_dev, capacity, local_max)),
        out_shape=(jax.ShapeDtypeStruct((4, slots, toks), F32), jax.ShapeDtypeStruct((4, slots, toks), F32),
                   jax.ShapeDtypeStruct((4, slots, 8, local_max), jnp.int32), jax.ShapeDtypeStruct((4, slots, 128), F32)),
        in_specs=[pl.BlockSpec(memory_space=pltpu.SMEM)] + [vmem] * 5,
        out_specs=(vmem,) * 4,
        scratch_shapes=[pltpu.VMEM((4 * slots, toks), F32)],
        cost_estimate=pl.CostEstimate(flops=1_000_000, transcendentals=0, bytes_accessed=2_000_000),
        name="route",
    )(ids, own, sib, nxt, far, prv)


def expert_kernel(n_src, classes, slots_dev, depth, *refs):
    refs = list(refs)

    def take(n):
        got = refs[:n]
        del refs[:n]
        return got

    lists, counts = take(n_src), take(n_src)
    ha, hb, slot_refs, gate_refs = take(n_src), take(n_src), take(n_src), take(n_src)
    own, sib = take(3), take(3)
    take(1)
    ya, yb = take(n_src), take(n_src)
    wg_ref, wu_ref, wd_ref = take(3)
    e_refs, y_refs = take(n_src), take(n_src)
    sems, = take(1)
    step = pl.program_id(0)
    steps = 2 * slots_dev
    half, hidden = ha[0].shape
    toks = 2 * half
    blocks = hidden // 128
    pitch = 16
    unroll = 8

    def copies(srcs, i, b):
        return [pltpu.make_async_copy(src.at[i], dst.at[b], sems.at[n, b])
                for n, (src, dst) in enumerate(zip(srcs, (wg_ref, wu_ref, wd_ref)))]

    def fetch(i):
        @pl.when(i < slots_dev)
        def _():
            for c in copies(own, i, i % depth):
                c.start()

        @pl.when((i >= slots_dev) & (i < steps))
        def _():
            for c in copies(sib, i - slots_dev, i % depth):
                c.start()

    @pl.when(step == 0)
    def _():
        for i in range(depth - 1):
            fetch(jnp.int32(i))
        for y_ref in y_refs:
            y_ref[...] = jnp.zeros_like(y_ref)

    fetch(step + depth - 1)
    buf = step % depth
    for c in copies(own, 0, buf):
        c.wait()
    row_of = lax.broadcasted_iota(jnp.int32, (steps, toks), 0)
    count = [c[step] for c in counts]
    most = count[0] if n_src == 1 else jnp.maximum(count[0], count[1])
    pos = [jnp.sum(jnp.where(row_of == step, r[...], 0.0), axis=0, keepdims=True) for r in slot_refs]
    gate = [jnp.sum(jnp.where(row_of == step, r[...], 0.0), axis=0, keepdims=True) for r in gate_refs]
    low = 0
    for rows in classes:
        @pl.when((most > low) & (most <= rows))
        def _(rows=rows):
            xs, gcols = [], []
            for q in range(n_src):
                hit = lax.broadcasted_iota(jnp.int32, (rows, toks), 0).astype(F32) == pos[q]
                pick = jnp.where(hit, 1.0, 0.0).astype(BF16)
                gcols.append(jnp.sum(jnp.where(hit, gate[q], 0.0), axis=1, keepdims=True))
                xs.append((jnp.dot(pick[:, :half], ha[q][...], preferred_element_type=F32)
                           + jnp.dot(pick[:, half:], hb[q][...], preferred_element_type=F32)).astype(BF16))
            x = xs[0] if n_src == 1 else jnp.concatenate(xs, axis=0)
            gate_proj = jnp.dot(x, wg_ref[buf], preferred_element_type=F32)
            up_proj = jnp.dot(x, wu_ref[buf], preferred_element_type=F32)
            act = (jax.nn.silu(gate_proj) * up_proj).astype(BF16)
            out = jnp.dot(act, wd_ref[buf], preferred_element_type=F32).astype(BF16).astype(F32)
            for q in range(n_src):
                part = out[q * rows:(q + 1) * rows] * gcols[q]
                for j in range(blocks):
                    e_refs[q][pl.ds(j, rows, stride=pitch), :] = part[:, j * 128:(j + 1) * 128]

        low = rows

    for q in range(n_src):
        y_ref, e_ref, list_ref = y_refs[q], e_refs[q], lists[q]

        def scatter(i, carry):
            spots, sums = [], []
            for u in range(unroll):
                r = i * unroll + u
                spot = pl.ds(pl.multiple_of(list_ref[step, r] * pitch, pitch), pitch)
                row = pl.ds(pl.multiple_of(r * pitch, pitch), pitch)
                spots.append(spot)
                sums.append(y_ref[spot, :] + e_ref[row, :])
            for spot, v in zip(spots, sums):
                y_ref[spot, :] = v
            return carry

        lax.fori_loop(0, (count[q] + unroll - 1) // unroll, scatter, 0)

    @pl.when(step == steps - 1)
    def _():
        group = 64

        def unpack(i, carry):
            to = pl.ds(pl.multiple_of(i * group, group), group)
            for q in range(n_src):
                for ref, start in ((ya[q], 0), (yb[q], half)):
                    for j in range(blocks):
                        ref[to, j * 128:(j + 1) * 128] = y_refs[q][pl.ds((start + i * group) * pitch + j, group, stride=pitch), :]
            return carry

        lax.fori_loop(0, half // group, unpack, 0)


def expert_call(sources, own, sib, dep, local_max):
    n_src = len(sources)
    lists, counts, has, hbs, slots, gates = zip(*sources)
    half, hidden = has[0].shape
    slots_dev, _, ff = own[0].shape
    depth = 4 if n_src == 1 else 3
    classes = tuple(c for c in CLASSES if c < local_max) + (local_max,)
    whole = pl.BlockSpec((half, hidden), lambda s: (0, 0), pipeline_mode=pl.Buffered(1))
    table = pl.BlockSpec(slots[0].shape, lambda s: (0, 0), pipeline_mode=pl.Buffered(1))
    smem = pl.BlockSpec(memory_space=pltpu.SMEM)
    hbm = pl.BlockSpec(memory_space=pl.ANY)
    out = jax.ShapeDtypeStruct((half, hidden), F32)
    got = pl.pallas_call(
        functools.partial(expert_kernel, n_src, classes, slots_dev, depth),
        grid=(2 * slots_dev,),
        out_shape=(out,) * (2 * n_src),
        in_specs=[smem] * (2 * n_src) + [whole] * (2 * n_src) + [table] * (2 * n_src) + [hbm] * 7,
        out_specs=(whole,) * (2 * n_src),
        scratch_shapes=[pltpu.VMEM((depth, hidden, ff), BF16), pltpu.VMEM((depth, hidden, ff), BF16), pltpu.VMEM((depth, ff, hidden), BF16)]
        + [pltpu.VMEM((local_max * 16, 128), F32)] * n_src + [pltpu.VMEM(((2 * half + 8) * 16, 128), F32)] * n_src
        + [pltpu.SemaphoreType.DMA((3, depth))],
        compiler_params=pltpu.CompilerParams(dimension_semantics=("arbitrary",), vmem_limit_bytes=62 * 1024 * 1024),
        cost_estimate=pl.CostEstimate(flops=1_000_000, transcendentals=0,
                                      bytes_accessed=2 * slots_dev * 3 * hidden * ff * 2),
        name="experts",
    )(*lists, *counts, *has, *hbs, *slots, *gates, *own, *sib, dep)
    return got[:n_src], got[n_src:]


def solution(mesh):
    group_size = mesh.shape['ep']
    cores = 2
    right = [(i, (i + cores) % group_size) for i in range(group_size)]
    left = [(i, (i - cores) % group_size) for i in range(group_size)]
    far = [(i, (i + group_size // 2) % group_size) for i in range(group_size)]
    sibling = [(i, i ^ 1) for i in range(group_size)]

    def block(hidden_in, topk_idx, norm_gain, w_router, w_sgate, s_gate, s_up, s_down, w_gate, w_up, w_down):
        tok_dev, _ = hidden_in.shape
        top_k = topk_idx.shape[1]
        experts = w_router.shape[1]
        slots_dev = w_gate.shape[0]
        half = tok_dev // 2
        capacity = (5 * tok_dev * group_size * top_k + 4 * experts - 1) // (4 * experts)
        local_max = (2 * tok_dev * top_k + experts - 1) // experts
        me = lax.axis_index('ep')

        def go_right(v):
            return lax.ppermute(v, 'ep', right)

        def go_left(v):
            return lax.ppermute(v, 'ep', left)

        chip, core = me // cores, me % cores

        def after(v, *deps):
            return lax.optimization_barrier((v,) + deps)[0]

        ha, hb = norm_call(hidden_in, norm_gain)
        ha_r1, hb_l1 = go_right(ha), go_left(hb)

        logits = jnp.concatenate([jnp.dot(h, w_router, preferred_element_type=F32) for h in (ha, hb)], axis=0)
        router_probs = jax.nn.softmax(logits, axis=-1)
        chosen = topk_idx[:, :, None] == jnp.arange(experts)[None, None, :]
        gate_vals = jnp.sum(jnp.where(chosen, router_probs[:, None, :], 0.0), axis=-1)
        pad = (-2 * top_k) % 8
        table = jnp.concatenate([topk_idx.T.astype(F32), gate_vals.T, jnp.zeros((pad, tok_dev), F32)], axis=0)
        sib_table = lax.ppermute(table, 'ep', sibling)
        own_w = (w_gate, w_up, w_down)
        sib_w = tuple(lax.ppermute(after(w, sib_table), 'ep', sibling) for w in own_w)
        pair = jnp.stack([table, sib_table])
        t_r1, t_l1 = go_right(pair), go_left(pair)
        t_far = lax.ppermute(pair, 'ep', far)

        ha_r2, hb_l2 = go_right(ha_r1), go_left(hb_l1)
        hb_r1, ha_l1 = go_right(after(hb, ha_r1)), go_left(after(ha, hb_l1))

        steps = jnp.arange(group_size // cores)
        rel = cores * ((chip + steps) % (group_size // cores))
        ids = jnp.concatenate([jnp.stack([rel + core, rel + 1 - core], axis=1).reshape(-1), jnp.stack([chip, core])]).astype(jnp.int32)
        slot, gate, lists, kept = route_call(ids, table, sib_table, t_l1, t_far, t_r1, top_k, slots_dev, capacity, local_max)
        lists = lists[:, :, 0, :]
        kept = kept[:, :, 0].astype(jnp.int32)

        def source(j, part_a, part_b):
            return lists[j], kept[j], part_a, part_b, slot[j], gate[j]

        (y2a,), (y2b,) = expert_call([source(2, ha_r2, hb_l2)], own_w, sib_w, ha, local_max)
        p_ra, p_lb = go_right(y2a), go_left(y2b)
        (y1a, y3a), (y1b, y3b) = expert_call([source(1, ha_l1, hb_l1), source(3, ha_r1, hb_r1)], own_w, sib_w, y2a, local_max)
        d_b, d_a = go_right(y1b), go_left(y3a)
        (y0a,), (y0b,) = expert_call([source(0, ha, hb)], own_w, sib_w, y3a, local_max)
        p_ra, p_lb = after(p_ra, y0a), after(p_lb, y0b)
        z_a, z_b = go_right(y1a + p_ra), go_left(y3b + p_lb)
        base = []
        for i, (h, y0) in enumerate(((ha, y0a), (hb, y0b))):
            shared_val = shared_expert(after(h, y0a), w_sgate, s_gate, s_up, s_down)
            base.append(hidden_in[i * half:(i + 1) * half].astype(F32) + shared_val + y0)
        return final_call(base[0] + d_a, base[1] + d_b, z_a, z_b)

    row_spec = P(('dp', 'ep'), None)
    full_spec = P(None, None)
    slot_spec = P('ep', None, None)
    in_specs = (row_spec, row_spec, P(None), full_spec, full_spec, full_spec, full_spec, full_spec,
                slot_spec, slot_spec, slot_spec)
    return jax.shard_map(block, mesh=mesh, in_specs=in_specs, out_specs=row_spec, check_vma=False)
```

```python
import functools

import jax
import jax.numpy as jnp
from jax import lax
from jax.experimental import pallas as pl
from jax.experimental.pallas import tpu as pltpu
from jax.sharding import PartitionSpec as P


F32, BF16 = jnp.float32, jnp.bfloat16
CLASSES = (64, 128, 192)


def norm_kernel(x_ref, gain_ref, ha_ref, hb_ref):
    gain = gain_ref[...].astype(F32)
    for i, out_ref in enumerate((ha_ref, hb_ref)):
        x = x_ref[i].astype(F32)
        inv_rms = lax.rsqrt(jnp.mean(x * x, axis=-1, keepdims=True) + 1e-6)
        out_ref[...] = (x * inv_rms * gain).astype(BF16)


def norm_call(hidden_in, norm_gain):
    toks, hidden = hidden_in.shape
    half, rows = toks // 2, 128
    out = jax.ShapeDtypeStruct((half, hidden), BF16)
    block = pl.BlockSpec((rows, hidden), lambda i: (i, 0))
    return pl.pallas_call(
        norm_kernel,
        grid=(half // rows,),
        out_shape=(out, out),
        in_specs=[pl.BlockSpec((2, rows, hidden), lambda i: (0, i, 0)), pl.BlockSpec((1, hidden), lambda i: (0, 0))],
        out_specs=(block, block),
        compiler_params=pltpu.CompilerParams(dimension_semantics=("arbitrary",)),
        cost_estimate=pl.CostEstimate(flops=4 * toks * hidden, transcendentals=toks, bytes_accessed=4 * toks * hidden),
        name="norm",
    )(hidden_in.reshape(2, half, hidden), norm_gain.reshape(1, hidden))


def final_kernel(base_a, base_b, za_ref, zb_ref, out_ref):
    out_ref[0] = (base_a[...] + za_ref[...]).astype(BF16)
    out_ref[1] = (base_b[...] + zb_ref[...]).astype(BF16)


def final_call(base_a, base_b, za, zb):
    half, hidden = za.shape
    rows = 128
    block = pl.BlockSpec((rows, hidden), lambda i: (i, 0))
    out = pl.pallas_call(
        final_kernel,
        grid=(half // rows,),
        out_shape=jax.ShapeDtypeStruct((2, half, hidden), BF16),
        in_specs=[block] * 4,
        out_specs=pl.BlockSpec((2, rows, hidden), lambda i: (0, i, 0)),
        compiler_params=pltpu.CompilerParams(dimension_semantics=("arbitrary",)),
        cost_estimate=pl.CostEstimate(flops=2 * half * hidden, transcendentals=0, bytes_accessed=20 * half * hidden),
        name="final",
    )(base_a, base_b, za, zb)
    return out.reshape(2 * half, hidden)


def shared_expert(normed, w_sgate, s_gate, s_up, s_down):
    shared_act = (jax.nn.silu(jnp.dot(normed, s_gate, preferred_element_type=F32))
                  * jnp.dot(normed, s_up, preferred_element_type=F32)).astype(BF16)
    shared_val = jnp.dot(shared_act, s_down, preferred_element_type=F32)
    return jax.nn.sigmoid(jnp.dot(normed, w_sgate, preferred_element_type=F32)) * shared_val


def route_kernel(geom, ids_ref, own_ref, next_ref, far_ref, prev_ref, list_ref, glist_ref, count_ref, slot_ref, gate_ref):
    top_k, slots_dev, capacity, local_max = geom
    toks = own_ref.shape[1]
    slots = 2 * slots_dev
    chip, core = ids_ref[8], ids_ref[9]

    def slot_column(like):
        order = lax.broadcasted_iota(jnp.int32, like, 0)
        mine = core * slots_dev + order
        other = (1 - core) * slots_dev + order - slots_dev
        return (chip * slots + jnp.where(order < slots_dev, mine, other)).astype(F32)

    slot_id = slot_column((slots, 1))
    lane_id = lax.broadcasted_iota(jnp.int32, (slots, 128), 1).astype(F32)
    hots, counts = [], []
    for j, ref in enumerate((own_ref, next_ref, far_ref, prev_ref)):
        table = ref[...]
        hot = jnp.zeros((slots, toks), F32)
        gate = jnp.zeros((slots, toks), F32)
        for k in range(top_k):
            hit = table[k:k + 1, :] == slot_id
            hot = hot + jnp.where(hit, 1.0, 0.0)
            gate = gate + jnp.where(hit, table[top_k + k:top_k + k + 1, :], 0.0)
        for i in range(2):
            row = table[2 * top_k + i:2 * top_k + i + 1, :128]
            counts.append(jnp.sum(jnp.where(lane_id == slot_id, row, 0.0), axis=1, keepdims=True))
        hots.append(hot)
        gate_ref[j] = gate
    hot_all = jnp.concatenate(hots, axis=0)
    hot_bf = hot_all.astype(BF16)
    tile = 256
    for c in range(toks // tile):
        rows = lax.broadcasted_iota(jnp.int32, (toks, tile), 0)
        cols = lax.broadcasted_iota(jnp.int32, (toks, tile), 1) + c * tile
        before = jnp.where(rows < cols, 1.0, 0.0).astype(BF16)
        pos = jnp.dot(hot_bf, before, preferred_element_type=F32)
        for j in range(4):
            lower = jnp.zeros((slots, 1), F32)
            for q in range(8):
                lower = lower + counts[q] * (ids_ref[q] < ids_ref[2 * j]).astype(F32)
            part = pos[j * slots:(j + 1) * slots]
            kept = (hot_all[j * slots:(j + 1) * slots, c * tile:(c + 1) * tile] > 0.0) & (part + lower < capacity)
            slot_ref[j, :, c * tile:(c + 1) * tile] = jnp.where(kept, part, -1.0)
            if c == 0:
                count_ref[j] = jnp.broadcast_to(jnp.clip(capacity - lower, 0.0, counts[2 * j]), (slots, 128))
    token = lax.broadcasted_iota(jnp.int32, (8, toks), 1)
    row8 = lax.broadcasted_iota(jnp.int32, (8, toks), 0)
    digits = jnp.where(row8 == 0, token // 32, token % 32).astype(F32)
    row_of = lax.broadcasted_iota(jnp.int32, (slots, toks), 0)
    count_row = lax.broadcasted_iota(jnp.int32, (slots, 128), 0)

    def lists(e, carry):
        for j in range(4):
            pos = jnp.sum(jnp.where(row_of == e, slot_ref[j], 0.0), axis=0, keepdims=True)
            gate = jnp.sum(jnp.where(row_of == e, gate_ref[j], 0.0), axis=0, keepdims=True)
            g1 = gate.astype(BF16).astype(F32)
            g2 = (gate - g1).astype(BF16).astype(F32)
            g3 = gate - g1 - g2
            left = jnp.where(row8 < 2, digits, jnp.where(row8 == 2, g1, jnp.where(row8 == 3, g2, g3))).astype(BF16)
            want = lax.broadcasted_iota(jnp.int32, (local_max, toks), 0).astype(F32)
            pick = jnp.where(want == pos, 1.0, 0.0).astype(BF16)
            got = lax.dot_general(left, pick, (((1,), (1,)), ((), ())), preferred_element_type=F32)
            found = 32.0 * got[0:1] + got[1:2]
            held = jnp.sum(jnp.where(count_row == e, count_ref[j], 0.0), axis=0, keepdims=True)[:, 0:1]
            lane = lax.broadcasted_iota(jnp.int32, (1, local_max), 1).astype(F32)
            found = jnp.where(lane < held, found, float(toks)).astype(jnp.int32)
            list_ref[j, e] = jnp.broadcast_to(found, (8, local_max))
            glist_ref[j, e] = jnp.broadcast_to((got[2:3] + got[3:4]) + got[4:5], (8, local_max))
        return carry

    lax.fori_loop(0, slots, lists, 0)


def route_call(ids, own, nxt, far, prv, top_k, slots_dev, capacity, local_max):
    toks = own.shape[1]
    slots = 2 * slots_dev
    vmem = pl.BlockSpec(memory_space=pltpu.VMEM)
    return pl.pallas_call(
        functools.partial(route_kernel, (top_k, slots_dev, capacity, local_max)),
        out_shape=(jax.ShapeDtypeStruct((4, slots, 8, local_max), jnp.int32), jax.ShapeDtypeStruct((4, slots, 8, local_max), F32),
                   jax.ShapeDtypeStruct((4, slots, 128), F32)),
        in_specs=[pl.BlockSpec(memory_space=pltpu.SMEM)] + [vmem] * 4,
        out_specs=(vmem,) * 3,
        scratch_shapes=[pltpu.VMEM((4, slots, toks), F32), pltpu.VMEM((4, slots, toks), F32)],
        cost_estimate=pl.CostEstimate(flops=1_000_000, transcendentals=0, bytes_accessed=2_000_000),
        name="route",
    )(ids, own, nxt, far, prv)


def expert_kernel(n_src, classes, slots_dev, depth, *refs):
    refs = list(refs)

    def take(n):
        got = refs[:n]
        del refs[:n]
        return got

    lists, glists, counts = take(n_src), take(n_src), take(n_src)
    has, hbs = take(n_src), take(n_src)
    own, sib = take(3), take(3)
    take(1)
    yas, ybs = take(n_src), take(n_src)
    wg_ref, wu_ref, wd_ref = take(3)
    row_refs, tok_refs, sum_refs = [take(2) for _ in range(n_src)], [take(2) for _ in range(n_src)], [take(2) for _ in range(n_src)]
    stage_ref, sems, out_sems = take(3)
    step = pl.program_id(0)
    steps = 2 * slots_dev
    half, hidden = has[0].shape
    blocks = hidden // 128
    pitch, unroll, group = 8, 8, 64
    split = [(j // pitch, j % pitch) for j in range(blocks)]

    def copies(srcs, i, b):
        return [pltpu.make_async_copy(src.at[i], dst.at[b], sems.at[n, b])
                for n, (src, dst) in enumerate(zip(srcs, (wg_ref, wu_ref, wd_ref)))]

    def fetch(i):
        @pl.when(i < slots_dev)
        def _():
            for c in copies(own, i, i % depth):
                c.start()

        @pl.when((i >= slots_dev) & (i < steps))
        def _():
            for c in copies(sib, i - slots_dev, i % depth):
                c.start()

    @pl.when(step == 0)
    def _():
        for i in range(depth - 1):
            fetch(jnp.int32(i))
        for q in range(n_src):
            for ref in sum_refs[q]:
                ref[...] = jnp.zeros_like(ref)
            for ref in tok_refs[q]:
                ref[pl.ds(2 * half * pitch, pitch), :] = jnp.zeros((pitch, 128), F32)

            def spread(i, carry):
                for src, start in ((has[q], 0), (hbs[q], half)):
                    v = src[pl.ds(pl.multiple_of(i * group, group), group), :].astype(F32)
                    for j, (w, k) in enumerate(split):
                        tok_refs[q][w][pl.ds((start + i * group) * pitch + k, group, stride=pitch), :] = v[:, j * 128:(j + 1) * 128]
                return carry

            lax.fori_loop(0, half // group, spread, 0)

    fetch(step + depth - 1)
    buf = step % depth
    for c in copies(own, 0, buf):
        c.wait()
    count = [c[step] for c in counts]
    most = count[0] if n_src == 1 else jnp.maximum(count[0], count[1])
    low = 0
    for rows in classes:
        @pl.when((most > low) & (most <= rows))
        def _(rows=rows):
            xs = []
            for q in range(n_src):
                def pick(i, carry):
                    for u in range(unroll):
                        r = i * unroll + u
                        spot = pl.ds(pl.multiple_of(lists[q][step, r] * pitch, pitch), pitch)
                        row = pl.ds(pl.multiple_of(r * pitch, pitch), pitch)
                        for w in range(2):
                            row_refs[q][w][row, :] = tok_refs[q][w][spot, :]
                    return carry

                lax.fori_loop(0, rows // unroll, pick, 0)
                xs.append(jnp.concatenate([row_refs[q][w][pl.ds(k, rows, stride=pitch), :].astype(BF16) for w, k in split], axis=1))
            x = xs[0] if n_src == 1 else jnp.concatenate(xs, axis=0)
            gate_proj = jnp.dot(x, wg_ref[buf], preferred_element_type=F32)
            up_proj = jnp.dot(x, wu_ref[buf], preferred_element_type=F32)
            act = (jax.nn.silu(gate_proj) * up_proj).astype(BF16)
            out = jnp.dot(act, wd_ref[buf], preferred_element_type=F32).astype(BF16).astype(F32)
            for q in range(n_src):
                for j, (w, k) in enumerate(split):
                    row_refs[q][w][pl.ds(k, rows, stride=pitch), :] = out[q * rows:(q + 1) * rows, j * 128:(j + 1) * 128]

        low = rows

    for q in range(n_src):
        def scatter(i, carry):
            spots, sums = [], []
            for u in range(unroll):
                r = i * unroll + u
                spot = pl.ds(pl.multiple_of(lists[q][step, r] * pitch, pitch), pitch)
                row = pl.ds(pl.multiple_of(r * pitch, pitch), pitch)
                g = glists[q][step, r]
                for w in range(2):
                    spots.append((w, spot))
                    sums.append(sum_refs[q][w][spot, :] + row_refs[q][w][row, :] * g)
            for (w, spot), v in zip(spots, sums):
                sum_refs[q][w][spot, :] = v
            return carry

        lax.fori_loop(0, (count[q] + unroll - 1) // unroll, scatter, 0)

    @pl.when(step == steps - 1)
    def _():
        outs = [(q, ref, start) for q in range(n_src) for ref, start in ((yas[q], 0), (ybs[q], half))]

        def put(n, ref, i):
            rows = pl.ds(pl.multiple_of(i * group, group), group)
            return pltpu.make_async_copy(stage_ref.at[i % 2, n], ref.at[rows], out_sems.at[i % 2, n])

        def unpack(i, carry):
            for n, (q, ref, start) in enumerate(outs):
                @pl.when(i >= 2)
                def _():
                    put(n, ref, i).wait()

                for j, (w, k) in enumerate(split):
                    stage_ref[i % 2, n, :, j * 128:(j + 1) * 128] = (
                        sum_refs[q][w][pl.ds((start + i * group) * pitch + k, group, stride=pitch), :])
                put(n, ref, i).start()
            return carry

        lax.fori_loop(0, half // group, unpack, 0)
        for i in range(2):
            for n, (q, ref, start) in enumerate(outs):
                put(n, ref, i).wait()


def expert_call(sources, own, sib, dep, local_max):
    n_src = len(sources)
    lists, glists, counts, has, hbs = zip(*sources)
    half, hidden = has[0].shape
    slots_dev, _, ff = own[0].shape
    depth = 4 if n_src == 1 else 2
    classes = tuple(c for c in CLASSES if c < local_max) + (local_max,)
    whole = pl.BlockSpec((half, hidden), lambda s: (0, 0), pipeline_mode=pl.Buffered(1))
    smem = pl.BlockSpec(memory_space=pltpu.SMEM)
    hbm = pl.BlockSpec(memory_space=pl.ANY)
    out = jax.ShapeDtypeStruct((half, hidden), F32)
    toks = (2 * half + 8) * 8
    got = pl.pallas_call(
        functools.partial(expert_kernel, n_src, classes, slots_dev, depth),
        grid=(2 * slots_dev,),
        out_shape=(out,) * (2 * n_src),
        in_specs=[smem] * (3 * n_src) + [whole] * (2 * n_src) + [hbm] * 7,
        out_specs=(hbm,) * (2 * n_src),
        scratch_shapes=[pltpu.VMEM((depth, hidden, ff), BF16), pltpu.VMEM((depth, hidden, ff), BF16), pltpu.VMEM((depth, ff, hidden), BF16)]
        + [pltpu.VMEM((local_max * 8, 128), F32)] * (2 * n_src) + [pltpu.VMEM((toks, 128), F32)] * (4 * n_src)
        + [pltpu.VMEM((2, 2 * n_src, 64, hidden), F32), pltpu.SemaphoreType.DMA((3, depth)), pltpu.SemaphoreType.DMA((2, 2 * n_src))],
        compiler_params=pltpu.CompilerParams(dimension_semantics=("arbitrary",), vmem_limit_bytes=63 * 1024 * 1024),
        cost_estimate=pl.CostEstimate(flops=1_000_000, transcendentals=0,
                                      bytes_accessed=2 * slots_dev * 3 * hidden * ff * 2),
        name="experts",
    )(*lists, *glists, *counts, *has, *hbs, *own, *sib, dep)
    return got[:n_src], got[n_src:]


def solution(mesh):
    group_size = mesh.shape['ep']
    cores = 2
    right = [(i, (i + cores) % group_size) for i in range(group_size)]
    left = [(i, (i - cores) % group_size) for i in range(group_size)]
    far = [(i, (i + group_size // 2) % group_size) for i in range(group_size)]
    sibling = [(i, i ^ 1) for i in range(group_size)]

    def block(hidden_in, topk_idx, norm_gain, w_router, w_sgate, s_gate, s_up, s_down, w_gate, w_up, w_down):
        tok_dev, _ = hidden_in.shape
        top_k = topk_idx.shape[1]
        experts = w_router.shape[1]
        slots_dev = w_gate.shape[0]
        half = tok_dev // 2
        capacity = (5 * tok_dev * group_size * top_k + 4 * experts - 1) // (4 * experts)
        local_max = (2 * tok_dev * top_k + experts - 1) // experts
        me = lax.axis_index('ep')

        def go_right(v):
            return lax.ppermute(v, 'ep', right)

        def go_left(v):
            return lax.ppermute(v, 'ep', left)

        chip, core = me // cores, me % cores

        def after(v, *deps):
            return lax.optimization_barrier((v,) + deps)[0]

        ha, hb = norm_call(hidden_in, norm_gain)
        ha_r1, hb_l1 = go_right(ha), go_left(hb)

        logits = jnp.concatenate([jnp.dot(h, w_router, preferred_element_type=F32) for h in (ha, hb)], axis=0)
        router_probs = jax.nn.softmax(logits, axis=-1)
        chosen = topk_idx[:, :, None] == jnp.arange(experts)[None, None, :]
        gate_vals = jnp.sum(jnp.where(chosen, router_probs[:, None, :], 0.0), axis=-1)
        own_counts = jnp.sum(chosen.astype(F32), axis=(0, 1)).reshape(1, experts)
        sib_counts = lax.ppermute(own_counts, 'ep', sibling)
        count_rows = jnp.pad(jnp.concatenate([own_counts, sib_counts], axis=0), ((0, (-2 * top_k - 2) % 8), (0, tok_dev - experts)))
        table = jnp.concatenate([topk_idx.T.astype(F32), gate_vals.T, count_rows], axis=0)
        own_w = (w_gate, w_up, w_down)
        sib_w = tuple(lax.ppermute(after(w, sib_counts), 'ep', sibling) for w in own_w)
        t_r1, t_l1 = go_right(table), go_left(table)
        t_far = lax.ppermute(table, 'ep', far)

        ha_r2, hb_l2 = go_right(ha_r1), go_left(hb_l1)
        hb_r1, ha_l1 = go_right(after(hb, ha_r1)), go_left(after(ha, hb_l1))

        steps = jnp.arange(group_size // cores)
        rel = cores * ((chip + steps) % (group_size // cores))
        ids = jnp.concatenate([jnp.stack([rel + core, rel + 1 - core], axis=1).reshape(-1), jnp.stack([chip, core])]).astype(jnp.int32)
        lists, glists, kept = route_call(ids, table, t_l1, t_far, t_r1, top_k, slots_dev, capacity, local_max)
        lists, glists = lists[:, :, 0, :], glists[:, :, 0, :]
        kept = kept[:, :, 0].astype(jnp.int32)

        def source(j, part_a, part_b):
            return lists[j], glists[j], kept[j], part_a, part_b

        (y2a,), (y2b,) = expert_call([source(2, ha_r2, hb_l2)], own_w, sib_w, ha, local_max)
        p_ra, p_lb = go_right(y2a), go_left(y2b)
        (y1a, y3a), (y1b, y3b) = expert_call([source(1, ha_l1, hb_l1), source(3, ha_r1, hb_r1)], own_w, sib_w, y2a, local_max)
        d_b, d_a = go_right(y1b), go_left(y3a)
        (y0a,), (y0b,) = expert_call([source(0, ha, hb)], own_w, sib_w, y3a, local_max)
        p_ra, p_lb = after(p_ra, y0a), after(p_lb, y0b)
        z_a, z_b = go_right(y1a + p_ra), go_left(y3b + p_lb)
        base = []
        for i, (h, y0) in enumerate(((ha, y0a), (hb, y0b))):
            shared_val = shared_expert(after(h, y0a), w_sgate, s_gate, s_up, s_down)
            base.append(hidden_in[i * half:(i + 1) * half].astype(F32) + shared_val + y0)
        return final_call(base[0] + d_a, base[1] + d_b, z_a, z_b)

    row_spec = P(('dp', 'ep'), None)
    full_spec = P(None, None)
    slot_spec = P('ep', None, None)
    in_specs = (row_spec, row_spec, P(None), full_spec, full_spec, full_spec, full_spec, full_spec,
                slot_spec, slot_spec, slot_spec)
    return jax.shard_map(block, mesh=mesh, in_specs=in_specs, out_specs=row_spec, check_vma=False)
```

```python
import functools

import jax
import jax.numpy as jnp
from jax import lax
from jax.experimental import pallas as pl
from jax.experimental.pallas import tpu as pltpu
from jax.sharding import PartitionSpec as P


F32, BF16 = jnp.float32, jnp.bfloat16
CLASSES = (64, 128, 192)
PAIRS = ((0, 0), (3, 1), (2, 2), (1, 3))


def norm_kernel(x_ref, gain_ref, ha_ref, hb_ref):
    gain = gain_ref[...].astype(F32)
    for i, out_ref in enumerate((ha_ref, hb_ref)):
        x = x_ref[i].astype(F32)
        inv_rms = lax.rsqrt(jnp.mean(x * x, axis=-1, keepdims=True) + 1e-6)
        out_ref[...] = (x * inv_rms * gain).astype(BF16)


def norm_call(hidden_in, norm_gain):
    toks, hidden = hidden_in.shape
    half, rows = toks // 2, 128
    out = jax.ShapeDtypeStruct((half, hidden), BF16)
    block = pl.BlockSpec((rows, hidden), lambda i: (i, 0))
    return pl.pallas_call(
        norm_kernel,
        grid=(half // rows,),
        out_shape=(out, out),
        in_specs=[pl.BlockSpec((2, rows, hidden), lambda i: (0, i, 0)), pl.BlockSpec((1, hidden), lambda i: (0, 0))],
        out_specs=(block, block),
        compiler_params=pltpu.CompilerParams(dimension_semantics=("arbitrary",)),
        cost_estimate=pl.CostEstimate(flops=4 * toks * hidden, transcendentals=toks, bytes_accessed=4 * toks * hidden),
        name="norm",
    )(hidden_in.reshape(2, half, hidden), norm_gain.reshape(1, hidden))


def final_kernel(base_a, base_b, za_ref, zb_ref, out_ref):
    out_ref[0] = (base_a[...] + za_ref[...]).astype(BF16)
    out_ref[1] = (base_b[...] + zb_ref[...]).astype(BF16)


def final_call(base_a, base_b, za, zb):
    half, hidden = za.shape
    rows = 128
    block = pl.BlockSpec((rows, hidden), lambda i: (i, 0))
    out = pl.pallas_call(
        final_kernel,
        grid=(half // rows,),
        out_shape=jax.ShapeDtypeStruct((2, half, hidden), BF16),
        in_specs=[block] * 4,
        out_specs=pl.BlockSpec((2, rows, hidden), lambda i: (0, i, 0)),
        compiler_params=pltpu.CompilerParams(dimension_semantics=("arbitrary",)),
        cost_estimate=pl.CostEstimate(flops=2 * half * hidden, transcendentals=0, bytes_accessed=20 * half * hidden),
        name="final",
    )(base_a, base_b, za, zb)
    return out.reshape(2 * half, hidden)


def shared_expert(normed, w_sgate, s_gate, s_up, s_down):
    shared_act = (jax.nn.silu(jnp.dot(normed, s_gate, preferred_element_type=F32))
                  * jnp.dot(normed, s_up, preferred_element_type=F32)).astype(BF16)
    shared_val = jnp.dot(shared_act, s_down, preferred_element_type=F32)
    return jax.nn.sigmoid(jnp.dot(normed, w_sgate, preferred_element_type=F32)) * shared_val


def route_kernel(geom, ids_ref, own_ref, next_ref, far_ref, prev_ref, list_ref, glist_ref, count_ref, slot_ref, gate_ref):
    top_k, slots_dev, capacity, local_max = geom
    toks = own_ref.shape[1]
    slots = 2 * slots_dev
    chip, core = ids_ref[8], ids_ref[9]

    def slot_column(like):
        order = lax.broadcasted_iota(jnp.int32, like, 0)
        mine = core * slots_dev + order
        other = (1 - core) * slots_dev + order - slots_dev
        return (chip * slots + jnp.where(order < slots_dev, mine, other)).astype(F32)

    slot_id = slot_column((slots, 1))
    lane_id = lax.broadcasted_iota(jnp.int32, (slots, 128), 1).astype(F32)
    hots, counts = [], []
    for j, ref in enumerate((own_ref, next_ref, far_ref, prev_ref)):
        table = ref[...]
        hot = jnp.zeros((slots, toks), F32)
        gate = jnp.zeros((slots, toks), F32)
        for k in range(top_k):
            hit = table[k:k + 1, :] == slot_id
            hot = hot + jnp.where(hit, 1.0, 0.0)
            gate = gate + jnp.where(hit, table[top_k + k:top_k + k + 1, :], 0.0)
        for i in range(2):
            row = table[2 * top_k + i:2 * top_k + i + 1, :128]
            counts.append(jnp.sum(jnp.where(lane_id == slot_id, row, 0.0), axis=1, keepdims=True))
        hots.append(hot)
        gate_ref[j] = gate
    hot_all = jnp.concatenate(hots, axis=0)
    hot_bf = hot_all.astype(BF16)
    tile, half = 256, toks // 2

    def before(c):
        rows = lax.broadcasted_iota(jnp.int32, (toks, tile), 0)
        cols = lax.broadcasted_iota(jnp.int32, (toks, tile), 1) + c * tile
        return jnp.where(rows < cols, 1.0, 0.0).astype(BF16)

    lowers = []
    for j in range(4):
        lower = jnp.zeros((slots, 1), F32)
        for q in range(8):
            lower = lower + counts[q] * (ids_ref[q] < ids_ref[2 * j]).astype(F32)
        lowers.append(lower)
    for c in range(toks // tile):
        pos = jnp.dot(hot_bf, before(c), preferred_element_type=F32)
        for j in range(4):
            part = pos[j * slots:(j + 1) * slots]
            kept = (hot_all[j * slots:(j + 1) * slots, c * tile:(c + 1) * tile] > 0.0) & (part + lowers[j] < capacity)
            slot_ref[j, :, c * tile:(c + 1) * tile] = jnp.where(kept, 1.0, 0.0)
    joined = []
    gates = [gate_ref[j] for j in range(4)]
    for v, (ja, jb) in enumerate(PAIRS):
        joined.append(jnp.concatenate([slot_ref[ja][:, :half], slot_ref[jb][:, half:]], axis=1))
        gate_ref[v] = jnp.concatenate([gates[ja][:, :half], gates[jb][:, half:]], axis=1)
        count_ref[v] = jnp.broadcast_to(jnp.sum(joined[v], axis=1, keepdims=True), (slots, 128))
    kept_all = jnp.concatenate(joined, axis=0)
    kept_bf = kept_all.astype(BF16)
    for c in range(toks // tile):
        pos = jnp.dot(kept_bf, before(c), preferred_element_type=F32)
        for v in range(4):
            kept = kept_all[v * slots:(v + 1) * slots, c * tile:(c + 1) * tile] > 0.0
            slot_ref[v, :, c * tile:(c + 1) * tile] = jnp.where(kept, pos[v * slots:(v + 1) * slots], -1.0)
    token = lax.broadcasted_iota(jnp.int32, (8, toks), 1)
    row8 = lax.broadcasted_iota(jnp.int32, (8, toks), 0)
    digits = jnp.where(row8 == 0, token // 32, token % 32).astype(F32)
    row_of = lax.broadcasted_iota(jnp.int32, (slots, toks), 0)
    count_row = lax.broadcasted_iota(jnp.int32, (slots, 128), 0)

    def lists(e, carry):
        for j in range(4):
            pos = jnp.sum(jnp.where(row_of == e, slot_ref[j], 0.0), axis=0, keepdims=True)
            gate = jnp.sum(jnp.where(row_of == e, gate_ref[j], 0.0), axis=0, keepdims=True)
            g1 = gate.astype(BF16).astype(F32)
            g2 = (gate - g1).astype(BF16).astype(F32)
            g3 = gate - g1 - g2
            left = jnp.where(row8 < 2, digits, jnp.where(row8 == 2, g1, jnp.where(row8 == 3, g2, g3))).astype(BF16)
            width = local_max if PAIRS[j][0] == PAIRS[j][1] else 2 * local_max
            want = lax.broadcasted_iota(jnp.int32, (width, toks), 0).astype(F32)
            pick = jnp.where(want == pos, 1.0, 0.0).astype(BF16)
            got = lax.dot_general(left, pick, (((1,), (1,)), ((), ())), preferred_element_type=F32)
            found = 32.0 * got[0:1] + got[1:2]
            held = jnp.sum(jnp.where(count_row == e, count_ref[j], 0.0), axis=0, keepdims=True)[:, 0:1]
            lane = lax.broadcasted_iota(jnp.int32, (1, width), 1).astype(F32)
            found = jnp.where(lane < held, found, float(toks)).astype(jnp.int32)
            list_ref[j, e, :, :width] = jnp.broadcast_to(found, (8, width))
            glist_ref[j, e, :, :width] = jnp.broadcast_to((got[2:3] + got[3:4]) + got[4:5], (8, width))
        return carry

    lax.fori_loop(0, slots, lists, 0)


def route_call(ids, own, nxt, far, prv, top_k, slots_dev, capacity, local_max):
    toks = own.shape[1]
    slots = 2 * slots_dev
    vmem = pl.BlockSpec(memory_space=pltpu.VMEM)
    return pl.pallas_call(
        functools.partial(route_kernel, (top_k, slots_dev, capacity, local_max)),
        out_shape=(jax.ShapeDtypeStruct((4, slots, 8, 2 * local_max), jnp.int32), jax.ShapeDtypeStruct((4, slots, 8, 2 * local_max), F32),
                   jax.ShapeDtypeStruct((4, slots, 128), F32)),
        in_specs=[pl.BlockSpec(memory_space=pltpu.SMEM)] + [vmem] * 4,
        out_specs=(vmem,) * 3,
        scratch_shapes=[pltpu.VMEM((4, slots, toks), F32), pltpu.VMEM((4, slots, toks), F32)],
        cost_estimate=pl.CostEstimate(flops=1_000_000, transcendentals=0, bytes_accessed=2_000_000),
        name="route",
    )(ids, own, nxt, far, prv)


def expert_kernel(pieces, classes, slots_dev, depth, *refs):
    refs = list(refs)
    n_src = 1

    def take(n):
        got = refs[:n]
        del refs[:n]
        return got

    lists, glists, counts = take(n_src), take(n_src), take(n_src)
    has, hbs = take(n_src), take(n_src)
    own, sib = take(3), take(3)
    take(1)
    ys = take(pieces)
    wg_ref, wu_ref, wd_ref = take(3)
    row_refs, tok_refs, sum_refs = [take(2) for _ in range(n_src)], [take(2) for _ in range(n_src)], [take(2) for _ in range(n_src)]
    stage_ref, sems, out_sems = take(3)
    step = pl.program_id(0)
    steps = 2 * slots_dev
    half, hidden = has[0].shape
    blocks = hidden // 128
    pitch, unroll, group = 8, 8, 64
    split = [(j // pitch, j % pitch) for j in range(blocks)]

    def copies(srcs, i, b):
        return [pltpu.make_async_copy(src.at[i], dst.at[b], sems.at[n, b])
                for n, (src, dst) in enumerate(zip(srcs, (wg_ref, wu_ref, wd_ref)))]

    def fetch(i):
        @pl.when(i < slots_dev)
        def _():
            for c in copies(own, i, i % depth):
                c.start()

        @pl.when((i >= slots_dev) & (i < steps))
        def _():
            for c in copies(sib, i - slots_dev, i % depth):
                c.start()

    @pl.when(step == 0)
    def _():
        for i in range(depth - 1):
            fetch(jnp.int32(i))
        for q in range(n_src):
            for ref in sum_refs[q]:
                ref[...] = jnp.zeros_like(ref)
            for ref in tok_refs[q]:
                ref[pl.ds(2 * half * pitch, pitch), :] = jnp.zeros((pitch, 128), F32)

            def spread(i, carry):
                for src, start in ((has[q], 0), (hbs[q], half)):
                    v = src[pl.ds(pl.multiple_of(i * group, group), group), :].astype(F32)
                    for j, (w, k) in enumerate(split):
                        tok_refs[q][w][pl.ds((start + i * group) * pitch + k, group, stride=pitch), :] = v[:, j * 128:(j + 1) * 128]
                return carry

            lax.fori_loop(0, half // group, spread, 0)

    fetch(step + depth - 1)
    buf = step % depth
    for c in copies(own, 0, buf):
        c.wait()
    count = [c[step] for c in counts]
    most = count[0] if n_src == 1 else jnp.maximum(count[0], count[1])
    low = 0
    for rows in classes:
        @pl.when((most > low) & (most <= rows))
        def _(rows=rows):
            xs = []
            for q in range(n_src):
                def pick(i, carry):
                    for u in range(unroll):
                        r = i * unroll + u
                        spot = pl.ds(pl.multiple_of(lists[q][step, r] * pitch, pitch), pitch)
                        row = pl.ds(pl.multiple_of(r * pitch, pitch), pitch)
                        for w in range(2):
                            row_refs[q][w][row, :] = tok_refs[q][w][spot, :]
                    return carry

                lax.fori_loop(0, rows // unroll, pick, 0)
                xs.append(jnp.concatenate([row_refs[q][w][pl.ds(k, rows, stride=pitch), :].astype(BF16) for w, k in split], axis=1))
            x = xs[0] if n_src == 1 else jnp.concatenate(xs, axis=0)
            gate_proj = jnp.dot(x, wg_ref[buf], preferred_element_type=F32)
            up_proj = jnp.dot(x, wu_ref[buf], preferred_element_type=F32)
            act = (jax.nn.silu(gate_proj) * up_proj).astype(BF16)
            out = jnp.dot(act, wd_ref[buf], preferred_element_type=F32).astype(BF16).astype(F32)
            for q in range(n_src):
                for j, (w, k) in enumerate(split):
                    row_refs[q][w][pl.ds(k, rows, stride=pitch), :] = out[q * rows:(q + 1) * rows, j * 128:(j + 1) * 128]

        low = rows

    for q in range(n_src):
        def scatter(i, carry):
            spots, sums = [], []
            for u in range(unroll):
                r = i * unroll + u
                spot = pl.ds(pl.multiple_of(lists[q][step, r] * pitch, pitch), pitch)
                row = pl.ds(pl.multiple_of(r * pitch, pitch), pitch)
                g = glists[q][step, r]
                for w in range(2):
                    spots.append((w, spot))
                    sums.append(sum_refs[q][w][spot, :] + row_refs[q][w][row, :] * g)
            for (w, spot), v in zip(spots, sums):
                sum_refs[q][w][spot, :] = v
            return carry

        lax.fori_loop(0, (count[q] + unroll - 1) // unroll, scatter, 0)

    @pl.when(step == steps - 1)
    def _():
        size = 2 * half // pieces
        outs = [(0, ref, n * size) for n, ref in enumerate(ys)]

        def put(n, ref, i):
            rows = pl.ds(pl.multiple_of(i * group, group), group)
            return pltpu.make_async_copy(stage_ref.at[i % 2, n], ref.at[rows], out_sems.at[i % 2, n])

        def unpack(i, carry):
            for n, (q, ref, start) in enumerate(outs):
                @pl.when(i >= 2)
                def _():
                    put(n, ref, i).wait()

                for j, (w, k) in enumerate(split):
                    stage_ref[i % 2, n, :, j * 128:(j + 1) * 128] = (
                        sum_refs[q][w][pl.ds((start + i * group) * pitch + k, group, stride=pitch), :])
                put(n, ref, i).start()
            return carry

        lax.fori_loop(0, size // group, unpack, 0)
        for i in range(2):
            for n, (q, ref, start) in enumerate(outs):
                put(n, ref, i).wait()


def expert_call(routes, ha, hb, own, sib, dep, row_max, pieces):
    half, hidden = ha.shape
    slots_dev, _, ff = own[0].shape
    depth = 4
    classes = tuple(c for c in CLASSES if c < row_max) + (row_max,)
    whole = pl.BlockSpec((half, hidden), lambda s: (0, 0), pipeline_mode=pl.Buffered(1))
    smem = pl.BlockSpec(memory_space=pltpu.SMEM)
    hbm = pl.BlockSpec(memory_space=pl.ANY)
    out = jax.ShapeDtypeStruct((2 * half // pieces, hidden), F32)
    toks = (2 * half + 8) * 8
    return pl.pallas_call(
        functools.partial(expert_kernel, pieces, classes, slots_dev, depth),
        grid=(2 * slots_dev,),
        out_shape=(out,) * pieces,
        in_specs=[smem] * 3 + [whole] * 2 + [hbm] * 7,
        out_specs=(hbm,) * pieces,
        scratch_shapes=[pltpu.VMEM((depth, hidden, ff), BF16), pltpu.VMEM((depth, hidden, ff), BF16), pltpu.VMEM((depth, ff, hidden), BF16)]
        + [pltpu.VMEM((row_max * 8, 128), F32)] * 2 + [pltpu.VMEM((toks, 128), F32)] * 4
        + [pltpu.VMEM((2, pieces, 64, hidden), F32), pltpu.SemaphoreType.DMA((3, depth)), pltpu.SemaphoreType.DMA((2, pieces))],
        compiler_params=pltpu.CompilerParams(dimension_semantics=("arbitrary",), vmem_limit_bytes=62 * 1024 * 1024),
        cost_estimate=pl.CostEstimate(flops=1_000_000, transcendentals=0,
                                      bytes_accessed=2 * slots_dev * 3 * hidden * ff * 2),
        name="experts",
    )(*routes, ha, hb, *own, *sib, dep)


def solution(mesh):
    group_size = mesh.shape['ep']
    cores = 2
    right = [(i, (i + cores) % group_size) for i in range(group_size)]
    left = [(i, (i - cores) % group_size) for i in range(group_size)]
    far = [(i, (i + group_size // 2) % group_size) for i in range(group_size)]
    sibling = [(i, i ^ 1) for i in range(group_size)]

    def block(hidden_in, topk_idx, norm_gain, w_router, w_sgate, s_gate, s_up, s_down, w_gate, w_up, w_down):
        tok_dev, _ = hidden_in.shape
        top_k = topk_idx.shape[1]
        experts = w_router.shape[1]
        slots_dev = w_gate.shape[0]
        half = tok_dev // 2
        capacity = (5 * tok_dev * group_size * top_k + 4 * experts - 1) // (4 * experts)
        local_max = (2 * tok_dev * top_k + experts - 1) // experts
        me = lax.axis_index('ep')

        def go_right(v):
            return lax.ppermute(v, 'ep', right)

        def go_left(v):
            return lax.ppermute(v, 'ep', left)

        chip, core = me // cores, me % cores

        def after(v, *deps):
            return lax.optimization_barrier((v,) + deps)[0]

        ha, hb = norm_call(hidden_in, norm_gain)
        ha_r1, hb_l1 = go_right(ha), go_left(hb)

        logits = jnp.concatenate([jnp.dot(h, w_router, preferred_element_type=F32) for h in (ha, hb)], axis=0)
        router_probs = jax.nn.softmax(logits, axis=-1)
        chosen = topk_idx[:, :, None] == jnp.arange(experts)[None, None, :]
        gate_vals = jnp.sum(jnp.where(chosen, router_probs[:, None, :], 0.0), axis=-1)
        own_counts = jnp.sum(chosen.astype(F32), axis=(0, 1)).reshape(1, experts)
        sib_counts = lax.ppermute(own_counts, 'ep', sibling)
        count_rows = jnp.pad(jnp.concatenate([own_counts, sib_counts], axis=0), ((0, (-2 * top_k - 2) % 8), (0, tok_dev - experts)))
        table = jnp.concatenate([topk_idx.T.astype(F32), gate_vals.T, count_rows], axis=0)
        own_w = (w_gate, w_up, w_down)
        sib_w = tuple(lax.ppermute(after(w, sib_counts), 'ep', sibling) for w in own_w)
        t_r1, t_l1 = go_right(table), go_left(table)
        t_far = lax.ppermute(table, 'ep', far)

        ha_r2, hb_l2 = go_right(ha_r1), go_left(hb_l1)
        hb_r1, ha_l1 = go_right(after(hb, ha_r1)), go_left(after(ha, hb_l1))

        steps = jnp.arange(group_size // cores)
        rel = cores * ((chip + steps) % (group_size // cores))
        ids = jnp.concatenate([jnp.stack([rel + core, rel + 1 - core], axis=1).reshape(-1), jnp.stack([chip, core])]).astype(jnp.int32)
        lists, glists, kept = route_call(ids, table, t_l1, t_far, t_r1, top_k, slots_dev, capacity, local_max)
        lists, glists = lists[:, :, 0, :], glists[:, :, 0, :]
        kept = kept[:, :, 0].astype(jnp.int32)

        def routes(v, row_max):
            return lists[v, :, :row_max], glists[v, :, :row_max], kept[v]

        d_a0, d_a1, d_b0, d_b1 = expert_call(routes(1, 2 * local_max), ha_r1, hb_l1, own_w, sib_w, ha, 2 * local_max, 4)
        d_a0, d_b0 = go_left(d_a0), go_right(d_b0)
        y2a, y2b = expert_call(routes(2, local_max), ha_r2, hb_l2, own_w, sib_w, d_a1, local_max, 2)
        p_ra, p_lb = go_right(y2a), go_left(y2b)
        d_a1, d_b1 = go_left(d_a1), go_right(d_b1)
        y1a, y3b = expert_call(routes(3, 2 * local_max), ha_l1, hb_r1, own_w, sib_w, y2a, 2 * local_max, 2)
        y0a, y0b = expert_call(routes(0, local_max), ha, hb, own_w, sib_w, y3b, local_max, 2)
        p_ra, p_lb = after(p_ra, y0a), after(p_lb, y0b)
        z_a, z_b = go_right(y1a + p_ra), go_left(y3b + p_lb)
        base = []
        for i, (h, y0) in enumerate(((ha, y0a), (hb, y0b))):
            shared_val = shared_expert(after(h, y0a), w_sgate, s_gate, s_up, s_down)
            base.append(hidden_in[i * half:(i + 1) * half].astype(F32) + shared_val + y0)
        d_a, d_b = jnp.concatenate([d_a0, d_a1], axis=0), jnp.concatenate([d_b0, d_b1], axis=0)
        return final_call(base[0] + d_a, base[1] + d_b, z_a, z_b)

    row_spec = P(('dp', 'ep'), None)
    full_spec = P(None, None)
    slot_spec = P('ep', None, None)
    in_specs = (row_spec, row_spec, P(None), full_spec, full_spec, full_spec, full_spec, full_spec,
                slot_spec, slot_spec, slot_spec)
    return jax.shard_map(block, mesh=mesh, in_specs=in_specs, out_specs=row_spec, check_vma=False)
```

```python
import functools

import jax
import jax.numpy as jnp
from jax import lax
from jax.experimental import pallas as pl
from jax.experimental.pallas import tpu as pltpu
from jax.sharding import PartitionSpec as P


F32, BF16 = jnp.float32, jnp.bfloat16
CLASSES = (64, 128, 192)
PAIRS = ((0, 0), (3, 1), (2, 2), (1, 3))


def norm_kernel(x_ref, gain_ref, ha_ref, hb_ref):
    gain = gain_ref[...].astype(F32)[None, :]
    for i, out_ref in enumerate((ha_ref, hb_ref)):
        x = x_ref[i].astype(F32)
        inv_rms = lax.rsqrt(jnp.mean(x * x, axis=-1, keepdims=True) + 1e-6)
        out_ref[...] = (x * inv_rms * gain).astype(BF16)


def norm_call(hidden_in, norm_gain):
    toks, hidden = hidden_in.shape
    half, rows = toks // 2, 128
    out = jax.ShapeDtypeStruct((half, hidden), BF16)
    block = pl.BlockSpec((rows, hidden), lambda i: (i, 0))
    return pl.pallas_call(
        norm_kernel,
        grid=(half // rows,),
        out_shape=(out, out),
        in_specs=[pl.BlockSpec((2, rows, hidden), lambda i: (0, i, 0)), pl.BlockSpec((hidden,), lambda i: (0,))],
        out_specs=(block, block),
        compiler_params=pltpu.CompilerParams(dimension_semantics=("arbitrary",)),
        cost_estimate=pl.CostEstimate(flops=4 * toks * hidden, transcendentals=toks, bytes_accessed=4 * toks * hidden),
        name="norm",
    )(hidden_in.reshape(2, half, hidden), norm_gain)


def final_kernel(base_a, base_b, za_ref, zb_ref, *rest):
    out_ref = rest[-1]
    out_ref[0] = (base_a[...] + za_ref[...]).astype(BF16)
    out_ref[1] = (base_b[...] + zb_ref[...]).astype(BF16)


def final_call(part, base_a, base_b, za, zb, so_far):
    size, hidden = za.shape
    rows = 64
    first = part * (size // rows)
    block = pl.BlockSpec((rows, hidden), lambda i: (i, 0))
    base = pl.BlockSpec((rows, hidden), lambda i: (i + first, 0))
    more = [] if so_far is None else [so_far]
    return pl.pallas_call(
        final_kernel,
        grid=(size // rows,),
        out_shape=jax.ShapeDtypeStruct((2, 2 * size, hidden), BF16),
        in_specs=[base] * 2 + [block] * 2 + [pl.BlockSpec(memory_space=pl.ANY)] * len(more),
        out_specs=pl.BlockSpec((2, rows, hidden), lambda i: (0, i + first, 0)),
        input_output_aliases={4: 0} if more else {},
        compiler_params=pltpu.CompilerParams(dimension_semantics=("arbitrary",)),
        cost_estimate=pl.CostEstimate(flops=4 * size * hidden, transcendentals=0, bytes_accessed=20 * size * hidden),
        name="final",
    )(base_a, base_b, za, zb, *more)


def shared_expert(normed, w_sgate, s_gate, s_up, s_down):
    shared_act = (jax.nn.silu(jnp.dot(normed, s_gate, preferred_element_type=F32))
                  * jnp.dot(normed, s_up, preferred_element_type=F32)).astype(BF16)
    shared_val = jnp.dot(shared_act, s_down, preferred_element_type=F32)
    return jax.nn.sigmoid(jnp.dot(normed, w_sgate, preferred_element_type=F32)) * shared_val


def route_kernel(geom, ids_ref, own_ref, next_ref, far_ref, prev_ref, list_ref, glist_ref, count_ref, slot_ref, gate_ref):
    top_k, slots_dev, capacity, local_max = geom
    toks = own_ref.shape[1]
    slots = 2 * slots_dev
    chip, core = ids_ref[8], ids_ref[9]

    def slot_column(like):
        order = lax.broadcasted_iota(jnp.int32, like, 0)
        mine = core * slots_dev + order
        other = (1 - core) * slots_dev + order - slots_dev
        return (chip * slots + jnp.where(order < slots_dev, mine, other)).astype(F32)

    slot_id = slot_column((slots, 1))
    lane_id = lax.broadcasted_iota(jnp.int32, (slots, 128), 1).astype(F32)
    hots, counts = [], []
    for j, ref in enumerate((own_ref, next_ref, far_ref, prev_ref)):
        table = ref[...]
        hot = jnp.zeros((slots, toks), F32)
        gate = jnp.zeros((slots, toks), F32)
        for k in range(top_k):
            hit = table[k:k + 1, :] == slot_id
            hot = hot + jnp.where(hit, 1.0, 0.0)
            gate = gate + jnp.where(hit, table[top_k + k:top_k + k + 1, :], 0.0)
        for i in range(2):
            row = table[2 * top_k + i:2 * top_k + i + 1, :128]
            counts.append(jnp.sum(jnp.where(lane_id == slot_id, row, 0.0), axis=1, keepdims=True))
        hots.append(hot)
        gate_ref[j] = gate
    hot_all = jnp.concatenate(hots, axis=0)
    hot_bf = hot_all.astype(BF16)
    tile, half = 256, toks // 2

    def before(c):
        rows = lax.broadcasted_iota(jnp.int32, (toks, tile), 0)
        cols = lax.broadcasted_iota(jnp.int32, (toks, tile), 1) + c * tile
        return jnp.where(rows < cols, 1.0, 0.0).astype(BF16)

    lowers = []
    for j in range(4):
        lower = jnp.zeros((slots, 1), F32)
        for q in range(8):
            lower = lower + counts[q] * (ids_ref[q] < ids_ref[2 * j]).astype(F32)
        lowers.append(lower)
    for c in range(toks // tile):
        pos = jnp.dot(hot_bf, before(c), preferred_element_type=F32)
        for j in range(4):
            part = pos[j * slots:(j + 1) * slots]
            kept = (hot_all[j * slots:(j + 1) * slots, c * tile:(c + 1) * tile] > 0.0) & (part + lowers[j] < capacity)
            slot_ref[j, :, c * tile:(c + 1) * tile] = jnp.where(kept, 1.0, 0.0)
    joined = []
    gates = [gate_ref[j] for j in range(4)]
    for v, (ja, jb) in enumerate(PAIRS):
        joined.append(jnp.concatenate([slot_ref[ja][:, :half], slot_ref[jb][:, half:]], axis=1))
        gate_ref[v] = jnp.concatenate([gates[ja][:, :half], gates[jb][:, half:]], axis=1)
        count_ref[v] = jnp.broadcast_to(jnp.sum(joined[v], axis=1, keepdims=True), (slots, 128))
    kept_all = jnp.concatenate(joined, axis=0)
    kept_bf = kept_all.astype(BF16)
    for c in range(toks // tile):
        pos = jnp.dot(kept_bf, before(c), preferred_element_type=F32)
        for v in range(4):
            kept = kept_all[v * slots:(v + 1) * slots, c * tile:(c + 1) * tile] > 0.0
            slot_ref[v, :, c * tile:(c + 1) * tile] = jnp.where(kept, pos[v * slots:(v + 1) * slots], -1.0)
    token = lax.broadcasted_iota(jnp.int32, (8, toks), 1)
    row8 = lax.broadcasted_iota(jnp.int32, (8, toks), 0)
    digits = jnp.where(row8 == 0, token // 32, token % 32).astype(F32)
    row_of = lax.broadcasted_iota(jnp.int32, (slots, toks), 0)
    count_row = lax.broadcasted_iota(jnp.int32, (slots, 128), 0)

    def lists(e, carry):
        for j in range(4):
            pos = jnp.sum(jnp.where(row_of == e, slot_ref[j], 0.0), axis=0, keepdims=True)
            gate = jnp.sum(jnp.where(row_of == e, gate_ref[j], 0.0), axis=0, keepdims=True)
            g1 = gate.astype(BF16).astype(F32)
            g2 = (gate - g1).astype(BF16).astype(F32)
            g3 = gate - g1 - g2
            left = jnp.where(row8 < 2, digits, jnp.where(row8 == 2, g1, jnp.where(row8 == 3, g2, g3))).astype(BF16)
            width = local_max if PAIRS[j][0] == PAIRS[j][1] else 2 * local_max
            want = lax.broadcasted_iota(jnp.int32, (width, toks), 0).astype(F32)
            pick = jnp.where(want == pos, 1.0, 0.0).astype(BF16)
            got = lax.dot_general(left, pick, (((1,), (1,)), ((), ())), preferred_element_type=F32)
            found = 32.0 * got[0:1] + got[1:2]
            held = jnp.sum(jnp.where(count_row == e, count_ref[j], 0.0), axis=0, keepdims=True)[:, 0:1]
            lane = lax.broadcasted_iota(jnp.int32, (1, width), 1).astype(F32)
            found = jnp.where(lane < held, found, float(toks)).astype(jnp.int32)
            list_ref[j, e, :, :width] = jnp.broadcast_to(found, (8, width))
            glist_ref[j, e, :, :width] = jnp.broadcast_to((got[2:3] + got[3:4]) + got[4:5], (8, width))
        return carry

    lax.fori_loop(0, slots, lists, 0)


def route_call(ids, own, nxt, far, prv, top_k, slots_dev, capacity, local_max):
    toks = own.shape[1]
    slots = 2 * slots_dev
    vmem = pl.BlockSpec(memory_space=pltpu.VMEM)
    return pl.pallas_call(
        functools.partial(route_kernel, (top_k, slots_dev, capacity, local_max)),
        out_shape=(jax.ShapeDtypeStruct((4, slots, 8, 2 * local_max), jnp.int32), jax.ShapeDtypeStruct((4, slots, 8, 2 * local_max), F32),
                   jax.ShapeDtypeStruct((4, slots, 128), F32)),
        in_specs=[pl.BlockSpec(memory_space=pltpu.SMEM)] + [vmem] * 4,
        out_specs=(vmem,) * 3,
        scratch_shapes=[pltpu.VMEM((4, slots, toks), F32), pltpu.VMEM((4, slots, toks), F32)],
        cost_estimate=pl.CostEstimate(flops=1_000_000, transcendentals=0, bytes_accessed=2_000_000),
        name="route",
    )(ids, own, nxt, far, prv)


def expert_kernel(pieces, classes, slots_dev, depth, *refs):
    refs = list(refs)
    n_src = 1

    def take(n):
        got = refs[:n]
        del refs[:n]
        return got

    lists, glists, counts = take(n_src), take(n_src), take(n_src)
    has, hbs = take(n_src), take(n_src)
    own, sib = take(3), take(3)
    take(1)
    ys = take(pieces)
    wg_ref, wu_ref, wd_ref = take(3)
    row_refs, tok_refs, sum_refs = [take(2) for _ in range(n_src)], [take(2) for _ in range(n_src)], [take(2) for _ in range(n_src)]
    stage_ref, sems, out_sems = take(3)
    step = pl.program_id(0)
    steps = 2 * slots_dev
    half, hidden = has[0].shape
    blocks = hidden // 128
    pitch, unroll, group = 8, 8, 64
    split = [(j // pitch, j % pitch) for j in range(blocks)]

    def copies(srcs, i, b):
        return [pltpu.make_async_copy(src.at[i], dst.at[b], sems.at[n, b])
                for n, (src, dst) in enumerate(zip(srcs, (wg_ref, wu_ref, wd_ref)))]

    def fetch(i):
        @pl.when(i < slots_dev)
        def _():
            for c in copies(own, i, i % depth):
                c.start()

        @pl.when((i >= slots_dev) & (i < steps))
        def _():
            for c in copies(sib, i - slots_dev, i % depth):
                c.start()

    @pl.when(step == 0)
    def _():
        for i in range(depth - 1):
            fetch(jnp.int32(i))
        for q in range(n_src):
            for ref in sum_refs[q]:
                ref[...] = jnp.zeros_like(ref)
            for ref in tok_refs[q]:
                ref[pl.ds(2 * half * pitch, pitch), :] = jnp.zeros((pitch, 128), F32)

            def spread(i, carry):
                for src, start in ((has[q], 0), (hbs[q], half)):
                    v = src[pl.ds(pl.multiple_of(i * group, group), group), :].astype(F32)
                    for j, (w, k) in enumerate(split):
                        tok_refs[q][w][pl.ds((start + i * group) * pitch + k, group, stride=pitch), :] = v[:, j * 128:(j + 1) * 128]
                return carry

            lax.fori_loop(0, half // group, spread, 0)

    fetch(step + depth - 1)
    buf = step % depth
    for c in copies(own, 0, buf):
        c.wait()
    count = [c[step] for c in counts]
    most = count[0] if n_src == 1 else jnp.maximum(count[0], count[1])
    low = 0
    for rows in classes:
        @pl.when((most > low) & (most <= rows))
        def _(rows=rows):
            xs = []
            for q in range(n_src):
                def pick(i, carry):
                    for u in range(unroll):
                        r = i * unroll + u
                        spot = pl.ds(pl.multiple_of(lists[q][step, r] * pitch, pitch), pitch)
                        row = pl.ds(pl.multiple_of(r * pitch, pitch), pitch)
                        for w in range(2):
                            row_refs[q][w][row, :] = tok_refs[q][w][spot, :]
                    return carry

                lax.fori_loop(0, rows // unroll, pick, 0)
                xs.append(jnp.concatenate([row_refs[q][w][pl.ds(k, rows, stride=pitch), :].astype(BF16) for w, k in split], axis=1))
            x = xs[0] if n_src == 1 else jnp.concatenate(xs, axis=0)
            gate_proj = jnp.dot(x, wg_ref[buf], preferred_element_type=F32)
            up_proj = jnp.dot(x, wu_ref[buf], preferred_element_type=F32)
            act = (jax.nn.silu(gate_proj) * up_proj).astype(BF16)
            out = jnp.dot(act, wd_ref[buf], preferred_element_type=F32).astype(BF16).astype(F32)
            for q in range(n_src):
                for j, (w, k) in enumerate(split):
                    row_refs[q][w][pl.ds(k, rows, stride=pitch), :] = out[q * rows:(q + 1) * rows, j * 128:(j + 1) * 128]

        low = rows

    for q in range(n_src):
        def scatter(i, carry):
            spots, sums = [], []
            for u in range(unroll):
                r = i * unroll + u
                spot = pl.ds(pl.multiple_of(lists[q][step, r] * pitch, pitch), pitch)
                row = pl.ds(pl.multiple_of(r * pitch, pitch), pitch)
                g = glists[q][step, r]
                for w in range(2):
                    spots.append((w, spot))
                    sums.append(sum_refs[q][w][spot, :] + row_refs[q][w][row, :] * g)
            for (w, spot), v in zip(spots, sums):
                sum_refs[q][w][spot, :] = v
            return carry

        lax.fori_loop(0, (count[q] + unroll - 1) // unroll, scatter, 0)

    @pl.when(step == steps - 1)
    def _():
        size = 2 * half // pieces
        outs = [(0, ref, n * size) for n, ref in enumerate(ys)]

        def put(n, ref, i):
            rows = pl.ds(pl.multiple_of(i * group, group), group)
            return pltpu.make_async_copy(stage_ref.at[i % 2, n], ref.at[rows], out_sems.at[i % 2, n])

        def unpack(i, carry):
            for n, (q, ref, start) in enumerate(outs):
                @pl.when(i >= 2)
                def _():
                    put(n, ref, i).wait()

                for j, (w, k) in enumerate(split):
                    stage_ref[i % 2, n, :, j * 128:(j + 1) * 128] = (
                        sum_refs[q][w][pl.ds((start + i * group) * pitch + k, group, stride=pitch), :])
                put(n, ref, i).start()
            return carry

        lax.fori_loop(0, size // group, unpack, 0)
        for i in range(2):
            for n, (q, ref, start) in enumerate(outs):
                put(n, ref, i).wait()


def expert_call(routes, ha, hb, own, sib, dep, row_max, pieces):
    half, hidden = ha.shape
    slots_dev, _, ff = own[0].shape
    depth = 4
    classes = tuple(c for c in CLASSES if c < row_max) + (row_max,)
    whole = pl.BlockSpec((half, hidden), lambda s: (0, 0), pipeline_mode=pl.Buffered(1))
    smem = pl.BlockSpec(memory_space=pltpu.SMEM)
    hbm = pl.BlockSpec(memory_space=pl.ANY)
    out = jax.ShapeDtypeStruct((2 * half // pieces, hidden), F32)
    toks = (2 * half + 8) * 8
    return pl.pallas_call(
        functools.partial(expert_kernel, pieces, classes, slots_dev, depth),
        grid=(2 * slots_dev,),
        out_shape=(out,) * pieces,
        in_specs=[smem] * 3 + [whole] * 2 + [hbm] * 7,
        out_specs=(hbm,) * pieces,
        scratch_shapes=[pltpu.VMEM((depth, hidden, ff), BF16), pltpu.VMEM((depth, hidden, ff), BF16), pltpu.VMEM((depth, ff, hidden), BF16)]
        + [pltpu.VMEM((row_max * 8, 128), F32)] * 2 + [pltpu.VMEM((toks, 128), F32)] * 4
        + [pltpu.VMEM((2, pieces, 64, hidden), F32), pltpu.SemaphoreType.DMA((3, depth)), pltpu.SemaphoreType.DMA((2, pieces))],
        compiler_params=pltpu.CompilerParams(dimension_semantics=("arbitrary",), vmem_limit_bytes=62 * 1024 * 1024),
        cost_estimate=pl.CostEstimate(flops=1_000_000, transcendentals=0,
                                      bytes_accessed=2 * slots_dev * 3 * hidden * ff * 2),
        name="experts",
    )(*routes, ha, hb, *own, *sib, dep)


def solution(mesh):
    group_size = mesh.shape['ep']
    cores = 2
    right = [(i, (i + cores) % group_size) for i in range(group_size)]
    left = [(i, (i - cores) % group_size) for i in range(group_size)]
    far = [(i, (i + group_size // 2) % group_size) for i in range(group_size)]
    sibling = [(i, i ^ 1) for i in range(group_size)]

    def block(hidden_in, topk_idx, norm_gain, w_router, w_sgate, s_gate, s_up, s_down, w_gate, w_up, w_down):
        tok_dev, hidden = hidden_in.shape
        top_k = topk_idx.shape[1]
        experts = w_router.shape[1]
        slots_dev = w_gate.shape[0]
        half = tok_dev // 2
        capacity = (5 * tok_dev * group_size * top_k + 4 * experts - 1) // (4 * experts)
        local_max = (2 * tok_dev * top_k + experts - 1) // experts
        me = lax.axis_index('ep')

        def go_right(v):
            return lax.ppermute(v, 'ep', right)

        def go_left(v):
            return lax.ppermute(v, 'ep', left)

        chip, core = me // cores, me % cores

        def after(v, *deps):
            return lax.optimization_barrier((v,) + deps)[0]

        ha, hb = norm_call(hidden_in, norm_gain)
        ha_r1, hb_l1 = go_right(ha), go_left(hb)

        logits = jnp.concatenate([jnp.dot(h, w_router, preferred_element_type=F32) for h in (ha, hb)], axis=0)
        router_probs = jax.nn.softmax(logits, axis=-1)
        chosen = topk_idx[:, :, None] == jnp.arange(experts)[None, None, :]
        gate_vals = jnp.sum(jnp.where(chosen, router_probs[:, None, :], 0.0), axis=-1)
        own_counts = jnp.sum(chosen.astype(F32), axis=(0, 1)).reshape(1, experts)
        sib_counts = lax.ppermute(own_counts, 'ep', sibling)
        count_rows = jnp.pad(jnp.concatenate([own_counts, sib_counts], axis=0), ((0, (-2 * top_k - 2) % 8), (0, tok_dev - experts)))
        table = jnp.concatenate([topk_idx.T.astype(F32), gate_vals.T, count_rows], axis=0)
        own_w = (w_gate, w_up, w_down)
        sib_w = tuple(lax.ppermute(after(w, sib_counts), 'ep', sibling) for w in own_w)
        t_r1, t_l1 = go_right(table), go_left(table)
        t_far = lax.ppermute(table, 'ep', far)

        hb_r1, ha_l1 = go_right(hb), go_left(ha)
        ha_r2, hb_l2 = go_right(ha_r1), go_left(hb_l1)

        steps = jnp.arange(group_size // cores)
        rel = cores * ((chip + steps) % (group_size // cores))
        ids = jnp.concatenate([jnp.stack([rel + core, rel + 1 - core], axis=1).reshape(-1), jnp.stack([chip, core])]).astype(jnp.int32)
        lists, glists, kept = route_call(ids, table, t_l1, t_far, t_r1, top_k, slots_dev, capacity, local_max)
        lists, glists = lists[:, :, 0, :], glists[:, :, 0, :]
        kept = kept[:, :, 0].astype(jnp.int32)

        def routes(v, row_max):
            return lists[v, :, :row_max], glists[v, :, :row_max], kept[v]

        d_a, d_b = expert_call(routes(1, 2 * local_max), ha_r1, hb_l1, own_w, sib_w, ha, 2 * local_max, 2)
        d_dep, d_a, d_b = d_a, go_left(d_a), go_right(d_b)
        y2 = expert_call(routes(2, local_max), ha_r2, hb_l2, own_w, sib_w, d_dep, local_max, 4)
        p = [go_right(y2[0]), go_left(y2[2])]
        p += [go_right(y2[1]), go_left(y2[3])]
        y1 = expert_call(routes(3, 2 * local_max), ha_l1, hb_r1, own_w, sib_w, y2[0], 2 * local_max, 4)
        y0 = expert_call(routes(0, local_max), ha, hb, own_w, sib_w, y1[0], local_max, 2)
        z, last = [], (y0[0],)
        for i in range(2):
            add_a, add_b = y1[i] + after(p[2 * i], *last), y1[2 + i] + after(p[2 * i + 1], *last)
            last = (add_a, add_b)
            z.append((go_right(add_a), go_left(add_b)))
        base = []
        for i, (h, y, d) in enumerate(((ha, y0[0], d_a), (hb, y0[1], d_b))):
            shared_val = shared_expert(after(h, y), w_sgate, s_gate, s_up, s_down)
            base.append(hidden_in[i * half:(i + 1) * half].astype(F32) + shared_val + y + d)
        out = final_call(0, base[0], base[1], *z[0], None)
        out = final_call(1, base[0], base[1], *z[1], out)
        return out.reshape(tok_dev, hidden)

    row_spec = P(('dp', 'ep'), None)
    full_spec = P(None, None)
    slot_spec = P('ep', None, None)
    in_specs = (row_spec, row_spec, P(None), full_spec, full_spec, full_spec, full_spec, full_spec,
                slot_spec, slot_spec, slot_spec)
    return jax.shard_map(block, mesh=mesh, in_specs=in_specs, out_specs=row_spec, check_vma=False)
```

```python
import functools

import jax
import jax.numpy as jnp
from jax import lax
from jax.experimental import pallas as pl
from jax.experimental.pallas import tpu as pltpu
from jax.sharding import PartitionSpec as P


F32, BF16 = jnp.float32, jnp.bfloat16
CLASSES = (64, 128, 192)
PAIRS = ((0, 0), (3, 1), (2, 2), (1, 3))


def norm_kernel(x_ref, gain_ref, ha_ref, hb_ref):
    gain = gain_ref[...].astype(F32)[None, :]
    for i, out_ref in enumerate((ha_ref, hb_ref)):
        x = x_ref[i].astype(F32)
        inv_rms = lax.rsqrt(jnp.mean(x * x, axis=-1, keepdims=True) + 1e-6)
        out_ref[...] = (x * inv_rms * gain).astype(BF16)


def norm_call(hidden_in, norm_gain):
    toks, hidden = hidden_in.shape
    half, rows = toks // 2, 128
    out = jax.ShapeDtypeStruct((half, hidden), BF16)
    block = pl.BlockSpec((rows, hidden), lambda i: (i, 0))
    return pl.pallas_call(
        norm_kernel,
        grid=(half // rows,),
        out_shape=(out, out),
        in_specs=[pl.BlockSpec((2, rows, hidden), lambda i: (0, i, 0)), pl.BlockSpec((hidden,), lambda i: (0,))],
        out_specs=(block, block),
        compiler_params=pltpu.CompilerParams(dimension_semantics=("arbitrary",)),
        cost_estimate=pl.CostEstimate(flops=4 * toks * hidden, transcendentals=toks, bytes_accessed=4 * toks * hidden),
        name="norm",
    )(hidden_in.reshape(2, half, hidden), norm_gain)


def final_kernel(base_a, base_b, za_ref, zb_ref, *rest):
    out_ref = rest[-1]
    out_ref[0] = (base_a[...] + za_ref[...]).astype(BF16)
    out_ref[1] = (base_b[...] + zb_ref[...]).astype(BF16)


def final_call(part, base_a, base_b, za, zb, so_far):
    size, hidden = za.shape
    rows = 64
    first = part * (size // rows)
    block = pl.BlockSpec((rows, hidden), lambda i: (i, 0))
    base = pl.BlockSpec((rows, hidden), lambda i: (i + first, 0))
    more = [] if so_far is None else [so_far]
    return pl.pallas_call(
        final_kernel,
        grid=(size // rows,),
        out_shape=jax.ShapeDtypeStruct((2, 2 * size, hidden), BF16),
        in_specs=[base] * 2 + [block] * 2 + [pl.BlockSpec(memory_space=pl.ANY)] * len(more),
        out_specs=pl.BlockSpec((2, rows, hidden), lambda i: (0, i + first, 0)),
        input_output_aliases={4: 0} if more else {},
        compiler_params=pltpu.CompilerParams(dimension_semantics=("arbitrary",)),
        cost_estimate=pl.CostEstimate(flops=4 * size * hidden, transcendentals=0, bytes_accessed=20 * size * hidden),
        name="final",
    )(base_a, base_b, za, zb, *more)


def shared_expert(normed, w_sgate, s_gate, s_up, s_down):
    shared_act = (jax.nn.silu(jnp.dot(normed, s_gate, preferred_element_type=F32))
                  * jnp.dot(normed, s_up, preferred_element_type=F32)).astype(BF16)
    shared_val = jnp.dot(shared_act, s_down, preferred_element_type=F32)
    return jax.nn.sigmoid(jnp.dot(normed, w_sgate, preferred_element_type=F32)) * shared_val


def route_kernel(geom, ids_ref, own_ref, next_ref, far_ref, prev_ref, list_ref, glist_ref, count_ref, slot_ref, gate_ref):
    top_k, slots_dev, capacity, local_max = geom
    toks = own_ref.shape[1]
    slots = 2 * slots_dev
    chip, core = ids_ref[8], ids_ref[9]

    def slot_column(like):
        order = lax.broadcasted_iota(jnp.int32, like, 0)
        mine = core * slots_dev + order
        other = (1 - core) * slots_dev + order - slots_dev
        return (chip * slots + jnp.where(order < slots_dev, mine, other)).astype(F32)

    slot_id = slot_column((slots, 1))
    lane_id = lax.broadcasted_iota(jnp.int32, (slots, 128), 1).astype(F32)
    hots, counts = [], []
    for j, ref in enumerate((own_ref, next_ref, far_ref, prev_ref)):
        table = ref[...]
        hot = jnp.zeros((slots, toks), F32)
        gate = jnp.zeros((slots, toks), F32)
        for k in range(top_k):
            hit = table[k:k + 1, :] == slot_id
            hot = hot + jnp.where(hit, 1.0, 0.0)
            gate = gate + jnp.where(hit, table[top_k + k:top_k + k + 1, :], 0.0)
        for i in range(2):
            row = table[2 * top_k + i:2 * top_k + i + 1, :128]
            counts.append(jnp.sum(jnp.where(lane_id == slot_id, row, 0.0), axis=1, keepdims=True))
        hots.append(hot)
        gate_ref[j] = gate
    hot_all = jnp.concatenate(hots, axis=0)
    hot_bf = hot_all.astype(BF16)
    tile, half = 256, toks // 2

    def before(c):
        rows = lax.broadcasted_iota(jnp.int32, (toks, tile), 0)
        cols = lax.broadcasted_iota(jnp.int32, (toks, tile), 1) + c * tile
        return jnp.where(rows < cols, 1.0, 0.0).astype(BF16)

    lowers = []
    for j in range(4):
        lower = jnp.zeros((slots, 1), F32)
        for q in range(8):
            lower = lower + counts[q] * (ids_ref[q] < ids_ref[2 * j]).astype(F32)
        lowers.append(lower)
    for c in range(toks // tile):
        pos = jnp.dot(hot_bf, before(c), preferred_element_type=F32)
        for j in range(4):
            part = pos[j * slots:(j + 1) * slots]
            kept = (hot_all[j * slots:(j + 1) * slots, c * tile:(c + 1) * tile] > 0.0) & (part + lowers[j] < capacity)
            slot_ref[j, :, c * tile:(c + 1) * tile] = jnp.where(kept, 1.0, 0.0)
    joined = []
    gates = [gate_ref[j] for j in range(4)]
    for v, (ja, jb) in enumerate(PAIRS):
        joined.append(jnp.concatenate([slot_ref[ja][:, :half], slot_ref[jb][:, half:]], axis=1))
        gate_ref[v] = jnp.concatenate([gates[ja][:, :half], gates[jb][:, half:]], axis=1)
        count_ref[v] = jnp.broadcast_to(jnp.sum(joined[v], axis=1, keepdims=True), (slots, 128))
    kept_all = jnp.concatenate(joined, axis=0)
    kept_bf = kept_all.astype(BF16)
    for c in range(toks // tile):
        pos = jnp.dot(kept_bf, before(c), preferred_element_type=F32)
        for v in range(4):
            kept = kept_all[v * slots:(v + 1) * slots, c * tile:(c + 1) * tile] > 0.0
            slot_ref[v, :, c * tile:(c + 1) * tile] = jnp.where(kept, pos[v * slots:(v + 1) * slots], -1.0)
    token = lax.broadcasted_iota(jnp.int32, (8, toks), 1)
    row8 = lax.broadcasted_iota(jnp.int32, (8, toks), 0)
    digits = jnp.where(row8 == 0, token // 32, token % 32).astype(F32)
    row_of = lax.broadcasted_iota(jnp.int32, (slots, toks), 0)
    count_row = lax.broadcasted_iota(jnp.int32, (slots, 128), 0)

    def lists(e, carry):
        for j in range(4):
            pos = jnp.sum(jnp.where(row_of == e, slot_ref[j], 0.0), axis=0, keepdims=True)
            gate = jnp.sum(jnp.where(row_of == e, gate_ref[j], 0.0), axis=0, keepdims=True)
            g1 = gate.astype(BF16).astype(F32)
            g2 = (gate - g1).astype(BF16).astype(F32)
            g3 = gate - g1 - g2
            left = jnp.where(row8 < 2, digits, jnp.where(row8 == 2, g1, jnp.where(row8 == 3, g2, g3))).astype(BF16)
            width = local_max if PAIRS[j][0] == PAIRS[j][1] else 2 * local_max
            want = lax.broadcasted_iota(jnp.int32, (width, toks), 0).astype(F32)
            pick = jnp.where(want == pos, 1.0, 0.0).astype(BF16)
            got = lax.dot_general(left, pick, (((1,), (1,)), ((), ())), preferred_element_type=F32)
            found = 32.0 * got[0:1] + got[1:2]
            held = jnp.sum(jnp.where(count_row == e, count_ref[j], 0.0), axis=0, keepdims=True)[:, 0:1]
            lane = lax.broadcasted_iota(jnp.int32, (1, width), 1).astype(F32)
            found = jnp.where(lane < held, found, float(toks)).astype(jnp.int32)
            list_ref[j, e, :, :width] = jnp.broadcast_to(found, (8, width))
            glist_ref[j, e, :, :width] = jnp.broadcast_to((got[2:3] + got[3:4]) + got[4:5], (8, width))
        return carry

    lax.fori_loop(0, slots, lists, 0)


def route_call(ids, own, nxt, far, prv, top_k, slots_dev, capacity, local_max):
    toks = own.shape[1]
    slots = 2 * slots_dev
    vmem = pl.BlockSpec(memory_space=pltpu.VMEM)
    return pl.pallas_call(
        functools.partial(route_kernel, (top_k, slots_dev, capacity, local_max)),
        out_shape=(jax.ShapeDtypeStruct((4, slots, 8, 2 * local_max), jnp.int32), jax.ShapeDtypeStruct((4, slots, 8, 2 * local_max), F32),
                   jax.ShapeDtypeStruct((4, slots, 128), F32)),
        in_specs=[pl.BlockSpec(memory_space=pltpu.SMEM)] + [vmem] * 4,
        out_specs=(vmem,) * 3,
        scratch_shapes=[pltpu.VMEM((4, slots, toks), F32), pltpu.VMEM((4, slots, toks), F32)],
        cost_estimate=pl.CostEstimate(flops=1_000_000, transcendentals=0, bytes_accessed=2_000_000),
        name="route",
    )(ids, own, nxt, far, prv)


def expert_kernel(pieces, classes, slots_dev, depth, *refs):
    refs = list(refs)
    n_src = 1

    def take(n):
        got = refs[:n]
        del refs[:n]
        return got

    lists, glists, counts = take(n_src), take(n_src), take(n_src)
    has, hbs = take(n_src), take(n_src)
    own, sib = take(3), take(3)
    take(1)
    ys = take(pieces)
    wg_ref, wu_ref, wd_ref = take(3)
    row_refs, tok_refs, sum_refs = [take(2) for _ in range(n_src)], [take(2) for _ in range(n_src)], [take(2) for _ in range(n_src)]
    stage_ref, sems, out_sems = take(3)
    step = pl.program_id(0)
    steps = 2 * slots_dev
    half, hidden = has[0].shape
    blocks = hidden // 128
    pitch, unroll, group = 8, 8, 64
    split = [(j // pitch, j % pitch) for j in range(blocks)]

    def copies(srcs, i, b):
        return [pltpu.make_async_copy(src.at[i], dst.at[b], sems.at[n, b])
                for n, (src, dst) in enumerate(zip(srcs, (wg_ref, wu_ref, wd_ref)))]

    def fetch(i):
        @pl.when(i < slots_dev)
        def _():
            for c in copies(own, i, i % depth):
                c.start()

        @pl.when((i >= slots_dev) & (i < steps))
        def _():
            for c in copies(sib, i - slots_dev, i % depth):
                c.start()

    @pl.when(step == 0)
    def _():
        for i in range(depth - 1):
            fetch(jnp.int32(i))
        for q in range(n_src):
            for ref in sum_refs[q]:
                ref[...] = jnp.zeros_like(ref)
            for ref in tok_refs[q]:
                ref[pl.ds(2 * half * pitch, pitch), :] = jnp.zeros((pitch, 128), F32)

            def spread(i, carry):
                for src, start in ((has[q], 0), (hbs[q], half)):
                    v = src[pl.ds(pl.multiple_of(i * group, group), group), :].astype(F32)
                    for j, (w, k) in enumerate(split):
                        tok_refs[q][w][pl.ds((start + i * group) * pitch + k, group, stride=pitch), :] = v[:, j * 128:(j + 1) * 128]
                return carry

            lax.fori_loop(0, half // group, spread, 0)

    fetch(step + depth - 1)
    buf = step % depth
    for c in copies(own, 0, buf):
        c.wait()
    count = [c[step] for c in counts]
    most = count[0] if n_src == 1 else jnp.maximum(count[0], count[1])
    low = 0
    for rows in classes:
        @pl.when((most > low) & (most <= rows))
        def _(rows=rows):
            xs = []
            for q in range(n_src):
                def pick(i, carry):
                    found = []
                    for u in range(unroll):
                        spot = pl.ds(pl.multiple_of(lists[q][step, i * unroll + u] * pitch, pitch), pitch)
                        found += [tok_refs[q][w][spot, :] for w in range(2)]
                    for u in range(unroll):
                        row = pl.ds(pl.multiple_of((i * unroll + u) * pitch, pitch), pitch)
                        for w in range(2):
                            row_refs[q][w][row, :] = found[2 * u + w]
                    return carry

                lax.fori_loop(0, rows // unroll, pick, 0)
                xs.append(jnp.concatenate([row_refs[q][w][pl.ds(k, rows, stride=pitch), :].astype(BF16) for w, k in split], axis=1))
            x = xs[0] if n_src == 1 else jnp.concatenate(xs, axis=0)
            gate_proj = jnp.dot(x, wg_ref[buf], preferred_element_type=F32)
            up_proj = jnp.dot(x, wu_ref[buf], preferred_element_type=F32)
            act = (jax.nn.silu(gate_proj) * up_proj).astype(BF16)
            out = jnp.dot(act, wd_ref[buf], preferred_element_type=F32).astype(BF16).astype(F32)
            for q in range(n_src):
                for j, (w, k) in enumerate(split):
                    row_refs[q][w][pl.ds(k, rows, stride=pitch), :] = out[q * rows:(q + 1) * rows, j * 128:(j + 1) * 128]

        low = rows

    for q in range(n_src):
        def scatter(i, carry):
            spots, sums = [], []
            for u in range(unroll):
                r = i * unroll + u
                spot = pl.ds(pl.multiple_of(lists[q][step, r] * pitch, pitch), pitch)
                row = pl.ds(pl.multiple_of(r * pitch, pitch), pitch)
                g = glists[q][step, r]
                for w in range(2):
                    spots.append((w, spot))
                    sums.append(sum_refs[q][w][spot, :] + row_refs[q][w][row, :] * g)
            for (w, spot), v in zip(spots, sums):
                sum_refs[q][w][spot, :] = v
            return carry

        lax.fori_loop(0, (count[q] + unroll - 1) // unroll, scatter, 0)

    @pl.when(step == steps - 1)
    def _():
        size = 2 * half // pieces
        outs = [(0, ref, n * size) for n, ref in enumerate(ys)]

        def put(n, ref, i):
            rows = pl.ds(pl.multiple_of(i * group, group), group)
            return pltpu.make_async_copy(stage_ref.at[i % 2, n], ref.at[rows], out_sems.at[i % 2, n])

        def unpack(i, carry):
            for n, (q, ref, start) in enumerate(outs):
                @pl.when(i >= 2)
                def _():
                    put(n, ref, i).wait()

                for j, (w, k) in enumerate(split):
                    stage_ref[i % 2, n, :, j * 128:(j + 1) * 128] = (
                        sum_refs[q][w][pl.ds((start + i * group) * pitch + k, group, stride=pitch), :])
                put(n, ref, i).start()
            return carry

        lax.fori_loop(0, size // group, unpack, 0)
        for i in range(2):
            for n, (q, ref, start) in enumerate(outs):
                put(n, ref, i).wait()


def expert_call(routes, ha, hb, own, sib, dep, row_max, pieces):
    half, hidden = ha.shape
    slots_dev, _, ff = own[0].shape
    depth = 4
    classes = tuple(c for c in CLASSES if c < row_max) + (row_max,)
    whole = pl.BlockSpec((half, hidden), lambda s: (0, 0), pipeline_mode=pl.Buffered(1))
    smem = pl.BlockSpec(memory_space=pltpu.SMEM)
    hbm = pl.BlockSpec(memory_space=pl.ANY)
    out = jax.ShapeDtypeStruct((2 * half // pieces, hidden), F32)
    toks = (2 * half + 8) * 8
    return pl.pallas_call(
        functools.partial(expert_kernel, pieces, classes, slots_dev, depth),
        grid=(2 * slots_dev,),
        out_shape=(out,) * pieces,
        in_specs=[smem] * 3 + [whole] * 2 + [hbm] * 7,
        out_specs=(hbm,) * pieces,
        scratch_shapes=[pltpu.VMEM((depth, hidden, ff), BF16), pltpu.VMEM((depth, hidden, ff), BF16), pltpu.VMEM((depth, ff, hidden), BF16)]
        + [pltpu.VMEM((row_max * 8, 128), F32)] * 2 + [pltpu.VMEM((toks, 128), F32)] * 4
        + [pltpu.VMEM((2, pieces, 64, hidden), F32), pltpu.SemaphoreType.DMA((3, depth)), pltpu.SemaphoreType.DMA((2, pieces))],
        compiler_params=pltpu.CompilerParams(dimension_semantics=("arbitrary",), vmem_limit_bytes=62 * 1024 * 1024),
        cost_estimate=pl.CostEstimate(flops=1_000_000, transcendentals=0,
                                      bytes_accessed=2 * slots_dev * 3 * hidden * ff * 2),
        name="experts",
    )(*routes, ha, hb, *own, *sib, dep)


def solution(mesh):
    group_size = mesh.shape['ep']
    cores = 2
    right = [(i, (i + cores) % group_size) for i in range(group_size)]
    left = [(i, (i - cores) % group_size) for i in range(group_size)]
    far = [(i, (i + group_size // 2) % group_size) for i in range(group_size)]
    sibling = [(i, i ^ 1) for i in range(group_size)]

    def block(hidden_in, topk_idx, norm_gain, w_router, w_sgate, s_gate, s_up, s_down, w_gate, w_up, w_down):
        tok_dev, hidden = hidden_in.shape
        top_k = topk_idx.shape[1]
        experts = w_router.shape[1]
        slots_dev = w_gate.shape[0]
        half = tok_dev // 2
        capacity = (5 * tok_dev * group_size * top_k + 4 * experts - 1) // (4 * experts)
        local_max = (2 * tok_dev * top_k + experts - 1) // experts
        me = lax.axis_index('ep')

        def go_right(v):
            return lax.ppermute(v, 'ep', right)

        def go_left(v):
            return lax.ppermute(v, 'ep', left)

        chip, core = me // cores, me % cores

        def after(v, *deps):
            return lax.optimization_barrier((v,) + deps)[0]

        ha, hb = norm_call(hidden_in, norm_gain)
        ha_r1, hb_l1 = go_right(ha), go_left(hb)

        logits = jnp.concatenate([jnp.dot(h, w_router, preferred_element_type=F32) for h in (ha, hb)], axis=0)
        router_probs = jax.nn.softmax(logits, axis=-1)
        chosen = topk_idx[:, :, None] == jnp.arange(experts)[None, None, :]
        gate_vals = jnp.sum(jnp.where(chosen, router_probs[:, None, :], 0.0), axis=-1)
        own_counts = jnp.sum(chosen.astype(F32), axis=(0, 1)).reshape(1, experts)
        sib_counts = lax.ppermute(own_counts, 'ep', sibling)
        count_rows = jnp.pad(jnp.concatenate([own_counts, sib_counts], axis=0), ((0, (-2 * top_k - 2) % 8), (0, tok_dev - experts)))
        table = jnp.concatenate([topk_idx.T.astype(F32), gate_vals.T, count_rows], axis=0)
        own_w = (w_gate, w_up, w_down)
        sib_w = tuple(lax.ppermute(after(w, sib_counts), 'ep', sibling) for w in own_w)
        t_r1, t_l1 = go_right(table), go_left(table)
        t_far = lax.ppermute(table, 'ep', far)

        hb_r1, ha_l1 = go_right(hb), go_left(ha)
        ha_r2, hb_l2 = go_right(ha_r1), go_left(hb_l1)

        steps = jnp.arange(group_size // cores)
        rel = cores * ((chip + steps) % (group_size // cores))
        ids = jnp.concatenate([jnp.stack([rel + core, rel + 1 - core], axis=1).reshape(-1), jnp.stack([chip, core])]).astype(jnp.int32)
        lists, glists, kept = route_call(ids, table, t_l1, t_far, t_r1, top_k, slots_dev, capacity, local_max)
        lists, glists = lists[:, :, 0, :], glists[:, :, 0, :]
        kept = kept[:, :, 0].astype(jnp.int32)

        def routes(v, row_max):
            return lists[v, :, :row_max], glists[v, :, :row_max], kept[v]

        d_a, d_b = expert_call(routes(1, 2 * local_max), ha_r1, hb_l1, own_w, sib_w, ha, 2 * local_max, 2)
        d_dep, d_a, d_b = d_a, go_left(d_a), go_right(d_b)
        y2 = expert_call(routes(2, local_max), ha_r2, hb_l2, own_w, sib_w, d_dep, local_max, 4)
        p = [go_right(y2[0]), go_left(y2[2])]
        p += [go_right(y2[1]), go_left(y2[3])]
        y1 = expert_call(routes(3, 2 * local_max), ha_l1, hb_r1, own_w, sib_w, y2[0], 2 * local_max, 4)
        half_sums = [shared_expert(after(h, y1[0]), w_sgate, s_gate, s_up, s_down) for h in (ha, hb)]

        def relay(i, *deps):
            return y1[i] + after(p[2 * i], *deps), y1[2 + i] + after(p[2 * i + 1], *deps)

        add_a, add_b = relay(0, *half_sums)
        z0 = go_right(add_a), go_left(add_b)
        y0 = expert_call(routes(0, local_max), ha, hb, own_w, sib_w, add_b, local_max, 2)
        add_a, add_b = relay(1, y0[0])
        z1 = go_right(add_a), go_left(add_b)
        base = [hidden_in[i * half:(i + 1) * half].astype(F32) + half_sums[i] + y0[i] + d for i, d in enumerate((d_a, d_b))]
        out = final_call(0, base[0], base[1], *z0, None)
        out = final_call(1, base[0], base[1], *z1, out)
        return out.reshape(tok_dev, hidden)

    row_spec = P(('dp', 'ep'), None)
    full_spec = P(None, None)
    slot_spec = P('ep', None, None)
    in_specs = (row_spec, row_spec, P(None), full_spec, full_spec, full_spec, full_spec, full_spec,
                slot_spec, slot_spec, slot_spec)
    return jax.shard_map(block, mesh=mesh, in_specs=in_specs, out_specs=row_spec, check_vma=False)
```

```python
import functools

import jax
import jax.numpy as jnp
from jax import lax
from jax.experimental import pallas as pl
from jax.experimental.pallas import tpu as pltpu
from jax.sharding import PartitionSpec as P


F32, BF16 = jnp.float32, jnp.bfloat16
CLASSES = (64, 128, 192)
PAIRS = ((0, 0), (3, 1), (2, 2), (1, 3))


def norm_kernel(x_ref, gain_ref, ha_ref, hb_ref):
    gain = gain_ref[...].astype(F32)[None, :]
    for i, out_ref in enumerate((ha_ref, hb_ref)):
        x = x_ref[i].astype(F32)
        inv_rms = lax.rsqrt(jnp.mean(x * x, axis=-1, keepdims=True) + 1e-6)
        out_ref[...] = (x * inv_rms * gain).astype(BF16)


def norm_call(hidden_in, norm_gain):
    toks, hidden = hidden_in.shape
    half, rows = toks // 2, 128
    out = jax.ShapeDtypeStruct((half, hidden), BF16)
    block = pl.BlockSpec((rows, hidden), lambda i: (i, 0))
    return pl.pallas_call(
        norm_kernel,
        grid=(half // rows,),
        out_shape=(out, out),
        in_specs=[pl.BlockSpec((2, rows, hidden), lambda i: (0, i, 0)), pl.BlockSpec((hidden,), lambda i: (0,))],
        out_specs=(block, block),
        compiler_params=pltpu.CompilerParams(dimension_semantics=("arbitrary",)),
        cost_estimate=pl.CostEstimate(flops=4 * toks * hidden, transcendentals=toks, bytes_accessed=4 * toks * hidden),
        name="norm",
    )(hidden_in.reshape(2, half, hidden), norm_gain)


def final_kernel(base_a, base_b, za_ref, zb_ref, *rest):
    out_ref = rest[-1]
    out_ref[0] = (base_a[...] + za_ref[...]).astype(BF16)
    out_ref[1] = (base_b[...] + zb_ref[...]).astype(BF16)


def final_call(start, base_a, base_b, za, zb, so_far):
    (size, hidden), half = za.shape, base_a.shape[0]
    rows = 64
    first = start // rows
    block = pl.BlockSpec((rows, hidden), lambda i: (i, 0))
    base = pl.BlockSpec((rows, hidden), lambda i: (i + first, 0))
    more = [] if so_far is None else [so_far]
    return pl.pallas_call(
        final_kernel,
        grid=(size // rows,),
        out_shape=jax.ShapeDtypeStruct((2, half, hidden), BF16),
        in_specs=[base] * 2 + [block] * 2 + [pl.BlockSpec(memory_space=pl.ANY)] * len(more),
        out_specs=pl.BlockSpec((2, rows, hidden), lambda i: (0, i + first, 0)),
        input_output_aliases={4: 0} if more else {},
        compiler_params=pltpu.CompilerParams(dimension_semantics=("arbitrary",)),
        cost_estimate=pl.CostEstimate(flops=4 * size * hidden, transcendentals=0, bytes_accessed=20 * size * hidden),
        name="final",
    )(base_a, base_b, za, zb, *more)


def shared_kernel(x_ref, ha_ref, hb_ref, gate_row, sg_ref, su_ref, sd_ref, outa_ref, outb_ref):
    step = pl.program_id(0)
    for i, (h_ref, out_ref) in enumerate(((ha_ref, outa_ref), (hb_ref, outb_ref))):
        h = h_ref[...]
        gate_proj = jnp.dot(h, sg_ref[...], preferred_element_type=F32)
        act = (jax.nn.silu(gate_proj) * jnp.dot(h, su_ref[...], preferred_element_type=F32)).astype(BF16)
        part = jnp.dot(act, sd_ref[...], preferred_element_type=F32)

        @pl.when(step == 0)
        def _():
            out_ref[...] = part

        @pl.when(step > 0)
        def _():
            out_ref[...] += part

        @pl.when(step == pl.num_programs(0) - 1)
        def _():
            weight = jnp.sum(h.astype(F32) * gate_row[...].astype(F32), axis=1, keepdims=True)
            out_ref[...] = x_ref[i].astype(F32) + jax.nn.sigmoid(weight) * out_ref[...]


def shared_call(hidden_in, ha, hb, w_sgate, s_gate, s_up, s_down):
    half, hidden = ha.shape
    ff = s_gate.shape[1]
    chunk = 256
    whole = pl.BlockSpec((half, hidden), lambda i: (0, 0), pipeline_mode=pl.Buffered(1))
    wide = pl.BlockSpec((hidden, chunk), lambda i: (0, i))
    out = jax.ShapeDtypeStruct((half, hidden), F32)
    return pl.pallas_call(
        shared_kernel,
        grid=(ff // chunk,),
        out_shape=(out, out),
        in_specs=[pl.BlockSpec((2, half, hidden), lambda i: (0, 0, 0), pipeline_mode=pl.Buffered(1)), whole, whole,
                  pl.BlockSpec((1, hidden), lambda i: (0, 0)), wide, wide, pl.BlockSpec((chunk, hidden), lambda i: (i, 0))],
        out_specs=(whole, whole),
        compiler_params=pltpu.CompilerParams(dimension_semantics=("arbitrary",), vmem_limit_bytes=60 * 1024 * 1024),
        cost_estimate=pl.CostEstimate(flops=1_000_000, transcendentals=0, bytes_accessed=6 * ff * hidden),
        name="shared",
    )(hidden_in.reshape(2, half, hidden), ha, hb, w_sgate.reshape(1, hidden), s_gate, s_up, s_down)


def route_kernel(geom, ids_ref, own_ref, next_ref, far_ref, prev_ref, list_ref, glist_ref, count_ref, slot_ref, gate_ref):
    top_k, slots_dev, capacity, local_max = geom
    toks = own_ref.shape[1]
    slots = 2 * slots_dev
    chip, core = ids_ref[8], ids_ref[9]

    def slot_column(like):
        order = lax.broadcasted_iota(jnp.int32, like, 0)
        mine = core * slots_dev + order
        other = (1 - core) * slots_dev + order - slots_dev
        return (chip * slots + jnp.where(order < slots_dev, mine, other)).astype(F32)

    slot_id = slot_column((slots, 1))
    lane_id = lax.broadcasted_iota(jnp.int32, (slots, 128), 1).astype(F32)
    hots, counts = [], []
    for j, ref in enumerate((own_ref, next_ref, far_ref, prev_ref)):
        table = ref[...]
        hot = jnp.zeros((slots, toks), F32)
        gate = jnp.zeros((slots, toks), F32)
        for k in range(top_k):
            hit = table[k:k + 1, :] == slot_id
            hot = hot + jnp.where(hit, 1.0, 0.0)
            gate = gate + jnp.where(hit, table[top_k + k:top_k + k + 1, :], 0.0)
        for i in range(2):
            row = table[2 * top_k + i:2 * top_k + i + 1, :128]
            counts.append(jnp.sum(jnp.where(lane_id == slot_id, row, 0.0), axis=1, keepdims=True))
        hots.append(hot)
        gate_ref[j] = gate
    hot_all = jnp.concatenate(hots, axis=0)
    hot_bf = hot_all.astype(BF16)
    tile, half = 256, toks // 2

    def before(c):
        rows = lax.broadcasted_iota(jnp.int32, (toks, tile), 0)
        cols = lax.broadcasted_iota(jnp.int32, (toks, tile), 1) + c * tile
        return jnp.where(rows < cols, 1.0, 0.0).astype(BF16)

    lowers = []
    for j in range(4):
        lower = jnp.zeros((slots, 1), F32)
        for q in range(8):
            lower = lower + counts[q] * (ids_ref[q] < ids_ref[2 * j]).astype(F32)
        lowers.append(lower)
    for c in range(toks // tile):
        pos = jnp.dot(hot_bf, before(c), preferred_element_type=F32)
        for j in range(4):
            part = pos[j * slots:(j + 1) * slots]
            kept = (hot_all[j * slots:(j + 1) * slots, c * tile:(c + 1) * tile] > 0.0) & (part + lowers[j] < capacity)
            slot_ref[j, :, c * tile:(c + 1) * tile] = jnp.where(kept, 1.0, 0.0)
    joined = []
    gates = [gate_ref[j] for j in range(4)]
    for v, (ja, jb) in enumerate(PAIRS):
        joined.append(jnp.concatenate([slot_ref[ja][:, :half], slot_ref[jb][:, half:]], axis=1))
        gate_ref[v] = jnp.concatenate([gates[ja][:, :half], gates[jb][:, half:]], axis=1)
        count_ref[v] = jnp.broadcast_to(jnp.sum(joined[v], axis=1, keepdims=True), (slots, 128))
    kept_all = jnp.concatenate(joined, axis=0)
    kept_bf = kept_all.astype(BF16)
    for c in range(toks // tile):
        pos = jnp.dot(kept_bf, before(c), preferred_element_type=F32)
        for v in range(4):
            kept = kept_all[v * slots:(v + 1) * slots, c * tile:(c + 1) * tile] > 0.0
            slot_ref[v, :, c * tile:(c + 1) * tile] = jnp.where(kept, pos[v * slots:(v + 1) * slots], -1.0)
    token = lax.broadcasted_iota(jnp.int32, (8, toks), 1)
    row8 = lax.broadcasted_iota(jnp.int32, (8, toks), 0)
    digits = jnp.where(row8 == 0, token // 32, token % 32).astype(F32)
    row_of = lax.broadcasted_iota(jnp.int32, (slots, toks), 0)
    count_row = lax.broadcasted_iota(jnp.int32, (slots, 128), 0)

    def lists(e, carry):
        for j in range(4):
            pos = jnp.sum(jnp.where(row_of == e, slot_ref[j], 0.0), axis=0, keepdims=True)
            gate = jnp.sum(jnp.where(row_of == e, gate_ref[j], 0.0), axis=0, keepdims=True)
            g1 = gate.astype(BF16).astype(F32)
            g2 = (gate - g1).astype(BF16).astype(F32)
            g3 = gate - g1 - g2
            left = jnp.where(row8 < 2, digits, jnp.where(row8 == 2, g1, jnp.where(row8 == 3, g2, g3))).astype(BF16)
            width = local_max if PAIRS[j][0] == PAIRS[j][1] else 2 * local_max
            want = lax.broadcasted_iota(jnp.int32, (width, toks), 0).astype(F32)
            pick = jnp.where(want == pos, 1.0, 0.0).astype(BF16)
            got = lax.dot_general(left, pick, (((1,), (1,)), ((), ())), preferred_element_type=F32)
            found = 32.0 * got[0:1] + got[1:2]
            held = jnp.sum(jnp.where(count_row == e, count_ref[j], 0.0), axis=0, keepdims=True)[:, 0:1]
            lane = lax.broadcasted_iota(jnp.int32, (1, width), 1).astype(F32)
            found = jnp.where(lane < held, found, float(toks)).astype(jnp.int32)
            list_ref[j, e, :, :width] = jnp.broadcast_to(found, (8, width))
            glist_ref[j, e, :, :width] = jnp.broadcast_to((got[2:3] + got[3:4]) + got[4:5], (8, width))
        return carry

    lax.fori_loop(0, slots, lists, 0)


def route_call(ids, own, nxt, far, prv, top_k, slots_dev, capacity, local_max):
    toks = own.shape[1]
    slots = 2 * slots_dev
    vmem = pl.BlockSpec(memory_space=pltpu.VMEM)
    return pl.pallas_call(
        functools.partial(route_kernel, (top_k, slots_dev, capacity, local_max)),
        out_shape=(jax.ShapeDtypeStruct((4, slots, 8, 2 * local_max), jnp.int32), jax.ShapeDtypeStruct((4, slots, 8, 2 * local_max), F32),
                   jax.ShapeDtypeStruct((4, slots, 128), F32)),
        in_specs=[pl.BlockSpec(memory_space=pltpu.SMEM)] + [vmem] * 4,
        out_specs=(vmem,) * 3,
        scratch_shapes=[pltpu.VMEM((4, slots, toks), F32), pltpu.VMEM((4, slots, toks), F32)],
        cost_estimate=pl.CostEstimate(flops=1_000_000, transcendentals=0, bytes_accessed=2_000_000),
        name="route",
    )(ids, own, nxt, far, prv)


def expert_kernel(sizes, classes, slots_dev, depth, *refs):
    refs = list(refs)
    n_src = 1

    def take(n):
        got = refs[:n]
        del refs[:n]
        return got

    lists, glists, counts = take(n_src), take(n_src), take(n_src)
    has, hbs = take(n_src), take(n_src)
    own, sib = take(3), take(3)
    take(1)
    ys = take(len(sizes))
    wg_ref, wu_ref, wd_ref = take(3)
    row_refs, tok_refs, sum_refs = [take(2) for _ in range(n_src)], [take(2) for _ in range(n_src)], [take(2) for _ in range(n_src)]
    stage_ref, sems, out_sems = take(3)
    step = pl.program_id(0)
    steps = 2 * slots_dev
    half, hidden = has[0].shape
    blocks = hidden // 128
    pitch, unroll, group = 8, 8, 64
    split = [(j // pitch, j % pitch) for j in range(blocks)]

    def copies(srcs, i, b):
        return [pltpu.make_async_copy(src.at[i], dst.at[b], sems.at[n, b])
                for n, (src, dst) in enumerate(zip(srcs, (wg_ref, wu_ref, wd_ref)))]

    def fetch(i):
        @pl.when(i < slots_dev)
        def _():
            for c in copies(own, i, i % depth):
                c.start()

        @pl.when((i >= slots_dev) & (i < steps))
        def _():
            for c in copies(sib, i - slots_dev, i % depth):
                c.start()

    @pl.when(step == 0)
    def _():
        for i in range(depth - 1):
            fetch(jnp.int32(i))
        for q in range(n_src):
            for ref in sum_refs[q]:
                ref[...] = jnp.zeros_like(ref)
            for ref in tok_refs[q]:
                ref[pl.ds(2 * half * pitch, pitch), :] = jnp.zeros((pitch, 128), F32)

            def spread(i, carry):
                for src, start in ((has[q], 0), (hbs[q], half)):
                    v = src[pl.ds(pl.multiple_of(i * group, group), group), :].astype(F32)
                    for j, (w, k) in enumerate(split):
                        tok_refs[q][w][pl.ds((start + i * group) * pitch + k, group, stride=pitch), :] = v[:, j * 128:(j + 1) * 128]
                return carry

            lax.fori_loop(0, half // group, spread, 0)

    fetch(step + depth - 1)
    buf = step % depth
    for c in copies(own, 0, buf):
        c.wait()
    count = [c[step] for c in counts]
    most = count[0] if n_src == 1 else jnp.maximum(count[0], count[1])
    low = 0
    for rows in classes:
        @pl.when((most > low) & (most <= rows))
        def _(rows=rows):
            xs = []
            for q in range(n_src):
                def pick(i, carry):
                    found = []
                    for u in range(unroll):
                        spot = pl.ds(pl.multiple_of(lists[q][step, i * unroll + u] * pitch, pitch), pitch)
                        found += [tok_refs[q][w][spot, :] for w in range(2)]
                    for u in range(unroll):
                        row = pl.ds(pl.multiple_of((i * unroll + u) * pitch, pitch), pitch)
                        for w in range(2):
                            row_refs[q][w][row, :] = found[2 * u + w]
                    return carry

                lax.fori_loop(0, rows // unroll, pick, 0)
                xs.append(jnp.concatenate([row_refs[q][w][pl.ds(k, rows, stride=pitch), :].astype(BF16) for w, k in split], axis=1))
            x = xs[0] if n_src == 1 else jnp.concatenate(xs, axis=0)
            gate_proj = jnp.dot(x, wg_ref[buf], preferred_element_type=F32)
            up_proj = jnp.dot(x, wu_ref[buf], preferred_element_type=F32)
            act = (jax.nn.silu(gate_proj) * up_proj).astype(BF16)
            out = jnp.dot(act, wd_ref[buf], preferred_element_type=F32).astype(BF16).astype(F32)
            for q in range(n_src):
                for j, (w, k) in enumerate(split):
                    row_refs[q][w][pl.ds(k, rows, stride=pitch), :] = out[q * rows:(q + 1) * rows, j * 128:(j + 1) * 128]

        low = rows

    for q in range(n_src):
        def scatter(i, carry):
            spots, sums = [], []
            for u in range(unroll):
                r = i * unroll + u
                spot = pl.ds(pl.multiple_of(lists[q][step, r] * pitch, pitch), pitch)
                row = pl.ds(pl.multiple_of(r * pitch, pitch), pitch)
                g = glists[q][step, r]
                for w in range(2):
                    spots.append((w, spot))
                    sums.append(sum_refs[q][w][spot, :] + row_refs[q][w][row, :] * g)
            for (w, spot), v in zip(spots, sums):
                sum_refs[q][w][spot, :] = v
            return carry

        lax.fori_loop(0, (count[q] + unroll - 1) // unroll, scatter, 0)

    @pl.when(step == steps - 1)
    def _():
        start = 0
        for n, (ref, size) in enumerate(zip(ys, sizes)):
            def put(i, n=n, ref=ref):
                rows = pl.ds(pl.multiple_of(i * group, group), group)
                return pltpu.make_async_copy(stage_ref.at[i % 2, n], ref.at[rows], out_sems.at[i % 2, n])

            def unpack(i, carry, n=n, start=start, put=put):
                @pl.when(i >= 2)
                def _():
                    put(i - 2).wait()

                for j, (w, k) in enumerate(split):
                    stage_ref[i % 2, n, :, j * 128:(j + 1) * 128] = (
                        sum_refs[0][w][pl.ds((start + i * group) * pitch + k, group, stride=pitch), :])
                put(i).start()
                return carry

            lax.fori_loop(0, size // group, unpack, 0)
            start += size
        for n, (ref, size) in enumerate(zip(ys, sizes)):
            for i in range(2):
                pltpu.make_async_copy(stage_ref.at[i, n], ref.at[pl.ds(0, group)], out_sems.at[i, n]).wait()


def expert_call(routes, ha, hb, own, sib, dep, row_max, sizes):
    half, hidden = ha.shape
    slots_dev, _, ff = own[0].shape
    depth = 4
    classes = tuple(c for c in CLASSES if c < row_max) + (row_max,)
    whole = pl.BlockSpec((half, hidden), lambda s: (0, 0), pipeline_mode=pl.Buffered(1))
    smem = pl.BlockSpec(memory_space=pltpu.SMEM)
    hbm = pl.BlockSpec(memory_space=pl.ANY)
    pieces = len(sizes)
    toks = (2 * half + 8) * 8
    return pl.pallas_call(
        functools.partial(expert_kernel, sizes, classes, slots_dev, depth),
        grid=(2 * slots_dev,),
        out_shape=tuple(jax.ShapeDtypeStruct((n, hidden), F32) for n in sizes),
        in_specs=[smem] * 3 + [whole] * 2 + [hbm] * 7,
        out_specs=(hbm,) * pieces,
        scratch_shapes=[pltpu.VMEM((depth, hidden, ff), BF16), pltpu.VMEM((depth, hidden, ff), BF16), pltpu.VMEM((depth, ff, hidden), BF16)]
        + [pltpu.VMEM((row_max * 8, 128), F32)] * 2 + [pltpu.VMEM((toks, 128), F32)] * 4
        + [pltpu.VMEM((2, pieces, 64, hidden), F32), pltpu.SemaphoreType.DMA((3, depth)), pltpu.SemaphoreType.DMA((2, pieces))],
        compiler_params=pltpu.CompilerParams(dimension_semantics=("arbitrary",), vmem_limit_bytes=62 * 1024 * 1024),
        cost_estimate=pl.CostEstimate(flops=1_000_000, transcendentals=0,
                                      bytes_accessed=2 * slots_dev * 3 * hidden * ff * 2),
        name="experts",
    )(*routes, ha, hb, *own, *sib, dep)


def solution(mesh):
    group_size = mesh.shape['ep']
    cores = 2
    right = [(i, (i + cores) % group_size) for i in range(group_size)]
    left = [(i, (i - cores) % group_size) for i in range(group_size)]
    far = [(i, (i + group_size // 2) % group_size) for i in range(group_size)]
    sibling = [(i, i ^ 1) for i in range(group_size)]

    def block(hidden_in, topk_idx, norm_gain, w_router, w_sgate, s_gate, s_up, s_down, w_gate, w_up, w_down):
        tok_dev, hidden = hidden_in.shape
        top_k = topk_idx.shape[1]
        experts = w_router.shape[1]
        slots_dev = w_gate.shape[0]
        half = tok_dev // 2
        parts = (3 * half // 4, half // 4)
        capacity = (5 * tok_dev * group_size * top_k + 4 * experts - 1) // (4 * experts)
        local_max = (2 * tok_dev * top_k + experts - 1) // experts
        me = lax.axis_index('ep')

        def go_right(v):
            return lax.ppermute(v, 'ep', right)

        def go_left(v):
            return lax.ppermute(v, 'ep', left)

        chip, core = me // cores, me % cores

        def after(v, *deps):
            return lax.optimization_barrier((v,) + deps)[0]

        ha, hb = norm_call(hidden_in, norm_gain)
        ha_r1, hb_l1 = go_right(ha), go_left(hb)

        logits = jnp.concatenate([jnp.dot(h, w_router, preferred_element_type=F32) for h in (ha, hb)], axis=0)
        router_probs = jax.nn.softmax(logits, axis=-1)
        chosen = topk_idx[:, :, None] == jnp.arange(experts)[None, None, :]
        gate_vals = jnp.sum(jnp.where(chosen, router_probs[:, None, :], 0.0), axis=-1)
        own_counts = jnp.sum(chosen.astype(F32), axis=(0, 1)).reshape(1, experts)
        sib_counts = lax.ppermute(own_counts, 'ep', sibling)
        count_rows = jnp.pad(jnp.concatenate([own_counts, sib_counts], axis=0), ((0, (-2 * top_k - 2) % 8), (0, tok_dev - experts)))
        table = jnp.concatenate([topk_idx.T.astype(F32), gate_vals.T, count_rows], axis=0)
        own_w = (w_gate, w_up, w_down)
        sib_w = tuple(lax.ppermute(after(w, sib_counts), 'ep', sibling) for w in own_w)
        t_r1, t_l1 = go_right(table), go_left(table)
        t_far = lax.ppermute(table, 'ep', far)

        hb_r1, ha_l1 = go_right(hb), go_left(ha)
        half_sums = shared_call(hidden_in, ha, hb, w_sgate, s_gate, s_up, s_down)

        ha_r2, hb_l2 = go_right(ha_r1), go_left(hb_l1)

        steps = jnp.arange(group_size // cores)
        rel = cores * ((chip + steps) % (group_size // cores))
        ids = jnp.concatenate([jnp.stack([rel + core, rel + 1 - core], axis=1).reshape(-1), jnp.stack([chip, core])]).astype(jnp.int32)
        lists, glists, kept = route_call(ids, table, t_l1, t_far, t_r1, top_k, slots_dev, capacity, local_max)
        lists, glists = lists[:, :, 0, :], glists[:, :, 0, :]
        kept = kept[:, :, 0].astype(jnp.int32)

        def routes(v, row_max):
            return lists[v, :, :row_max], glists[v, :, :row_max], kept[v]

        d_a, d_b = expert_call(routes(1, 2 * local_max), ha_r1, hb_l1, own_w, sib_w, ha, 2 * local_max, (half, half))
        d_dep, d_a, d_b = d_a, go_left(d_a), go_right(d_b)
        y2 = expert_call(routes(2, local_max), ha_r2, hb_l2, own_w, sib_w, d_dep, local_max, parts * 2)
        p = [go_right(y2[0]), go_left(y2[2])]
        p += [go_right(y2[1]), go_left(y2[3])]
        y1 = expert_call(routes(3, 2 * local_max), ha_l1, hb_r1, own_w, sib_w, y2[0], 2 * local_max, parts * 2)

        def relay(i, *deps):
            return y1[i] + after(p[2 * i], *deps), y1[2 + i] + after(p[2 * i + 1], *deps)

        add_a, add_b = relay(0, y1[0])
        z0 = go_right(add_a), go_left(add_b)
        y0 = expert_call(routes(0, local_max), ha, hb, own_w, sib_w, add_b, local_max, (half, half))
        add_a, add_b = relay(1, y0[0])
        z1 = go_right(add_a), go_left(add_b)
        base = [half_sums[i] + y0[i] + d for i, d in enumerate((d_a, d_b))]
        out = final_call(0, base[0], base[1], *z0, None)
        out = final_call(parts[0], base[0], base[1], *z1, out)
        return out.reshape(tok_dev, hidden)

    row_spec = P(('dp', 'ep'), None)
    full_spec = P(None, None)
    slot_spec = P('ep', None, None)
    in_specs = (row_spec, row_spec, P(None), full_spec, full_spec, full_spec, full_spec, full_spec,
                slot_spec, slot_spec, slot_spec)
    return jax.shard_map(block, mesh=mesh, in_specs=in_specs, out_specs=row_spec, check_vma=False)
```

```python
import functools

import jax
import jax.numpy as jnp
from jax import lax
from jax.experimental import pallas as pl
from jax.experimental.pallas import tpu as pltpu
from jax.sharding import PartitionSpec as P


F32, BF16 = jnp.float32, jnp.bfloat16
CLASSES = (64, 128, 192)
PAIRS = ((0, 0), (3, 1), (2, 2), (1, 3))


def norm_kernel(x_ref, gain_ref, wr_ref, a0_ref, a1_ref, b0_ref, b1_ref, logit_ref):
    step = pl.program_id(0)
    gain = gain_ref[...].astype(F32)[None, :]
    for i, refs in enumerate(((a0_ref, a1_ref), (b0_ref, b1_ref))):
        x = x_ref[i].astype(F32)
        inv_rms = lax.rsqrt(jnp.mean(x * x, axis=-1, keepdims=True) + 1e-6)
        h = (x * inv_rms * gain).astype(BF16)
        logit_ref[i] = jnp.dot(h, wr_ref[...], preferred_element_type=F32)
        for n, ref in enumerate(refs):
            @pl.when(step // 2 == n)
            def _(ref=ref, h=h):
                ref[...] = h


def norm_call(hidden_in, norm_gain, w_router):
    toks, hidden = hidden_in.shape
    experts = w_router.shape[1]
    half = toks // 2
    rows = half // 4
    out = jax.ShapeDtypeStruct((half // 2, hidden), BF16)
    early = pl.BlockSpec((rows, hidden), lambda i: (jnp.minimum(i, 1), 0))
    late = pl.BlockSpec((rows, hidden), lambda i: (jnp.maximum(i - 2, 0), 0))
    return pl.pallas_call(
        norm_kernel,
        grid=(4,),
        out_shape=(out,) * 4 + (jax.ShapeDtypeStruct((2, half, experts), F32),),
        in_specs=[pl.BlockSpec((2, rows, hidden), lambda i: (0, i, 0)), pl.BlockSpec((hidden,), lambda i: (0,)),
                  pl.BlockSpec((hidden, experts), lambda i: (0, 0))],
        out_specs=(early, late, early, late, pl.BlockSpec((2, rows, experts), lambda i: (0, i, 0))),
        compiler_params=pltpu.CompilerParams(dimension_semantics=("arbitrary",)),
        cost_estimate=pl.CostEstimate(flops=4 * toks * hidden, transcendentals=toks, bytes_accessed=4 * toks * hidden),
        name="norm",
    )(hidden_in.reshape(2, half, hidden), norm_gain, w_router)


def final_kernel(base_a, base_b, za_ref, zb_ref, *rest):
    out_ref = rest[-1]
    out_ref[0] = (base_a[...] + za_ref[...]).astype(BF16)
    out_ref[1] = (base_b[...] + zb_ref[...]).astype(BF16)


def final_call(start, base_a, base_b, za, zb, so_far):
    (size, hidden), half = za.shape, base_a.shape[0]
    rows = 64
    first = start // rows
    block = pl.BlockSpec((rows, hidden), lambda i: (i, 0))
    base = pl.BlockSpec((rows, hidden), lambda i: (i + first, 0))
    more = [] if so_far is None else [so_far]
    return pl.pallas_call(
        final_kernel,
        grid=(size // rows,),
        out_shape=jax.ShapeDtypeStruct((2, half, hidden), BF16),
        in_specs=[base] * 2 + [block] * 2 + [pl.BlockSpec(memory_space=pl.ANY)] * len(more),
        out_specs=pl.BlockSpec((2, rows, hidden), lambda i: (0, i + first, 0)),
        input_output_aliases={4: 0} if more else {},
        compiler_params=pltpu.CompilerParams(dimension_semantics=("arbitrary",)),
        cost_estimate=pl.CostEstimate(flops=4 * size * hidden, transcendentals=0, bytes_accessed=20 * size * hidden),
        name="final",
    )(base_a, base_b, za, zb, *more)


def shared_kernel(x_ref, a0_ref, a1_ref, b0_ref, b1_ref, gate_row, sg_ref, su_ref, sd_ref, outa_ref, outb_ref):
    step = pl.program_id(0)
    for i, (h0_ref, h1_ref, out_ref) in enumerate(((a0_ref, a1_ref, outa_ref), (b0_ref, b1_ref, outb_ref))):
        h = jnp.concatenate([h0_ref[...], h1_ref[...]], axis=0)
        gate_proj = jnp.dot(h, sg_ref[...], preferred_element_type=F32)
        act = (jax.nn.silu(gate_proj) * jnp.dot(h, su_ref[...], preferred_element_type=F32)).astype(BF16)
        part = jnp.dot(act, sd_ref[...], preferred_element_type=F32)

        @pl.when(step == 0)
        def _():
            out_ref[...] = part

        @pl.when(step > 0)
        def _():
            out_ref[...] += part

        @pl.when(step == pl.num_programs(0) - 1)
        def _():
            weight = jnp.sum(h.astype(F32) * gate_row[...].astype(F32), axis=1, keepdims=True)
            out_ref[...] = x_ref[i].astype(F32) + jax.nn.sigmoid(weight) * out_ref[...]


def shared_call(hidden_in, quarters, w_sgate, s_gate, s_up, s_down):
    half, hidden = 2 * quarters[0].shape[0], quarters[0].shape[1]
    quarter = pl.BlockSpec((half // 2, hidden), lambda i: (0, 0), pipeline_mode=pl.Buffered(1))
    ff = s_gate.shape[1]
    chunk = 256
    whole = pl.BlockSpec((half, hidden), lambda i: (0, 0), pipeline_mode=pl.Buffered(1))
    wide = pl.BlockSpec((hidden, chunk), lambda i: (0, i))
    out = jax.ShapeDtypeStruct((half, hidden), F32)
    return pl.pallas_call(
        shared_kernel,
        grid=(ff // chunk,),
        out_shape=(out, out),
        in_specs=[pl.BlockSpec((2, half, hidden), lambda i: (0, 0, 0), pipeline_mode=pl.Buffered(1))] + [quarter] * 4
        + [pl.BlockSpec((1, hidden), lambda i: (0, 0)), wide, wide, pl.BlockSpec((chunk, hidden), lambda i: (i, 0))],
        out_specs=(whole, whole),
        compiler_params=pltpu.CompilerParams(dimension_semantics=("arbitrary",), vmem_limit_bytes=60 * 1024 * 1024),
        cost_estimate=pl.CostEstimate(flops=1_000_000, transcendentals=0, bytes_accessed=6 * ff * hidden),
        name="shared",
    )(hidden_in.reshape(2, half, hidden), *quarters, w_sgate.reshape(1, hidden), s_gate, s_up, s_down)


def route_kernel(geom, ids_ref, own_ref, next_ref, far_ref, prev_ref, list_ref, glist_ref, count_ref, slot_ref, gate_ref):
    top_k, slots_dev, capacity, local_max = geom
    toks = own_ref.shape[1]
    slots = 2 * slots_dev
    chip, core = ids_ref[8], ids_ref[9]

    def slot_column(like):
        order = lax.broadcasted_iota(jnp.int32, like, 0)
        mine = core * slots_dev + order
        other = (1 - core) * slots_dev + order - slots_dev
        return (chip * slots + jnp.where(order < slots_dev, mine, other)).astype(F32)

    slot_id = slot_column((slots, 1))
    lane_id = lax.broadcasted_iota(jnp.int32, (slots, 128), 1).astype(F32)
    hots, counts = [], []
    for j, ref in enumerate((own_ref, next_ref, far_ref, prev_ref)):
        table = ref[...]
        hot = jnp.zeros((slots, toks), F32)
        gate = jnp.zeros((slots, toks), F32)
        for k in range(top_k):
            hit = table[k:k + 1, :] == slot_id
            hot = hot + jnp.where(hit, 1.0, 0.0)
            gate = gate + jnp.where(hit, table[top_k + k:top_k + k + 1, :], 0.0)
        for i in range(2):
            row = table[2 * top_k + i:2 * top_k + i + 1, :128]
            counts.append(jnp.sum(jnp.where(lane_id == slot_id, row, 0.0), axis=1, keepdims=True))
        hots.append(hot)
        gate_ref[j] = gate
    hot_all = jnp.concatenate(hots, axis=0)
    hot_bf = hot_all.astype(BF16)
    tile, half = 256, toks // 2

    def before(c):
        rows = lax.broadcasted_iota(jnp.int32, (toks, tile), 0)
        cols = lax.broadcasted_iota(jnp.int32, (toks, tile), 1) + c * tile
        return jnp.where(rows < cols, 1.0, 0.0).astype(BF16)

    lowers = []
    for j in range(4):
        lower = jnp.zeros((slots, 1), F32)
        for q in range(8):
            lower = lower + counts[q] * (ids_ref[q] < ids_ref[2 * j]).astype(F32)
        lowers.append(lower)
    for c in range(toks // tile):
        pos = jnp.dot(hot_bf, before(c), preferred_element_type=F32)
        for j in range(4):
            part = pos[j * slots:(j + 1) * slots]
            kept = (hot_all[j * slots:(j + 1) * slots, c * tile:(c + 1) * tile] > 0.0) & (part + lowers[j] < capacity)
            slot_ref[j, :, c * tile:(c + 1) * tile] = jnp.where(kept, 1.0, 0.0)
    joined = []
    gates = [gate_ref[j] for j in range(4)]
    for v, (ja, jb) in enumerate(PAIRS):
        joined.append(jnp.concatenate([slot_ref[ja][:, :half], slot_ref[jb][:, half:]], axis=1))
        gate_ref[v] = jnp.concatenate([gates[ja][:, :half], gates[jb][:, half:]], axis=1)
        count_ref[v] = jnp.broadcast_to(jnp.sum(joined[v], axis=1, keepdims=True), (slots, 128))
    kept_all = jnp.concatenate(joined, axis=0)
    kept_bf = kept_all.astype(BF16)
    for c in range(toks // tile):
        pos = jnp.dot(kept_bf, before(c), preferred_element_type=F32)
        for v in range(4):
            kept = kept_all[v * slots:(v + 1) * slots, c * tile:(c + 1) * tile] > 0.0
            slot_ref[v, :, c * tile:(c + 1) * tile] = jnp.where(kept, pos[v * slots:(v + 1) * slots], -1.0)
    token = lax.broadcasted_iota(jnp.int32, (8, toks), 1)
    row8 = lax.broadcasted_iota(jnp.int32, (8, toks), 0)
    digits = jnp.where(row8 == 0, token // 32, token % 32).astype(F32)
    row_of = lax.broadcasted_iota(jnp.int32, (slots, toks), 0)
    count_row = lax.broadcasted_iota(jnp.int32, (slots, 128), 0)

    def lists(e, carry):
        for j in range(4):
            pos = jnp.sum(jnp.where(row_of == e, slot_ref[j], 0.0), axis=0, keepdims=True)
            gate = jnp.sum(jnp.where(row_of == e, gate_ref[j], 0.0), axis=0, keepdims=True)
            g1 = gate.astype(BF16).astype(F32)
            g2 = (gate - g1).astype(BF16).astype(F32)
            g3 = gate - g1 - g2
            left = jnp.where(row8 < 2, digits, jnp.where(row8 == 2, g1, jnp.where(row8 == 3, g2, g3))).astype(BF16)
            width = local_max if PAIRS[j][0] == PAIRS[j][1] else 2 * local_max
            want = lax.broadcasted_iota(jnp.int32, (width, toks), 0).astype(F32)
            pick = jnp.where(want == pos, 1.0, 0.0).astype(BF16)
            got = lax.dot_general(left, pick, (((1,), (1,)), ((), ())), preferred_element_type=F32)
            found = 32.0 * got[0:1] + got[1:2]
            held = jnp.sum(jnp.where(count_row == e, count_ref[j], 0.0), axis=0, keepdims=True)[:, 0:1]
            lane = lax.broadcasted_iota(jnp.int32, (1, width), 1).astype(F32)
            found = jnp.where(lane < held, found, float(toks)).astype(jnp.int32)
            list_ref[j, e, :, :width] = jnp.broadcast_to(found, (8, width))
            glist_ref[j, e, :, :width] = jnp.broadcast_to((got[2:3] + got[3:4]) + got[4:5], (8, width))
        return carry

    lax.fori_loop(0, slots, lists, 0)


def route_call(ids, own, nxt, far, prv, top_k, slots_dev, capacity, local_max):
    toks = own.shape[1]
    slots = 2 * slots_dev
    vmem = pl.BlockSpec(memory_space=pltpu.VMEM)
    return pl.pallas_call(
        functools.partial(route_kernel, (top_k, slots_dev, capacity, local_max)),
        out_shape=(jax.ShapeDtypeStruct((4, slots, 8, 2 * local_max), jnp.int32), jax.ShapeDtypeStruct((4, slots, 8, 2 * local_max), F32),
                   jax.ShapeDtypeStruct((4, slots, 128), F32)),
        in_specs=[pl.BlockSpec(memory_space=pltpu.SMEM)] + [vmem] * 4,
        out_specs=(vmem,) * 3,
        scratch_shapes=[pltpu.VMEM((4, slots, toks), F32), pltpu.VMEM((4, slots, toks), F32)],
        cost_estimate=pl.CostEstimate(flops=1_000_000, transcendentals=0, bytes_accessed=2_000_000),
        name="route",
    )(ids, own, nxt, far, prv)


def expert_kernel(sizes, classes, slots_dev, depth, *refs):
    refs = list(refs)
    n_src = 1

    def take(n):
        got = refs[:n]
        del refs[:n]
        return got

    lists, glists, counts = take(n_src), take(n_src), take(n_src)
    quarters = take(4)
    own, sib = take(3), take(3)
    take(1)
    ys = take(len(sizes))
    wg_ref, wu_ref, wd_ref = take(3)
    row_refs, tok_refs, sum_refs = [take(2) for _ in range(n_src)], [take(2) for _ in range(n_src)], [take(2) for _ in range(n_src)]
    stage_ref, sems, out_sems = take(3)
    step = pl.program_id(0)
    steps = 2 * slots_dev
    half, hidden = 2 * quarters[0].shape[0], quarters[0].shape[1]
    blocks = hidden // 128
    pitch, unroll, group = 8, 8, 64
    split = [(j // pitch, j % pitch) for j in range(blocks)]

    def copies(srcs, i, b):
        return [pltpu.make_async_copy(src.at[i], dst.at[b], sems.at[n, b])
                for n, (src, dst) in enumerate(zip(srcs, (wg_ref, wu_ref, wd_ref)))]

    def fetch(i):
        @pl.when(i < slots_dev)
        def _():
            for c in copies(own, i, i % depth):
                c.start()

        @pl.when((i >= slots_dev) & (i < steps))
        def _():
            for c in copies(sib, i - slots_dev, i % depth):
                c.start()

    @pl.when(step == 0)
    def _():
        for i in range(depth - 1):
            fetch(jnp.int32(i))
        for q in range(n_src):
            for ref in sum_refs[q]:
                ref[...] = jnp.zeros_like(ref)
            for ref in tok_refs[q]:
                ref[pl.ds(2 * half * pitch, pitch), :] = jnp.zeros((pitch, 128), F32)

            def spread(i, carry):
                for src, start in zip(quarters, range(0, 2 * half, half // 2)):
                    v = src[pl.ds(pl.multiple_of(i * group, group), group), :].astype(F32)
                    for j, (w, k) in enumerate(split):
                        tok_refs[q][w][pl.ds((start + i * group) * pitch + k, group, stride=pitch), :] = v[:, j * 128:(j + 1) * 128]
                return carry

            lax.fori_loop(0, half // 2 // group, spread, 0)

    fetch(step + depth - 1)
    buf = step % depth
    for c in copies(own, 0, buf):
        c.wait()
    count = [c[step] for c in counts]
    most = count[0] if n_src == 1 else jnp.maximum(count[0], count[1])
    low = 0
    for rows in classes:
        @pl.when((most > low) & (most <= rows))
        def _(rows=rows):
            xs = []
            for q in range(n_src):
                def pick(i, carry):
                    found = []
                    for u in range(unroll):
                        spot = pl.ds(pl.multiple_of(lists[q][step, i * unroll + u] * pitch, pitch), pitch)
                        found += [tok_refs[q][w][spot, :] for w in range(2)]
                    for u in range(unroll):
                        row = pl.ds(pl.multiple_of((i * unroll + u) * pitch, pitch), pitch)
                        for w in range(2):
                            row_refs[q][w][row, :] = found[2 * u + w]
                    return carry

                lax.fori_loop(0, rows // unroll, pick, 0)
                xs.append(jnp.concatenate([row_refs[q][w][pl.ds(k, rows, stride=pitch), :].astype(BF16) for w, k in split], axis=1))
            x = xs[0] if n_src == 1 else jnp.concatenate(xs, axis=0)
            gate_proj = jnp.dot(x, wg_ref[buf], preferred_element_type=F32)
            up_proj = jnp.dot(x, wu_ref[buf], preferred_element_type=F32)
            act = (jax.nn.silu(gate_proj) * up_proj).astype(BF16)
            out = jnp.dot(act, wd_ref[buf], preferred_element_type=F32).astype(BF16).astype(F32)
            for q in range(n_src):
                for j, (w, k) in enumerate(split):
                    row_refs[q][w][pl.ds(k, rows, stride=pitch), :] = out[q * rows:(q + 1) * rows, j * 128:(j + 1) * 128]

        low = rows

    for q in range(n_src):
        def scatter(i, carry):
            spots, sums = [], []
            for u in range(unroll):
                r = i * unroll + u
                spot = pl.ds(pl.multiple_of(lists[q][step, r] * pitch, pitch), pitch)
                row = pl.ds(pl.multiple_of(r * pitch, pitch), pitch)
                g = glists[q][step, r]
                for w in range(2):
                    spots.append((w, spot))
                    sums.append(sum_refs[q][w][spot, :] + row_refs[q][w][row, :] * g)
            for (w, spot), v in zip(spots, sums):
                sum_refs[q][w][spot, :] = v
            return carry

        lax.fori_loop(0, (count[q] + unroll - 1) // unroll, scatter, 0)

    @pl.when(step == steps - 1)
    def _():
        start = 0
        for n, (ref, size) in enumerate(zip(ys, sizes)):
            def put(i, n=n, ref=ref):
                rows = pl.ds(pl.multiple_of(i * group, group), group)
                return pltpu.make_async_copy(stage_ref.at[i % 2, n], ref.at[rows], out_sems.at[i % 2, n])

            def unpack(i, carry, n=n, start=start, put=put):
                @pl.when(i >= 2)
                def _():
                    put(i - 2).wait()

                for j, (w, k) in enumerate(split):
                    stage_ref[i % 2, n, :, j * 128:(j + 1) * 128] = (
                        sum_refs[0][w][pl.ds((start + i * group) * pitch + k, group, stride=pitch), :])
                put(i).start()
                return carry

            lax.fori_loop(0, size // group, unpack, 0)
            start += size
        for n, (ref, size) in enumerate(zip(ys, sizes)):
            for i in range(2):
                pltpu.make_async_copy(stage_ref.at[i, n], ref.at[pl.ds(0, group)], out_sems.at[i, n]).wait()


def expert_call(routes, quarters, own, sib, dep, row_max, sizes):
    half, hidden = 2 * quarters[0].shape[0], quarters[0].shape[1]
    slots_dev, _, ff = own[0].shape
    depth = 4
    classes = tuple(c for c in CLASSES if c < row_max) + (row_max,)
    quarter = pl.BlockSpec((half // 2, hidden), lambda s: (0, 0), pipeline_mode=pl.Buffered(1))
    smem = pl.BlockSpec(memory_space=pltpu.SMEM)
    hbm = pl.BlockSpec(memory_space=pl.ANY)
    pieces = len(sizes)
    toks = (2 * half + 8) * 8
    return pl.pallas_call(
        functools.partial(expert_kernel, sizes, classes, slots_dev, depth),
        grid=(2 * slots_dev,),
        out_shape=tuple(jax.ShapeDtypeStruct((n, hidden), F32) for n in sizes),
        in_specs=[smem] * 3 + [quarter] * 4 + [hbm] * 7,
        out_specs=(hbm,) * pieces,
        scratch_shapes=[pltpu.VMEM((depth, hidden, ff), BF16), pltpu.VMEM((depth, hidden, ff), BF16), pltpu.VMEM((depth, ff, hidden), BF16)]
        + [pltpu.VMEM((row_max * 8, 128), F32)] * 2 + [pltpu.VMEM((toks, 128), F32)] * 4
        + [pltpu.VMEM((2, pieces, 64, hidden), F32), pltpu.SemaphoreType.DMA((3, depth)), pltpu.SemaphoreType.DMA((2, pieces))],
        compiler_params=pltpu.CompilerParams(dimension_semantics=("arbitrary",), vmem_limit_bytes=62 * 1024 * 1024),
        cost_estimate=pl.CostEstimate(flops=1_000_000, transcendentals=0,
                                      bytes_accessed=2 * slots_dev * 3 * hidden * ff * 2),
        name="experts",
    )(*routes, *quarters, *own, *sib, dep)


def solution(mesh):
    group_size = mesh.shape['ep']
    cores = 2
    right = [(i, (i + cores) % group_size) for i in range(group_size)]
    left = [(i, (i - cores) % group_size) for i in range(group_size)]
    far = [(i, (i + group_size // 2) % group_size) for i in range(group_size)]
    sibling = [(i, i ^ 1) for i in range(group_size)]

    def block(hidden_in, topk_idx, norm_gain, w_router, w_sgate, s_gate, s_up, s_down, w_gate, w_up, w_down):
        tok_dev, hidden = hidden_in.shape
        top_k = topk_idx.shape[1]
        experts = w_router.shape[1]
        slots_dev = w_gate.shape[0]
        half = tok_dev // 2
        parts = (3 * half // 4, half // 4)
        capacity = (5 * tok_dev * group_size * top_k + 4 * experts - 1) // (4 * experts)
        local_max = (2 * tok_dev * top_k + experts - 1) // experts
        me = lax.axis_index('ep')

        def go_right(v):
            return lax.ppermute(v, 'ep', right)

        def go_left(v):
            return lax.ppermute(v, 'ep', left)

        chip, core = me // cores, me % cores

        def after(v, *deps):
            return lax.optimization_barrier((v,) + deps)[0]

        *quarters, logits = norm_call(hidden_in, norm_gain, w_router)
        ha, hb = quarters[:2], quarters[2:]
        first = go_right(ha[0]), go_left(hb[0])

        router_probs = jax.nn.softmax(logits.reshape(tok_dev, experts), axis=-1)
        chosen = topk_idx[:, :, None] == jnp.arange(experts)[None, None, :]
        gate_vals = jnp.sum(jnp.where(chosen, router_probs[:, None, :], 0.0), axis=-1)
        own_counts = jnp.sum(chosen.astype(F32), axis=(0, 1)).reshape(1, experts)
        sib_counts = lax.ppermute(own_counts, 'ep', sibling)
        count_rows = jnp.pad(jnp.concatenate([own_counts, sib_counts], axis=0), ((0, (-2 * top_k - 2) % 8), (0, tok_dev - experts)))
        table = jnp.concatenate([topk_idx.T.astype(F32), gate_vals.T, count_rows], axis=0)
        own_w = (w_gate, w_up, w_down)
        sib_w = tuple(lax.ppermute(w, 'ep', sibling) for w in (w_gate, after(w_up, sib_counts), after(w_down, sib_counts)))
        t_r1, t_l1 = go_right(table), go_left(table)
        t_far = lax.ppermute(table, 'ep', far)

        second = go_right(ha[1]), go_left(hb[1])
        ha_r1, hb_l1 = [first[0], second[0]], [first[1], second[1]]
        hb_r1, ha_l1 = [go_right(h) for h in hb], [go_left(h) for h in ha]
        ha_r2, hb_l2 = [go_right(h) for h in ha_r1], [go_left(h) for h in hb_l1]

        steps = jnp.arange(group_size // cores)
        rel = cores * ((chip + steps) % (group_size // cores))
        ids = jnp.concatenate([jnp.stack([rel + core, rel + 1 - core], axis=1).reshape(-1), jnp.stack([chip, core])]).astype(jnp.int32)
        lists, glists, kept = route_call(ids, table, t_l1, t_far, t_r1, top_k, slots_dev, capacity, local_max)
        lists, glists = lists[:, :, 0, :], glists[:, :, 0, :]
        kept = kept[:, :, 0].astype(jnp.int32)

        def routes(v, row_max):
            return lists[v, :, :row_max], glists[v, :, :row_max], kept[v]

        d_a, d_b = expert_call(routes(1, 2 * local_max), ha_r1 + hb_l1, own_w, sib_w, ha[0], 2 * local_max, (half, half))
        d_dep, d_a, d_b = d_a, go_left(d_a), go_right(d_b)
        y0 = expert_call(routes(0, local_max), quarters, own_w, sib_w, d_dep, local_max, (half, half))
        y2 = expert_call(routes(2, local_max), ha_r2 + hb_l2, own_w, sib_w, y0[0], local_max, parts * 2)
        p = [go_right(y2[0]), go_left(y2[2])]
        p += [go_right(y2[1]), go_left(y2[3])]
        y1 = expert_call(routes(3, 2 * local_max), ha_l1 + hb_r1, own_w, sib_w, y2[0], 2 * local_max, parts * 2)
        half_sums = shared_call(hidden_in, [after(quarters[0], y1[0])] + quarters[1:], w_sgate, s_gate, s_up, s_down)

        def relay(i, *deps):
            return y1[i] + after(p[2 * i], *deps), y1[2 + i] + after(p[2 * i + 1], *deps)

        add_a, add_b = relay(0, half_sums[0])
        z0 = go_right(add_a), go_left(add_b)
        add_a, add_b = relay(1, add_a, add_b)
        z1 = go_right(add_a), go_left(add_b)
        base = [half_sums[i] + y0[i] + d for i, d in enumerate((d_a, d_b))]
        out = final_call(0, base[0], base[1], *z0, None)
        out = final_call(parts[0], base[0], base[1], *z1, out)
        return out.reshape(tok_dev, hidden)

    row_spec = P(('dp', 'ep'), None)
    full_spec = P(None, None)
    slot_spec = P('ep', None, None)
    in_specs = (row_spec, row_spec, P(None), full_spec, full_spec, full_spec, full_spec, full_spec,
                slot_spec, slot_spec, slot_spec)
    return jax.shard_map(block, mesh=mesh, in_specs=in_specs, out_specs=row_spec, check_vma=False)
```

```python
import functools

import jax
import jax.numpy as jnp
from jax import lax
from jax.experimental import pallas as pl
from jax.experimental.pallas import tpu as pltpu
from jax.sharding import PartitionSpec as P


F32, BF16 = jnp.float32, jnp.bfloat16
CLASSES = (64, 128, 192)
PAIRS = ((0, 0), (3, 1), (2, 2), (1, 3))


def norm_kernel(x_ref, gain_ref, ha_ref, hb_ref):
    gain = gain_ref[...].astype(F32)[None, :]
    for i, out_ref in enumerate((ha_ref, hb_ref)):
        x = x_ref[i].astype(F32)
        inv_rms = lax.rsqrt(jnp.mean(x * x, axis=-1, keepdims=True) + 1e-6)
        out_ref[...] = (x * inv_rms * gain).astype(BF16)


def norm_call(hidden_in, norm_gain):
    toks, hidden = hidden_in.shape
    half, rows = toks // 2, 128
    out = jax.ShapeDtypeStruct((half, hidden), BF16)
    block = pl.BlockSpec((rows, hidden), lambda i: (i, 0))
    return pl.pallas_call(
        norm_kernel,
        grid=(half // rows,),
        out_shape=(out, out),
        in_specs=[pl.BlockSpec((2, rows, hidden), lambda i: (0, i, 0)), pl.BlockSpec((hidden,), lambda i: (0,))],
        out_specs=(block, block),
        compiler_params=pltpu.CompilerParams(dimension_semantics=("arbitrary",)),
        cost_estimate=pl.CostEstimate(flops=4 * toks * hidden, transcendentals=toks, bytes_accessed=4 * toks * hidden),
        name="norm",
    )(hidden_in.reshape(2, half, hidden), norm_gain)


def final_kernel(base_a, base_b, za_ref, zb_ref, *rest):
    out_ref = rest[-1]
    out_ref[0] = (base_a[...] + za_ref[...]).astype(BF16)
    out_ref[1] = (base_b[...] + zb_ref[...]).astype(BF16)


def final_call(start, base_a, base_b, za, zb, so_far):
    (size, hidden), half = za.shape, base_a.shape[0]
    rows = 64
    first = start // rows
    block = pl.BlockSpec((rows, hidden), lambda i: (i, 0))
    base = pl.BlockSpec((rows, hidden), lambda i: (i + first, 0))
    more = [] if so_far is None else [so_far]
    return pl.pallas_call(
        final_kernel,
        grid=(size // rows,),
        out_shape=jax.ShapeDtypeStruct((2, half, hidden), BF16),
        in_specs=[base] * 2 + [block] * 2 + [pl.BlockSpec(memory_space=pl.ANY)] * len(more),
        out_specs=pl.BlockSpec((2, rows, hidden), lambda i: (0, i + first, 0)),
        input_output_aliases={4: 0} if more else {},
        compiler_params=pltpu.CompilerParams(dimension_semantics=("arbitrary",)),
        cost_estimate=pl.CostEstimate(flops=4 * size * hidden, transcendentals=0, bytes_accessed=20 * size * hidden),
        name="final",
    )(base_a, base_b, za, zb, *more)


def shared_kernel(x_ref, ha_ref, hb_ref, gate_row, sg_ref, su_ref, sd_ref, outa_ref, outb_ref):
    step = pl.program_id(0)
    for i, (h_ref, out_ref) in enumerate(((ha_ref, outa_ref), (hb_ref, outb_ref))):
        h = h_ref[...]
        gate_proj = jnp.dot(h, sg_ref[...], preferred_element_type=F32)
        act = (jax.nn.silu(gate_proj) * jnp.dot(h, su_ref[...], preferred_element_type=F32)).astype(BF16)
        part = jnp.dot(act, sd_ref[...], preferred_element_type=F32)

        @pl.when(step == 0)
        def _():
            out_ref[...] = part

        @pl.when(step > 0)
        def _():
            out_ref[...] += part

        @pl.when(step == pl.num_programs(0) - 1)
        def _():
            weight = jnp.sum(h.astype(F32) * gate_row[...].astype(F32), axis=1, keepdims=True)
            out_ref[...] = x_ref[i].astype(F32) + jax.nn.sigmoid(weight) * out_ref[...]


def shared_call(hidden_in, ha, hb, w_sgate, s_gate, s_up, s_down):
    half, hidden = ha.shape
    ff = s_gate.shape[1]
    chunk = 256
    whole = pl.BlockSpec((half, hidden), lambda i: (0, 0), pipeline_mode=pl.Buffered(1))
    wide = pl.BlockSpec((hidden, chunk), lambda i: (0, i))
    out = jax.ShapeDtypeStruct((half, hidden), F32)
    return pl.pallas_call(
        shared_kernel,
        grid=(ff // chunk,),
        out_shape=(out, out),
        in_specs=[pl.BlockSpec((2, half, hidden), lambda i: (0, 0, 0), pipeline_mode=pl.Buffered(1)), whole, whole,
                  pl.BlockSpec((1, hidden), lambda i: (0, 0)), wide, wide, pl.BlockSpec((chunk, hidden), lambda i: (i, 0))],
        out_specs=(whole, whole),
        compiler_params=pltpu.CompilerParams(dimension_semantics=("arbitrary",), vmem_limit_bytes=60 * 1024 * 1024),
        cost_estimate=pl.CostEstimate(flops=1_000_000, transcendentals=0, bytes_accessed=6 * ff * hidden),
        name="shared",
    )(hidden_in.reshape(2, half, hidden), ha, hb, w_sgate.reshape(1, hidden), s_gate, s_up, s_down)


def route_kernel(geom, ids_ref, own_ref, next_ref, far_ref, prev_ref, list_ref, glist_ref, count_ref, slot_ref, gate_ref):
    top_k, slots_dev, capacity, local_max = geom
    toks = own_ref.shape[1]
    slots = 2 * slots_dev
    chip, core = ids_ref[8], ids_ref[9]

    def slot_column(like):
        order = lax.broadcasted_iota(jnp.int32, like, 0)
        mine = core * slots_dev + order
        other = (1 - core) * slots_dev + order - slots_dev
        return (chip * slots + jnp.where(order < slots_dev, mine, other)).astype(F32)

    slot_id = slot_column((slots, 1))
    lane_id = lax.broadcasted_iota(jnp.int32, (slots, 128), 1).astype(F32)
    hots, counts = [], []
    for j, ref in enumerate((own_ref, next_ref, far_ref, prev_ref)):
        table = ref[...]
        hot = jnp.zeros((slots, toks), F32)
        gate = jnp.zeros((slots, toks), F32)
        for k in range(top_k):
            hit = table[k:k + 1, :] == slot_id
            hot = hot + jnp.where(hit, 1.0, 0.0)
            gate = gate + jnp.where(hit, table[top_k + k:top_k + k + 1, :], 0.0)
        for i in range(2):
            row = table[2 * top_k + i:2 * top_k + i + 1, :128]
            counts.append(jnp.sum(jnp.where(lane_id == slot_id, row, 0.0), axis=1, keepdims=True))
        hots.append(hot)
        gate_ref[j] = gate
    hot_all = jnp.concatenate(hots, axis=0)
    hot_bf = hot_all.astype(BF16)
    tile, half = 256, toks // 2

    def before(c):
        rows = lax.broadcasted_iota(jnp.int32, (toks, tile), 0)
        cols = lax.broadcasted_iota(jnp.int32, (toks, tile), 1) + c * tile
        return jnp.where(rows < cols, 1.0, 0.0).astype(BF16)

    lowers = []
    for j in range(4):
        lower = jnp.zeros((slots, 1), F32)
        for q in range(8):
            lower = lower + counts[q] * (ids_ref[q] < ids_ref[2 * j]).astype(F32)
        lowers.append(lower)
    for c in range(toks // tile):
        pos = jnp.dot(hot_bf, before(c), preferred_element_type=F32)
        for j in range(4):
            part = pos[j * slots:(j + 1) * slots]
            kept = (hot_all[j * slots:(j + 1) * slots, c * tile:(c + 1) * tile] > 0.0) & (part + lowers[j] < capacity)
            slot_ref[j, :, c * tile:(c + 1) * tile] = jnp.where(kept, 1.0, 0.0)
    joined = []
    gates = [gate_ref[j] for j in range(4)]
    for v, (ja, jb) in enumerate(PAIRS):
        joined.append(jnp.concatenate([slot_ref[ja][:, :half], slot_ref[jb][:, half:]], axis=1))
        gate_ref[v] = jnp.concatenate([gates[ja][:, :half], gates[jb][:, half:]], axis=1)
        count_ref[v] = jnp.broadcast_to(jnp.sum(joined[v], axis=1, keepdims=True), (slots, 128))
    kept_all = jnp.concatenate(joined, axis=0)
    kept_bf = kept_all.astype(BF16)
    for c in range(toks // tile):
        pos = jnp.dot(kept_bf, before(c), preferred_element_type=F32)
        for v in range(4):
            kept = kept_all[v * slots:(v + 1) * slots, c * tile:(c + 1) * tile] > 0.0
            slot_ref[v, :, c * tile:(c + 1) * tile] = jnp.where(kept, pos[v * slots:(v + 1) * slots], -1.0)
    token = lax.broadcasted_iota(jnp.int32, (8, toks), 1)
    row8 = lax.broadcasted_iota(jnp.int32, (8, toks), 0)
    digits = jnp.where(row8 == 0, token // 32, token % 32).astype(F32)
    row_of = lax.broadcasted_iota(jnp.int32, (slots, toks), 0)
    count_row = lax.broadcasted_iota(jnp.int32, (slots, 128), 0)

    def lists(e, carry):
        for j in range(4):
            pos = jnp.sum(jnp.where(row_of == e, slot_ref[j], 0.0), axis=0, keepdims=True)
            gate = jnp.sum(jnp.where(row_of == e, gate_ref[j], 0.0), axis=0, keepdims=True)
            g1 = gate.astype(BF16).astype(F32)
            g2 = (gate - g1).astype(BF16).astype(F32)
            g3 = gate - g1 - g2
            left = jnp.where(row8 < 2, digits, jnp.where(row8 == 2, g1, jnp.where(row8 == 3, g2, g3))).astype(BF16)
            width = local_max if PAIRS[j][0] == PAIRS[j][1] else 2 * local_max
            want = lax.broadcasted_iota(jnp.int32, (width, toks), 0).astype(F32)
            pick = jnp.where(want == pos, 1.0, 0.0).astype(BF16)
            got = lax.dot_general(left, pick, (((1,), (1,)), ((), ())), preferred_element_type=F32)
            found = 32.0 * got[0:1] + got[1:2]
            held = jnp.sum(jnp.where(count_row == e, count_ref[j], 0.0), axis=0, keepdims=True)[:, 0:1]
            lane = lax.broadcasted_iota(jnp.int32, (1, width), 1).astype(F32)
            found = jnp.where(lane < held, found, float(toks)).astype(jnp.int32)
            list_ref[j, e, :, :width] = jnp.broadcast_to(found, (8, width))
            glist_ref[j, e, :, :width] = jnp.broadcast_to((got[2:3] + got[3:4]) + got[4:5], (8, width))
        return carry

    lax.fori_loop(0, slots, lists, 0)


def route_call(ids, own, nxt, far, prv, top_k, slots_dev, capacity, local_max):
    toks = own.shape[1]
    slots = 2 * slots_dev
    vmem = pl.BlockSpec(memory_space=pltpu.VMEM)
    return pl.pallas_call(
        functools.partial(route_kernel, (top_k, slots_dev, capacity, local_max)),
        out_shape=(jax.ShapeDtypeStruct((4, slots, 8, 2 * local_max), jnp.int32), jax.ShapeDtypeStruct((4, slots, 8, 2 * local_max), F32),
                   jax.ShapeDtypeStruct((4, slots, 128), F32)),
        in_specs=[pl.BlockSpec(memory_space=pltpu.SMEM)] + [vmem] * 4,
        out_specs=(vmem,) * 3,
        scratch_shapes=[pltpu.VMEM((4, slots, toks), F32), pltpu.VMEM((4, slots, toks), F32)],
        cost_estimate=pl.CostEstimate(flops=1_000_000, transcendentals=0, bytes_accessed=2_000_000),
        name="route",
    )(ids, own, nxt, far, prv)


def expert_kernel(sizes, classes, slots_dev, depth, *refs):
    refs = list(refs)
    n_src = 1

    def take(n):
        got = refs[:n]
        del refs[:n]
        return got

    lists, glists, counts = take(n_src), take(n_src), take(n_src)
    has, hbs = take(n_src), take(n_src)
    own, sib = take(3), take(3)
    take(1)
    ys = take(len(sizes))
    wg_ref, wu_ref, wd_ref = take(3)
    row_refs, tok_refs, sum_refs = [take(2) for _ in range(n_src)], [take(2) for _ in range(n_src)], [take(2) for _ in range(n_src)]
    stage_ref, sems, out_sems = take(3)
    step = pl.program_id(0)
    steps = 2 * slots_dev
    half, hidden = has[0].shape
    blocks = hidden // 128
    pitch, unroll, group = 8, 8, 64
    split = [(j // pitch, j % pitch) for j in range(blocks)]

    def copies(srcs, i, b):
        return [pltpu.make_async_copy(src.at[i], dst.at[b], sems.at[n, b])
                for n, (src, dst) in enumerate(zip(srcs, (wg_ref, wu_ref, wd_ref)))]

    def fetch(i):
        @pl.when(i < slots_dev)
        def _():
            for c in copies(own, i, i % depth):
                c.start()

        @pl.when((i >= slots_dev) & (i < steps))
        def _():
            for c in copies(sib, i - slots_dev, i % depth):
                c.start()

    @pl.when(step == 0)
    def _():
        for i in range(depth - 1):
            fetch(jnp.int32(i))
        for q in range(n_src):
            for ref in sum_refs[q]:
                ref[...] = jnp.zeros_like(ref)
            for ref in tok_refs[q]:
                ref[pl.ds(2 * half * pitch, pitch), :] = jnp.zeros((pitch, 128), F32)

            def spread(i, carry):
                for src, start in ((has[q], 0), (hbs[q], half)):
                    v = src[pl.ds(pl.multiple_of(i * group, group), group), :].astype(F32)
                    for j, (w, k) in enumerate(split):
                        tok_refs[q][w][pl.ds((start + i * group) * pitch + k, group, stride=pitch), :] = v[:, j * 128:(j + 1) * 128]
                return carry

            lax.fori_loop(0, half // group, spread, 0)

    fetch(step + depth - 1)
    buf = step % depth
    for c in copies(own, 0, buf):
        c.wait()
    count = [c[step] for c in counts]
    most = count[0] if n_src == 1 else jnp.maximum(count[0], count[1])
    low = 0
    for rows in classes:
        @pl.when((most > low) & (most <= rows))
        def _(rows=rows):
            xs = []
            for q in range(n_src):
                def pick(i, carry):
                    found = []
                    for u in range(unroll):
                        spot = pl.ds(pl.multiple_of(lists[q][step, i * unroll + u] * pitch, pitch), pitch)
                        found += [tok_refs[q][w][spot, :] for w in range(2)]
                    for u in range(unroll):
                        row = pl.ds(pl.multiple_of((i * unroll + u) * pitch, pitch), pitch)
                        for w in range(2):
                            row_refs[q][w][row, :] = found[2 * u + w]
                    return carry

                lax.fori_loop(0, rows // unroll, pick, 0)
                xs.append(jnp.concatenate([row_refs[q][w][pl.ds(k, rows, stride=pitch), :].astype(BF16) for w, k in split], axis=1))
            x = xs[0] if n_src == 1 else jnp.concatenate(xs, axis=0)
            gate_proj = jnp.dot(x, wg_ref[buf], preferred_element_type=F32)
            up_proj = jnp.dot(x, wu_ref[buf], preferred_element_type=F32)
            act = (jax.nn.silu(gate_proj) * up_proj).astype(BF16)
            out = jnp.dot(act, wd_ref[buf], preferred_element_type=F32).astype(BF16).astype(F32)
            for q in range(n_src):
                for j, (w, k) in enumerate(split):
                    row_refs[q][w][pl.ds(k, rows, stride=pitch), :] = out[q * rows:(q + 1) * rows, j * 128:(j + 1) * 128]

        low = rows

    for q in range(n_src):
        def scatter(i, carry):
            spots, sums = [], []
            for u in range(unroll):
                r = i * unroll + u
                spot = pl.ds(pl.multiple_of(lists[q][step, r] * pitch, pitch), pitch)
                row = pl.ds(pl.multiple_of(r * pitch, pitch), pitch)
                g = glists[q][step, r]
                for w in range(2):
                    spots.append((w, spot))
                    sums.append(sum_refs[q][w][spot, :] + row_refs[q][w][row, :] * g)
            for (w, spot), v in zip(spots, sums):
                sum_refs[q][w][spot, :] = v
            return carry

        lax.fori_loop(0, (count[q] + unroll - 1) // unroll, scatter, 0)

    @pl.when(step == steps - 1)
    def _():
        start = 0
        for n, (ref, size) in enumerate(zip(ys, sizes)):
            def put(i, n=n, ref=ref):
                rows = pl.ds(pl.multiple_of(i * group, group), group)
                return pltpu.make_async_copy(stage_ref.at[i % 2, n], ref.at[rows], out_sems.at[i % 2, n])

            def unpack(i, carry, n=n, start=start, put=put):
                @pl.when(i >= 2)
                def _():
                    put(i - 2).wait()

                for j, (w, k) in enumerate(split):
                    stage_ref[i % 2, n, :, j * 128:(j + 1) * 128] = (
                        sum_refs[0][w][pl.ds((start + i * group) * pitch + k, group, stride=pitch), :])
                put(i).start()
                return carry

            lax.fori_loop(0, size // group, unpack, 0)
            start += size
        for n, (ref, size) in enumerate(zip(ys, sizes)):
            for i in range(2):
                pltpu.make_async_copy(stage_ref.at[i, n], ref.at[pl.ds(0, group)], out_sems.at[i, n]).wait()


def expert_call(routes, ha, hb, own, sib, dep, row_max, sizes):
    half, hidden = ha.shape
    slots_dev, _, ff = own[0].shape
    depth = 4
    classes = tuple(c for c in CLASSES if c < row_max) + (row_max,)
    whole = pl.BlockSpec((half, hidden), lambda s: (0, 0), pipeline_mode=pl.Buffered(1))
    smem = pl.BlockSpec(memory_space=pltpu.SMEM)
    hbm = pl.BlockSpec(memory_space=pl.ANY)
    pieces = len(sizes)
    toks = (2 * half + 8) * 8
    return pl.pallas_call(
        functools.partial(expert_kernel, sizes, classes, slots_dev, depth),
        grid=(2 * slots_dev,),
        out_shape=tuple(jax.ShapeDtypeStruct((n, hidden), F32) for n in sizes),
        in_specs=[smem] * 3 + [whole] * 2 + [hbm] * 7,
        out_specs=(hbm,) * pieces,
        scratch_shapes=[pltpu.VMEM((depth, hidden, ff), BF16), pltpu.VMEM((depth, hidden, ff), BF16), pltpu.VMEM((depth, ff, hidden), BF16)]
        + [pltpu.VMEM((row_max * 8, 128), F32)] * 2 + [pltpu.VMEM((toks, 128), F32)] * 4
        + [pltpu.VMEM((2, pieces, 64, hidden), F32), pltpu.SemaphoreType.DMA((3, depth)), pltpu.SemaphoreType.DMA((2, pieces))],
        compiler_params=pltpu.CompilerParams(dimension_semantics=("arbitrary",), vmem_limit_bytes=62 * 1024 * 1024),
        cost_estimate=pl.CostEstimate(flops=1_000_000, transcendentals=0,
                                      bytes_accessed=2 * slots_dev * 3 * hidden * ff * 2),
        name="experts",
    )(*routes, ha, hb, *own, *sib, dep)


def solution(mesh):
    group_size = mesh.shape['ep']
    cores = 2
    right = [(i, (i + cores) % group_size) for i in range(group_size)]
    left = [(i, (i - cores) % group_size) for i in range(group_size)]
    far = [(i, (i + group_size // 2) % group_size) for i in range(group_size)]
    sibling = [(i, i ^ 1) for i in range(group_size)]

    def block(hidden_in, topk_idx, norm_gain, w_router, w_sgate, s_gate, s_up, s_down, w_gate, w_up, w_down):
        tok_dev, hidden = hidden_in.shape
        top_k = topk_idx.shape[1]
        experts = w_router.shape[1]
        slots_dev = w_gate.shape[0]
        half = tok_dev // 2
        parts = (5 * half // 8, 3 * half // 8)
        capacity = (5 * tok_dev * group_size * top_k + 4 * experts - 1) // (4 * experts)
        local_max = (2 * tok_dev * top_k + experts - 1) // experts
        me = lax.axis_index('ep')

        def go_right(v):
            return lax.ppermute(v, 'ep', right)

        def go_left(v):
            return lax.ppermute(v, 'ep', left)

        chip, core = me // cores, me % cores

        def after(v, *deps):
            return lax.optimization_barrier((v,) + deps)[0]

        sib_gate = lax.ppermute(w_gate, 'ep', sibling)
        ha, hb = norm_call(hidden_in, norm_gain)
        ha_r1, hb_l1 = go_right(ha), go_left(hb)

        logits = jnp.concatenate([jnp.dot(h, w_router, preferred_element_type=F32) for h in (ha, hb)], axis=0)
        router_probs = jax.nn.softmax(logits, axis=-1)
        chosen = topk_idx[:, :, None] == jnp.arange(experts)[None, None, :]
        gate_vals = jnp.sum(jnp.where(chosen, router_probs[:, None, :], 0.0), axis=-1)
        own_counts = jnp.sum(chosen.astype(F32), axis=(0, 1)).reshape(1, experts)
        sib_counts = lax.ppermute(own_counts, 'ep', sibling)
        count_rows = jnp.pad(jnp.concatenate([own_counts, sib_counts], axis=0), ((0, (-2 * top_k - 2) % 8), (0, tok_dev - experts)))
        table = jnp.concatenate([topk_idx.T.astype(F32), gate_vals.T, count_rows], axis=0)
        own_w = (w_gate, w_up, w_down)
        sib_w = (sib_gate, *(lax.ppermute(after(w, sib_counts), 'ep', sibling) for w in own_w[1:]))
        t_r1, t_l1 = go_right(table), go_left(table)
        t_far = lax.ppermute(table, 'ep', far)

        hb_r1, ha_l1 = go_right(hb), go_left(ha)
        ha_r2, hb_l2 = go_right(ha_r1), go_left(hb_l1)

        steps = jnp.arange(group_size // cores)
        rel = cores * ((chip + steps) % (group_size // cores))
        ids = jnp.concatenate([jnp.stack([rel + core, rel + 1 - core], axis=1).reshape(-1), jnp.stack([chip, core])]).astype(jnp.int32)
        lists, glists, kept = route_call(ids, table, t_l1, t_far, t_r1, top_k, slots_dev, capacity, local_max)
        lists, glists = lists[:, :, 0, :], glists[:, :, 0, :]
        kept = kept[:, :, 0].astype(jnp.int32)

        def routes(v, row_max):
            return lists[v, :, :row_max], glists[v, :, :row_max], kept[v]

        d_a, d_b = expert_call(routes(1, 2 * local_max), ha_r1, hb_l1, own_w, sib_w, ha, 2 * local_max, (half, half))
        d_dep, d_a, d_b = d_a, go_left(d_a), go_right(d_b)
        y2 = expert_call(routes(2, local_max), ha_r2, hb_l2, own_w, sib_w, d_dep, local_max, parts * 2)
        p = [go_right(y2[0]), go_left(y2[2])]
        p += [go_right(y2[1]), go_left(y2[3])]
        y1 = expert_call(routes(3, 2 * local_max), ha_l1, hb_r1, own_w, sib_w, y2[0], 2 * local_max, parts * 2)
        half_sums = shared_call(hidden_in, after(ha, y1[0]), hb, w_sgate, s_gate, s_up, s_down)

        def relay(i, *deps):
            return y1[i] + after(p[2 * i], *deps), y1[2 + i] + after(p[2 * i + 1], *deps)

        add_a, add_b = relay(0, half_sums[0])
        z0 = go_right(add_a), go_left(add_b)
        y0 = expert_call(routes(0, local_max), ha, hb, own_w, sib_w, add_b, local_max, (half, half))
        add_a, add_b = relay(1, y0[0])
        z1 = go_right(add_a), go_left(add_b)
        base = [half_sums[i] + y0[i] + d for i, d in enumerate((d_a, d_b))]
        out = final_call(0, base[0], base[1], *z0, None)
        out = final_call(parts[0], base[0], base[1], *z1, out)
        return out.reshape(tok_dev, hidden)

    row_spec = P(('dp', 'ep'), None)
    full_spec = P(None, None)
    slot_spec = P('ep', None, None)
    in_specs = (row_spec, row_spec, P(None), full_spec, full_spec, full_spec, full_spec, full_spec,
                slot_spec, slot_spec, slot_spec)
    return jax.shard_map(block, mesh=mesh, in_specs=in_specs, out_specs=row_spec, check_vma=False)
```

```python
import functools

import jax
import jax.numpy as jnp
from jax import lax
from jax.experimental import pallas as pl
from jax.experimental.pallas import tpu as pltpu
from jax.sharding import PartitionSpec as P


F32, BF16 = jnp.float32, jnp.bfloat16
CLASSES = (64, 128, 192)
PAIRS = ((0, 0), (3, 1), (2, 2), (1, 3))


def norm_kernel(x_ref, gain_ref, ha_ref, hb_ref):
    gain = gain_ref[...].astype(F32)[None, :]
    for i, out_ref in enumerate((ha_ref, hb_ref)):
        x = x_ref[i].astype(F32)
        inv_rms = lax.rsqrt(jnp.mean(x * x, axis=-1, keepdims=True) + 1e-6)
        out_ref[...] = (x * inv_rms * gain).astype(BF16)


def norm_call(hidden_in, norm_gain):
    toks, hidden = hidden_in.shape
    half, rows = toks // 2, 128
    out = jax.ShapeDtypeStruct((half, hidden), BF16)
    block = pl.BlockSpec((rows, hidden), lambda i: (i, 0))
    return pl.pallas_call(
        norm_kernel,
        grid=(half // rows,),
        out_shape=(out, out),
        in_specs=[pl.BlockSpec((2, rows, hidden), lambda i: (0, i, 0)), pl.BlockSpec((hidden,), lambda i: (0,))],
        out_specs=(block, block),
        compiler_params=pltpu.CompilerParams(dimension_semantics=("arbitrary",)),
        cost_estimate=pl.CostEstimate(flops=4 * toks * hidden, transcendentals=toks, bytes_accessed=4 * toks * hidden),
        name="norm",
    )(hidden_in.reshape(2, half, hidden), norm_gain)


def final_kernel(base_a, base_b, za_ref, zb_ref, *rest):
    out_ref = rest[-1]
    out_ref[0] = (base_a[...] + za_ref[...]).astype(BF16)
    out_ref[1] = (base_b[...] + zb_ref[...]).astype(BF16)


def final_call(start, base_a, base_b, za, zb, so_far):
    (size, hidden), half = za.shape, base_a.shape[0]
    rows = 64
    first = start // rows
    block = pl.BlockSpec((rows, hidden), lambda i: (i, 0))
    base = pl.BlockSpec((rows, hidden), lambda i: (i + first, 0))
    more = [] if so_far is None else [so_far]
    return pl.pallas_call(
        final_kernel,
        grid=(size // rows,),
        out_shape=jax.ShapeDtypeStruct((2, half, hidden), BF16),
        in_specs=[base] * 2 + [block] * 2 + [pl.BlockSpec(memory_space=pl.ANY)] * len(more),
        out_specs=pl.BlockSpec((2, rows, hidden), lambda i: (0, i + first, 0)),
        input_output_aliases={4: 0} if more else {},
        compiler_params=pltpu.CompilerParams(dimension_semantics=("arbitrary",)),
        cost_estimate=pl.CostEstimate(flops=4 * size * hidden, transcendentals=0, bytes_accessed=20 * size * hidden),
        name="final",
    )(base_a, base_b, za, zb, *more)


def shared_kernel(x_ref, ha_ref, hb_ref, gate_row, sg_ref, su_ref, sd_ref, outa_ref, outb_ref):
    step = pl.program_id(0)
    for i, (h_ref, out_ref) in enumerate(((ha_ref, outa_ref), (hb_ref, outb_ref))):
        h = h_ref[...]
        gate_proj = jnp.dot(h, sg_ref[...], preferred_element_type=F32)
        act = (jax.nn.silu(gate_proj) * jnp.dot(h, su_ref[...], preferred_element_type=F32)).astype(BF16)
        part = jnp.dot(act, sd_ref[...], preferred_element_type=F32)

        @pl.when(step == 0)
        def _():
            out_ref[...] = part

        @pl.when(step > 0)
        def _():
            out_ref[...] += part

        @pl.when(step == pl.num_programs(0) - 1)
        def _():
            weight = jnp.sum(h.astype(F32) * gate_row[...].astype(F32), axis=1, keepdims=True)
            out_ref[...] = x_ref[i].astype(F32) + jax.nn.sigmoid(weight) * out_ref[...]


def shared_call(hidden_in, ha, hb, w_sgate, s_gate, s_up, s_down):
    half, hidden = ha.shape
    ff = s_gate.shape[1]
    chunk = 256
    whole = pl.BlockSpec((half, hidden), lambda i: (0, 0), pipeline_mode=pl.Buffered(1))
    wide = pl.BlockSpec((hidden, chunk), lambda i: (0, i))
    out = jax.ShapeDtypeStruct((half, hidden), F32)
    return pl.pallas_call(
        shared_kernel,
        grid=(ff // chunk,),
        out_shape=(out, out),
        in_specs=[pl.BlockSpec((2, half, hidden), lambda i: (0, 0, 0), pipeline_mode=pl.Buffered(1)), whole, whole,
                  pl.BlockSpec((1, hidden), lambda i: (0, 0)), wide, wide, pl.BlockSpec((chunk, hidden), lambda i: (i, 0))],
        out_specs=(whole, whole),
        compiler_params=pltpu.CompilerParams(dimension_semantics=("arbitrary",), vmem_limit_bytes=60 * 1024 * 1024),
        cost_estimate=pl.CostEstimate(flops=1_000_000, transcendentals=0, bytes_accessed=6 * ff * hidden),
        name="shared",
    )(hidden_in.reshape(2, half, hidden), ha, hb, w_sgate.reshape(1, hidden), s_gate, s_up, s_down)


def route_kernel(geom, which, ids_ref, own_ref, next_ref, far_ref, prev_ref, list_ref, glist_ref, count_ref, slot_ref, gate_ref):
    top_k, slots_dev, capacity, local_max = geom
    toks = own_ref.shape[1]
    slots = 2 * slots_dev
    chip, core = ids_ref[8], ids_ref[9]

    def slot_column(like):
        order = lax.broadcasted_iota(jnp.int32, like, 0)
        mine = core * slots_dev + order
        other = (1 - core) * slots_dev + order - slots_dev
        return (chip * slots + jnp.where(order < slots_dev, mine, other)).astype(F32)

    slot_id = slot_column((slots, 1))
    lane_id = lax.broadcasted_iota(jnp.int32, (slots, 128), 1).astype(F32)
    hots, counts = [], []
    for j, ref in enumerate((own_ref, next_ref, far_ref, prev_ref)):
        table = ref[...]
        hot = jnp.zeros((slots, toks), F32)
        gate = jnp.zeros((slots, toks), F32)
        for k in range(top_k):
            hit = table[k:k + 1, :] == slot_id
            hot = hot + jnp.where(hit, 1.0, 0.0)
            gate = gate + jnp.where(hit, table[top_k + k:top_k + k + 1, :], 0.0)
        for i in range(2):
            row = table[2 * top_k + i:2 * top_k + i + 1, :128]
            counts.append(jnp.sum(jnp.where(lane_id == slot_id, row, 0.0), axis=1, keepdims=True))
        hots.append(hot)
        gate_ref[j] = gate
    hot_all = jnp.concatenate(hots, axis=0)
    hot_bf = hot_all.astype(BF16)
    tile, half = 256, toks // 2

    def before(c):
        rows = lax.broadcasted_iota(jnp.int32, (toks, tile), 0)
        cols = lax.broadcasted_iota(jnp.int32, (toks, tile), 1) + c * tile
        return jnp.where(rows < cols, 1.0, 0.0).astype(BF16)

    lowers = []
    for j in range(4):
        lower = jnp.zeros((slots, 1), F32)
        for q in range(8):
            lower = lower + counts[q] * (ids_ref[q] < ids_ref[2 * j]).astype(F32)
        lowers.append(lower)
    for c in range(toks // tile):
        pos = jnp.dot(hot_bf, before(c), preferred_element_type=F32)
        for j in range(4):
            part = pos[j * slots:(j + 1) * slots]
            kept = (hot_all[j * slots:(j + 1) * slots, c * tile:(c + 1) * tile] > 0.0) & (part + lowers[j] < capacity)
            slot_ref[j, :, c * tile:(c + 1) * tile] = jnp.where(kept, 1.0, 0.0)
    joined = []
    gates = [gate_ref[j] for j in range(4)]
    for v, (ja, jb) in enumerate(PAIRS[w] for w in which):
        joined.append(jnp.concatenate([slot_ref[ja][:, :half], slot_ref[jb][:, half:]], axis=1))
        gate_ref[v] = jnp.concatenate([gates[ja][:, :half], gates[jb][:, half:]], axis=1)
        count_ref[v] = jnp.broadcast_to(jnp.sum(joined[v], axis=1, keepdims=True), (slots, 128))
    kept_all = jnp.concatenate(joined, axis=0)
    kept_bf = kept_all.astype(BF16)
    for c in range(toks // tile):
        pos = jnp.dot(kept_bf, before(c), preferred_element_type=F32)
        for v in range(len(which)):
            kept = kept_all[v * slots:(v + 1) * slots, c * tile:(c + 1) * tile] > 0.0
            slot_ref[v, :, c * tile:(c + 1) * tile] = jnp.where(kept, pos[v * slots:(v + 1) * slots], -1.0)
    token = lax.broadcasted_iota(jnp.int32, (8, toks), 1)
    row8 = lax.broadcasted_iota(jnp.int32, (8, toks), 0)
    digits = jnp.where(row8 == 0, token // 32, token % 32).astype(F32)
    row_of = lax.broadcasted_iota(jnp.int32, (slots, toks), 0)
    count_row = lax.broadcasted_iota(jnp.int32, (slots, 128), 0)

    def lists(e, carry):
        for j, w in enumerate(which):
            pos = jnp.sum(jnp.where(row_of == e, slot_ref[j], 0.0), axis=0, keepdims=True)
            gate = jnp.sum(jnp.where(row_of == e, gate_ref[j], 0.0), axis=0, keepdims=True)
            g1 = gate.astype(BF16).astype(F32)
            g2 = (gate - g1).astype(BF16).astype(F32)
            g3 = gate - g1 - g2
            left = jnp.where(row8 < 2, digits, jnp.where(row8 == 2, g1, jnp.where(row8 == 3, g2, g3))).astype(BF16)
            width = local_max if PAIRS[w][0] == PAIRS[w][1] else 2 * local_max
            want = lax.broadcasted_iota(jnp.int32, (width, toks), 0).astype(F32)
            pick = jnp.where(want == pos, 1.0, 0.0).astype(BF16)
            got = lax.dot_general(left, pick, (((1,), (1,)), ((), ())), preferred_element_type=F32)
            found = 32.0 * got[0:1] + got[1:2]
            held = jnp.sum(jnp.where(count_row == e, count_ref[j], 0.0), axis=0, keepdims=True)[:, 0:1]
            lane = lax.broadcasted_iota(jnp.int32, (1, width), 1).astype(F32)
            found = jnp.where(lane < held, found, float(toks)).astype(jnp.int32)
            list_ref[j, e, :, :width] = jnp.broadcast_to(found, (8, width))
            glist_ref[j, e, :, :width] = jnp.broadcast_to((got[2:3] + got[3:4]) + got[4:5], (8, width))
        return carry

    lax.fori_loop(0, slots, lists, 0)


def route_call(which, ids, own, nxt, far, prv, top_k, slots_dev, capacity, local_max):
    toks = own.shape[1]
    slots = 2 * slots_dev
    vmem = pl.BlockSpec(memory_space=pltpu.VMEM)
    return pl.pallas_call(
        functools.partial(route_kernel, (top_k, slots_dev, capacity, local_max), which),
        out_shape=(jax.ShapeDtypeStruct((len(which), slots, 8, 2 * local_max), jnp.int32),
                   jax.ShapeDtypeStruct((len(which), slots, 8, 2 * local_max), F32), jax.ShapeDtypeStruct((len(which), slots, 128), F32)),
        in_specs=[pl.BlockSpec(memory_space=pltpu.SMEM)] + [vmem] * 4,
        out_specs=(vmem,) * 3,
        scratch_shapes=[pltpu.VMEM((4, slots, toks), F32), pltpu.VMEM((4, slots, toks), F32)],
        cost_estimate=pl.CostEstimate(flops=1_000_000, transcendentals=0, bytes_accessed=2_000_000),
        name="route",
    )(ids, own, nxt, far, prv)


def expert_kernel(sizes, classes, slots_dev, depth, *refs):
    refs = list(refs)
    n_src = 1

    def take(n):
        got = refs[:n]
        del refs[:n]
        return got

    lists, glists, counts = take(n_src), take(n_src), take(n_src)
    has, hbs = take(n_src), take(n_src)
    own, sib = take(3), take(3)
    take(1)
    ys = take(len(sizes))
    wg_ref, wu_ref, wd_ref = take(3)
    row_refs, tok_refs, sum_refs = [take(2) for _ in range(n_src)], [take(2) for _ in range(n_src)], [take(2) for _ in range(n_src)]
    stage_ref, sems, out_sems = take(3)
    step = pl.program_id(0)
    steps = 2 * slots_dev
    half, hidden = has[0].shape
    blocks = hidden // 128
    pitch, unroll, group = 8, 8, 64
    split = [(j // pitch, j % pitch) for j in range(blocks)]

    def copies(srcs, i, b):
        return [pltpu.make_async_copy(src.at[i], dst.at[b], sems.at[n, b])
                for n, (src, dst) in enumerate(zip(srcs, (wg_ref, wu_ref, wd_ref)))]

    def fetch(i):
        @pl.when(i < slots_dev)
        def _():
            for c in copies(own, i, i % depth):
                c.start()

        @pl.when((i >= slots_dev) & (i < steps))
        def _():
            for c in copies(sib, i - slots_dev, i % depth):
                c.start()

    @pl.when(step == 0)
    def _():
        for i in range(depth - 1):
            fetch(jnp.int32(i))
        for q in range(n_src):
            for ref in sum_refs[q]:
                ref[...] = jnp.zeros_like(ref)
            for ref in tok_refs[q]:
                ref[pl.ds(2 * half * pitch, pitch), :] = jnp.zeros((pitch, 128), F32)

            def spread(i, carry):
                for src, start in ((has[q], 0), (hbs[q], half)):
                    v = src[pl.ds(pl.multiple_of(i * group, group), group), :].astype(F32)
                    for j, (w, k) in enumerate(split):
                        tok_refs[q][w][pl.ds((start + i * group) * pitch + k, group, stride=pitch), :] = v[:, j * 128:(j + 1) * 128]
                return carry

            lax.fori_loop(0, half // group, spread, 0)

    fetch(step + depth - 1)
    buf = step % depth
    for c in copies(own, 0, buf):
        c.wait()
    count = [c[step] for c in counts]
    most = count[0] if n_src == 1 else jnp.maximum(count[0], count[1])
    low = 0
    for rows in classes:
        @pl.when((most > low) & (most <= rows))
        def _(rows=rows):
            xs = []
            for q in range(n_src):
                def pick(i, carry):
                    found = []
                    for u in range(unroll):
                        spot = pl.ds(pl.multiple_of(lists[q][step, i * unroll + u] * pitch, pitch), pitch)
                        found += [tok_refs[q][w][spot, :] for w in range(2)]
                    for u in range(unroll):
                        row = pl.ds(pl.multiple_of((i * unroll + u) * pitch, pitch), pitch)
                        for w in range(2):
                            row_refs[q][w][row, :] = found[2 * u + w]
                    return carry

                lax.fori_loop(0, rows // unroll, pick, 0)
                xs.append(jnp.concatenate([row_refs[q][w][pl.ds(k, rows, stride=pitch), :].astype(BF16) for w, k in split], axis=1))
            x = xs[0] if n_src == 1 else jnp.concatenate(xs, axis=0)
            gate_proj = jnp.dot(x, wg_ref[buf], preferred_element_type=F32)
            up_proj = jnp.dot(x, wu_ref[buf], preferred_element_type=F32)
            act = (jax.nn.silu(gate_proj) * up_proj).astype(BF16)
            out = jnp.dot(act, wd_ref[buf], preferred_element_type=F32).astype(BF16).astype(F32)
            for q in range(n_src):
                for j, (w, k) in enumerate(split):
                    row_refs[q][w][pl.ds(k, rows, stride=pitch), :] = out[q * rows:(q + 1) * rows, j * 128:(j + 1) * 128]

        low = rows

    for q in range(n_src):
        def scatter(i, carry):
            spots, sums = [], []
            for u in range(unroll):
                r = i * unroll + u
                spot = pl.ds(pl.multiple_of(lists[q][step, r] * pitch, pitch), pitch)
                row = pl.ds(pl.multiple_of(r * pitch, pitch), pitch)
                g = glists[q][step, r]
                for w in range(2):
                    spots.append((w, spot))
                    sums.append(sum_refs[q][w][spot, :] + row_refs[q][w][row, :] * g)
            for (w, spot), v in zip(spots, sums):
                sum_refs[q][w][spot, :] = v
            return carry

        lax.fori_loop(0, (count[q] + unroll - 1) // unroll, scatter, 0)

    @pl.when(step == steps - 1)
    def _():
        size = sizes[0]
        outs = [(0, ref, n * size) for n, ref in enumerate(ys)]

        def put(n, ref, i):
            rows = pl.ds(pl.multiple_of(i * group, group), group)
            return pltpu.make_async_copy(stage_ref.at[i % 2, n], ref.at[rows], out_sems.at[i % 2, n])

        def unpack(i, carry):
            for n, (q, ref, start) in enumerate(outs):
                @pl.when(i >= 2)
                def _():
                    put(n, ref, i).wait()

                for j, (w, k) in enumerate(split):
                    stage_ref[i % 2, n, :, j * 128:(j + 1) * 128] = (
                        sum_refs[q][w][pl.ds((start + i * group) * pitch + k, group, stride=pitch), :])
                put(n, ref, i).start()
            return carry

        lax.fori_loop(0, size // group, unpack, 0)
        for i in range(2):
            for n, (q, ref, start) in enumerate(outs):
                put(n, ref, i).wait()


def expert_call(routes, ha, hb, own, sib, dep, row_max, sizes):
    half, hidden = ha.shape
    slots_dev, _, ff = own[0].shape
    depth = 4
    classes = tuple(c for c in CLASSES if c < row_max) + (row_max,)
    whole = pl.BlockSpec((half, hidden), lambda s: (0, 0), pipeline_mode=pl.Buffered(1))
    smem = pl.BlockSpec(memory_space=pltpu.SMEM)
    hbm = pl.BlockSpec(memory_space=pl.ANY)
    pieces = len(sizes)
    toks = (2 * half + 8) * 8
    return pl.pallas_call(
        functools.partial(expert_kernel, sizes, classes, slots_dev, depth),
        grid=(2 * slots_dev,),
        out_shape=tuple(jax.ShapeDtypeStruct((n, hidden), F32) for n in sizes),
        in_specs=[smem] * 3 + [whole] * 2 + [hbm] * 7,
        out_specs=(hbm,) * pieces,
        scratch_shapes=[pltpu.VMEM((depth, hidden, ff), BF16), pltpu.VMEM((depth, hidden, ff), BF16), pltpu.VMEM((depth, ff, hidden), BF16)]
        + [pltpu.VMEM((row_max * 8, 128), F32)] * 2 + [pltpu.VMEM((toks, 128), F32)] * 4
        + [pltpu.VMEM((2, pieces, 64, hidden), F32), pltpu.SemaphoreType.DMA((3, depth)), pltpu.SemaphoreType.DMA((2, pieces))],
        compiler_params=pltpu.CompilerParams(dimension_semantics=("arbitrary",), vmem_limit_bytes=62 * 1024 * 1024),
        cost_estimate=pl.CostEstimate(flops=1_000_000, transcendentals=0,
                                      bytes_accessed=2 * slots_dev * 3 * hidden * ff * 2),
        name="experts",
    )(*routes, ha, hb, *own, *sib, dep)


def solution(mesh):
    group_size = mesh.shape['ep']
    cores = 2
    right = [(i, (i + cores) % group_size) for i in range(group_size)]
    left = [(i, (i - cores) % group_size) for i in range(group_size)]
    far = [(i, (i + group_size // 2) % group_size) for i in range(group_size)]
    sibling = [(i, i ^ 1) for i in range(group_size)]

    def block(hidden_in, topk_idx, norm_gain, w_router, w_sgate, s_gate, s_up, s_down, w_gate, w_up, w_down):
        tok_dev, hidden = hidden_in.shape
        top_k = topk_idx.shape[1]
        experts = w_router.shape[1]
        slots_dev = w_gate.shape[0]
        half = tok_dev // 2
        parts = (half // 2, half // 2)
        capacity = (5 * tok_dev * group_size * top_k + 4 * experts - 1) // (4 * experts)
        local_max = (2 * tok_dev * top_k + experts - 1) // experts
        me = lax.axis_index('ep')

        def go_right(v):
            return lax.ppermute(v, 'ep', right)

        def go_left(v):
            return lax.ppermute(v, 'ep', left)

        chip, core = me // cores, me % cores

        def after(v, *deps):
            return lax.optimization_barrier((v,) + deps)[0]

        sib_gate = lax.ppermute(w_gate, 'ep', sibling)
        ha, hb = norm_call(hidden_in, norm_gain)
        ha_r1, hb_l1 = go_right(ha), go_left(hb)

        logits = jnp.concatenate([jnp.dot(h, w_router, preferred_element_type=F32) for h in (ha, hb)], axis=0)
        router_probs = jax.nn.softmax(logits, axis=-1)
        chosen = topk_idx[:, :, None] == jnp.arange(experts)[None, None, :]
        gate_vals = jnp.sum(jnp.where(chosen, router_probs[:, None, :], 0.0), axis=-1)
        own_counts = jnp.sum(chosen.astype(F32), axis=(0, 1)).reshape(1, experts)
        sib_counts = lax.ppermute(own_counts, 'ep', sibling)
        count_rows = jnp.pad(jnp.concatenate([own_counts, sib_counts], axis=0), ((0, (-2 * top_k - 2) % 8), (0, tok_dev - experts)))
        table = jnp.concatenate([topk_idx.T.astype(F32), gate_vals.T, count_rows], axis=0)
        own_w = (w_gate, w_up, w_down)
        sib_w = (sib_gate, *(lax.ppermute(after(w, sib_counts), 'ep', sibling) for w in own_w[1:]))
        t_r1, t_l1 = go_right(table), go_left(table)
        t_far = lax.ppermute(table, 'ep', far)

        hb_r1, ha_l1 = go_right(hb), go_left(ha)
        ha_r2, hb_l2 = go_right(ha_r1), go_left(hb_l1)

        steps = jnp.arange(group_size // cores)
        rel = cores * ((chip + steps) % (group_size // cores))
        ids = jnp.concatenate([jnp.stack([rel + core, rel + 1 - core], axis=1).reshape(-1), jnp.stack([chip, core])]).astype(jnp.int32)

        def plan(which, *deps):
            got = route_call(which, ids, after(table, *deps), t_l1, t_far, t_r1, top_k, slots_dev, capacity, local_max)
            lists, glists, kept = got[0][:, :, 0, :], got[1][:, :, 0, :], got[2][:, :, 0].astype(jnp.int32)
            return {v: (lists[n], glists[n], kept[n]) for n, v in enumerate(which)}

        plans = plan((1,))

        def routes(v, row_max):
            return plans[v][0][:, :row_max], plans[v][1][:, :row_max], plans[v][2]

        d_a, d_b = expert_call(routes(1, 2 * local_max), ha_r1, hb_l1, own_w, sib_w, ha, 2 * local_max, (half, half))
        d_dep, d_a, d_b = d_a, go_left(d_a), go_right(d_b)
        plans.update(plan((2, 3, 0), d_dep))
        y2 = expert_call(routes(2, local_max), ha_r2, hb_l2, own_w, sib_w, d_dep, local_max, parts * 2)
        p = [go_right(y2[0]), go_left(y2[2])]
        p += [go_right(y2[1]), go_left(y2[3])]
        y1 = expert_call(routes(3, 2 * local_max), ha_l1, hb_r1, own_w, sib_w, y2[0], 2 * local_max, parts * 2)
        half_sums = shared_call(hidden_in, after(ha, y1[0]), hb, w_sgate, s_gate, s_up, s_down)

        def relay(i, *deps):
            return y1[i] + after(p[2 * i], *deps), y1[2 + i] + after(p[2 * i + 1], *deps)

        add_a, add_b = relay(0, half_sums[0])
        z0 = go_right(add_a), go_left(add_b)
        y0 = expert_call(routes(0, local_max), ha, hb, own_w, sib_w, add_b, local_max, (half, half))
        add_a, add_b = relay(1, y0[0])
        z1 = go_right(add_a), go_left(add_b)
        base = [half_sums[i] + y0[i] + d for i, d in enumerate((d_a, d_b))]
        out = final_call(0, base[0], base[1], *z0, None)
        out = final_call(parts[0], base[0], base[1], *z1, out)
        return out.reshape(tok_dev, hidden)

    row_spec = P(('dp', 'ep'), None)
    full_spec = P(None, None)
    slot_spec = P('ep', None, None)
    in_specs = (row_spec, row_spec, P(None), full_spec, full_spec, full_spec, full_spec, full_spec,
                slot_spec, slot_spec, slot_spec)
    return jax.shard_map(block, mesh=mesh, in_specs=in_specs, out_specs=row_spec, check_vma=False)
```
